128 devices in a mesh: gx: 8 (over x, core), gy: 16 (over y, z).
Axes of the slice: x: 4, y: 4, z: 4, core: 2. Of those that a mesh axis runs over, the one named last changes fastest.
Arguments:
- fine_start: float32 [3, 2048, 8192], P(None, 'gx', 'gy'), may hold values from -6 to 6
- fine_known: float32 [3, 2048, 8192], P(None, 'gx', 'gy'), may hold values from -18 to 18
- fine_mu: float32 [2048, 8192], P('gx', 'gy'), may hold values from 1 to 10
- coarse_start: float32 [3, 1024, 4096], P(None, ('gx', 'gy')), may hold values from -6 to 6
- coarse_known: float32 [3, 1024, 4096], P(None, ('gx', 'gy')), may hold values from -18 to 18
- coarse_mu: float32 [1024, 4096], P(('gx', 'gy')), may hold values from 1 to 10
Outputs:
- fine_ghost: float32 [3, 2048, 8192], P(None, 'gx', 'gy')
- coarse_ghost: float32 [3, 1024, 4096], P(None, ('gx', 'gy'))
- norms: float32 [3], replicated
The draws below stay inside these ranges and needn't reach their ends.
All inputs are finite; a program needn't handle non-finite values.
Results may differ from the reference program's by a relative error of at most 0.0001.
Values sent between devices are 32-bit elements; how exact they have to be, the bound alone decides.
A program may use at most 128 MiB of HBM per device.

```python
import math
import jax
import jax.numpy as jnp

ITERS = 3
NCX = 1024
NCY = 4096
NFX = 2048
NFY = 8192


def rising_field(key, rows, cols):
    ramp = 1.0 + 2.0 * jnp.arange(rows, dtype=jnp.float32)[:, None] / max(rows - 1, 1)
    base = jnp.clip(jax.random.normal(key, (3, rows, cols), jnp.float32), -6.0, 6.0)
    return base * ramp[None]


def draw_fine_known(key, part):
    return rising_field(jax.random.fold_in(key, 11), NFX, NFY)


def draw_coarse_known(key, part):
    return rising_field(jax.random.fold_in(key, 23), NCX, NCY)


def steps_of(stream_key, extent, split, least, top_value):
    def one(dim, blocks):
        steps = jax.random.uniform(jax.random.fold_in(jax.random.fold_in(stream_key, 6), dim), (blocks,), jnp.float32, least / len(split), top_value / len(split))
        return jnp.repeat(jnp.exp(steps), extent[dim] // blocks).reshape((-1,) + (1,) * (len(extent) - dim - 1))

    gain = one(*split[0])
    for cut in split[1:]:
        gain = gain * one(*cut)
    return gain


def bell_draw(key, extent, spread, limit, split=(), kind=jnp.bfloat16):
    factor_of = steps_of(key, extent, split, -0.22, 0.18) if split else 1.0
    drawn = jax.random.normal(key, extent, jnp.float32) * spread * factor_of
    return jnp.minimum(jnp.maximum(drawn, -limit), limit).astype(kind)


def setup_inputs(seed: int = 0) -> dict:
    arg_keys = jax.random.split(jax.random.key(seed), 7)
    return {
        "fine_start": bell_draw(arg_keys[0], (3, NFX, NFY), 1.0, 6.0, ((1, 8), (2, 16)), jnp.float32),
        "fine_known": draw_fine_known(jax.random.fold_in(arg_keys[6], 71), 0),
        "fine_mu": jnp.clip(jnp.exp(math.log(10.0) - 2.3025851 * jax.random.uniform(arg_keys[2], (NFX, NFY), jnp.float32) ** steps_of(arg_keys[2], (NFX, NFY), ((0, 8), (1, 16)), -0.2, 0.2)), 1.0, 10.0),
        "coarse_start": bell_draw(arg_keys[3], (3, NCX, NCY), 1.0, 6.0, ((1, 128),), jnp.float32),
        "coarse_known": draw_coarse_known(jax.random.fold_in(arg_keys[6], 71), 0),
        "coarse_mu": jnp.clip(jnp.exp(math.log(10.0) - 2.3025851 * jax.random.uniform(arg_keys[5], (NCX, NCY), jnp.float32) ** steps_of(arg_keys[5], (NCX, NCY), ((0, 128),), -0.2, 0.2)), 1.0, 10.0),
    }


def neighbours(padded):
    return padded[:, 2:, 1:-1] + padded[:, :-2, 1:-1] + padded[:, 1:-1, 2:] + padded[:, 1:-1, :-2]

def prolong(padded):
    components, rows_plus, cols_plus = padded.shape
    middle = padded[:, 1:-1, :]
    even_rows = 0.75 * middle + 0.25 * padded[:, :-2, :]
    odd_rows = 0.75 * middle + 0.25 * padded[:, 2:, :]
    row_fine = jnp.stack([even_rows, odd_rows], axis=2).reshape(components, 2 * (rows_plus - 2), cols_plus)
    centre = row_fine[:, :, 1:-1]
    even_cols = 0.75 * centre + 0.25 * row_fine[:, :, :-2]
    odd_cols = 0.75 * centre + 0.25 * row_fine[:, :, 2:]
    return jnp.stack([even_cols, odd_cols], axis=3).reshape(components, 2 * (rows_plus - 2), 2 * (cols_plus - 2))

def restrict(fine):
    return 0.25 * (fine[:, 0::2, 0::2] + fine[:, 1::2, 0::2] + fine[:, 0::2, 1::2] + fine[:, 1::2, 1::2])

def pad_plane(field):
    return jnp.pad(field, ((0, 0), (1, 1), (1, 1)))

def reference(fine_start, fine_known, fine_mu, coarse_start, coarse_known, coarse_mu):
    fine_diag = (fine_mu + 1.0)[None]
    coarse_diag = (coarse_mu + 1.0)[None]
    fine_ghost = fine_start
    coarse_ghost = coarse_start
    cell_total = 3.0 * (NFX * NFY + NCX * NCY)
    norm_list = []
    for sweep in range(ITERS):
        coarse_padded = pad_plane(coarse_ghost)
        fine_res = fine_known + 0.25 * neighbours(pad_plane(fine_ghost)) + 0.5 * prolong(coarse_padded) - fine_diag * fine_ghost
        coarse_res = coarse_known + 0.25 * neighbours(coarse_padded) + 0.5 * restrict(fine_ghost) - coarse_diag * coarse_ghost
        total = jnp.sum(fine_res * fine_res) + jnp.sum(coarse_res * coarse_res)
        norm_list.append(jnp.sqrt(total / cell_total))
        fine_ghost = fine_ghost + fine_res / fine_diag
        coarse_ghost = coarse_ghost + coarse_res / coarse_diag
    return (fine_ghost, coarse_ghost, jnp.stack(norm_list))
```

```python
import functools

import jax
import jax.numpy as jnp
from jax import lax
from jax.experimental import pallas as pl
from jax.experimental.pallas import tpu as pltpu
from jax.sharding import PartitionSpec as P

MESH = pl.DeviceIdType.MESH
F32 = jnp.float32
SWEEPS = 3
LANES = 128
SUB = 8
FINE_OFF = 24
COARSE_OFF = 16
EDGE = 4


class Shape:
    def __init__(self, gx, gy, fine_rows, fine_cols):
        self.gx, self.gy = gx, gy
        self.fine_rows, self.fine_cols = fine_rows, fine_cols
        self.coarse_rows, self.coarse_cols = fine_rows // 2, fine_cols // 2
        self.tiles = self.coarse_rows // SUB
        self.slabs = fine_cols // LANES
        self.halo = self.slabs
        self.all_slabs = self.slabs + 1
        self.wide = self.coarse_cols
        self.fine_buf = fine_rows + 2 * FINE_OFF
        self.coarse_buf = self.coarse_rows + 2 * COARSE_OFF
        self.blocks = fine_rows // LANES
        self.cells = 3.0 * gx * gy * fine_rows * fine_cols * 1.25


def lane_iota():
    return lax.broadcasted_iota(jnp.int32, (SUB, LANES), 1)


def kernel(
    sh,
    fine_start,
    fine_known,
    fine_mu,
    coarse_start,
    coarse_known,
    coarse_mu,
    fine_out,
    coarse_out,
    norm_out,
    f_a,
    f_b,
    kn,
    mu,
    fd,
    fi,
    c_a,
    c_b,
    q_a,
    q_b,
    w_a,
    w_b,
    ck,
    cd,
    ci,
    pre,
    own,
    pack,
    got_c,
    got_p,
    got_k,
    edge_out,
    edge_in,
    fin,
    part,
    part_gy,
    part_gx,
    load_sem,
    edge_send,
    edge_recv,
    row_send,
    row_recv,
    a_send,
    a_recv,
    fwd_send,
    fwd_recv,
    fin_send,
    fin_recv,
    out_sem,
    norm_send,
    norm_recv_y,
    norm_recv_x,
):
    gx, gy = sh.gx, sh.gy
    i = lax.axis_index("gx")
    j = lax.axis_index("gy")
    halo, slabs, tiles = sh.halo, sh.slabs, sh.tiles
    wide = sh.wide
    lane = lane_iota()
    even = lane % 2 == 0
    first = lane == 0
    last = lane == LANES - 1

    def remote(src, dst, send, recv, to_i, to_j):
        return pltpu.make_async_remote_copy(
            src_ref=src,
            dst_ref=dst,
            send_sem=send,
            recv_sem=recv,
            device_id=(to_i, to_j),
            device_id_type=MESH,
        )

    loads = []

    def load(src, dst):
        copy = pltpu.make_async_copy(src, dst, load_sem.at[len(loads)])
        copy.start()
        loads.append(copy)
        return copy

    own_loads = [
        load(coarse_start, own.at[pl.ds(0, 3)]),
        load(coarse_known, own.at[pl.ds(3, 3)]),
        load(coarse_mu, own.at[6]),
    ]
    rows_in = pl.ds(FINE_OFF, sh.fine_rows)
    fine_loads = []
    for t in [halo - 1, 0] + list(range(1, slabs - 1)):
        cols = pl.ds(LANES * t, LANES)
        fine_loads.append(load(fine_start.at[:, :, cols], f_a.at[:, t, rows_in, :]))
        fine_loads.append(load(fine_known.at[:, :, cols], kn.at[:, t, rows_in, :]))
        fine_loads.append(load(fine_mu.at[:, cols], mu.at[t, rows_in, :]))

    zero = jnp.zeros((SUB, LANES), F32)
    fine_end = FINE_OFF + sh.fine_rows

    def zero_fine(step, carry):
        for row in (0, 8, 16, fine_end, fine_end + 8, fine_end + 16):
            rows = pl.ds(row, SUB)
            mu[step, rows, :] = zero
            for k in range(3):
                f_a[k, step, rows, :] = zero
                f_b[k, step, rows, :] = zero
                kn[k, step, rows, :] = zero
        for row in (0, 8, sh.coarse_buf - 16, sh.coarse_buf - 8):
            rows = pl.ds(row, SUB)
            for k in range(3):
                for ref in (c_a, c_b, q_a, q_b):
                    ref[k, step, rows, :] = zero
        return carry

    lax.fori_loop(0, sh.all_slabs, zero_fine, 0)
    for side in range(2):
        for p in range(7):
            edge_in[side, p] = zero
    for slot in (0, gy + 1):
        got_p[slot] = zero
        for u in range(wide // LANES):
            cols = pl.ds(LANES * u, LANES)
            for p in range(3):
                got_c[slot, p, :, cols] = zero
            for p in range(4):
                got_k[slot, p, :, cols] = zero

    barrier = pltpu.get_barrier_semaphore()
    for step in range(1, gy):
        pl.semaphore_signal(
            barrier, inc=1, device_id=(i, lax.rem(j + step, gy)), device_id_type=MESH
        )
    for step in range(1, gx):
        pl.semaphore_signal(
            barrier, inc=1, device_id=(lax.rem(i + step, gx), j), device_id_type=MESH
        )

    for copy in own_loads:
        copy.wait()

    def pack_for(dest, carry):
        after = pl.multiple_of(lax.rem(dest + 1, gy) * wide, LANES)
        before = pl.multiple_of(lax.rem(dest + gy - 1, gy) * wide + wide - LANES, LANES)
        keep_after = jnp.where(dest < gy - 1, 1.0, 0.0).astype(F32)
        keep_before = jnp.where(dest > 0, 1.0, 0.0).astype(F32)
        keep = jnp.where(lane < 64, keep_after, keep_before)
        tile = zero
        for p in range(7):
            both = jnp.where(
                lane < 64, own[p, :, pl.ds(after, LANES)], own[p, :, pl.ds(before, LANES)]
            )
            both = pltpu.roll(both * keep, 8 * p + EDGE, 1)
            here = (lane >= 8 * p) & (lane < 8 * p + 8)
            tile = jnp.where(here, both, tile)
        pack[dest] = tile
        return carry

    lax.fori_loop(0, gy, pack_for, 0)

    for copy in fine_loads:
        copy.wait()

    def planes():
        return [(f_a, k) for k in range(3)] + [(kn, k) for k in range(3)] + [(mu, None)]

    def slab_of(ref, k, t, rows):
        return ref[t, rows, :] if k is None else ref[k, t, rows, :]

    for p, (ref, k) in enumerate(planes()):
        for b in range(sh.blocks):
            rows = pl.ds(FINE_OFF + LANES * b, LANES)
            to_right = slab_of(ref, k, slabs - 1, rows).T
            to_left = slab_of(ref, k, 0, rows).T
            edge_out[0, p, pl.ds(EDGE * b, EDGE), :] = to_right[LANES - EDGE :, :]
            edge_out[1, p, pl.ds(EDGE * b, EDGE), :] = to_left[:EDGE, :]

    pl.semaphore_wait(barrier, gy + gx - 2)

    edge_right = remote(
        edge_out.at[0], edge_in.at[0], edge_send.at[0], edge_recv.at[0], i, lax.rem(j + 1, gy)
    )
    edge_left = remote(
        edge_out.at[1], edge_in.at[1], edge_send.at[1], edge_recv.at[1], i, lax.rem(j + gy - 1, gy)
    )

    @pl.when(j < gy - 1)
    def _():
        edge_right.start()

    @pl.when(j > 0)
    def _():
        edge_left.start()

    def sends_first(step):
        to = lax.rem(j + step, gy)
        from_ = lax.rem(j + gy - step, gy)
        cols = pl.ds(pl.multiple_of(to * wide, LANES), wide)
        return (
            remote(
                own.at[pl.ds(0, 3), :, cols],
                got_c.at[j + 1],
                a_send.at[0, step],
                a_recv.at[0, step],
                i,
                to,
            ),
            remote(pack.at[to], got_p.at[j + 1], a_send.at[1, step], a_recv.at[1, step], i, to),
        )

    def sends_second(step):
        to = lax.rem(j + step, gy)
        cols = pl.ds(pl.multiple_of(to * wide, LANES), wide)
        return remote(
            own.at[pl.ds(3, 4), :, cols],
            got_k.at[j + 1],
            a_send.at[2, step],
            a_recv.at[2, step],
            i,
            to,
        )

    order = list(range(1, gy))
    firsts = {step: sends_first(step) for step in order}
    seconds = {step: sends_second(step) for step in order}
    for step in order:
        firsts[step][0].start()
        firsts[step][1].start()
    for step in order:
        seconds[step].start()

    got_p[j + 1] = pack[j]
    for u in range(wide // LANES):
        cols = pl.ds(pl.multiple_of(j * wide + LANES * u, LANES), LANES)
        for p in range(7):
            piece = own[p, :, cols]
            if p < 3:
                got_c[j + 1, p, :, pl.ds(LANES * u, LANES)] = piece
            else:
                got_k[j + 1, p - 3, :, pl.ds(LANES * u, LANES)] = piece

    @pl.when(j > 0)
    def _():
        edge_right.wait_recv()

    @pl.when(j < gy - 1)
    def _():
        edge_left.wait_recv()

    between = jnp.zeros((LANES - 2 * EDGE, LANES), F32)
    for p, (ref, k) in enumerate(planes()):
        for b in range(sh.blocks):
            from_left = edge_in[0, p, pl.ds(EDGE * b, EDGE), :]
            from_right = edge_in[1, p, pl.ds(EDGE * b, EDGE), :]
            slab = jnp.concatenate([from_right, between, from_left], axis=0).T
            rows = pl.ds(FINE_OFF + LANES * b, LANES)
            if k is None:
                ref[halo, rows, :] = slab
            else:
                ref[k, halo, rows, :] = slab

    down_i, up_i = lax.rem(i + 1, gx), lax.rem(i + gx - 1, gx)
    lo_src, hi_src = pl.ds(FINE_OFF, SUB), pl.ds(fine_end - SUB, SUB)
    lo_dst, hi_dst = pl.ds(FINE_OFF - SUB, SUB), pl.ds(fine_end, SUB)

    def row_copies(src, dst, direction, to_i):
        made = []
        for n, ref in enumerate((f_a, kn)):
            made.append(
                remote(
                    ref.at[:, :, src, :],
                    ref.at[:, :, dst, :],
                    row_send.at[direction, n],
                    row_recv.at[direction, n],
                    to_i,
                    j,
                )
            )
        made.append(
            remote(
                mu.at[:, src, :],
                mu.at[:, dst, :],
                row_send.at[direction, 2],
                row_recv.at[direction, 2],
                to_i,
                j,
            )
        )
        return made

    rows_down = row_copies(hi_src, lo_dst, 0, down_i)
    rows_up = row_copies(lo_src, hi_dst, 1, up_i)

    @pl.when(i < gx - 1)
    def _():
        for copy in rows_down:
            copy.start()

    @pl.when(i > 0)
    def _():
        for copy in rows_up:
            copy.start()

    has_up, has_down = i > 0, i < gx - 1
    has_left, has_right = j > 0, j < gy - 1
    pair = lane // 2

    def spread_index(p):
        right = 8 * p + EDGE + pair
        left = 8 * p + pair - (LANES - 8) // 2
        return jnp.where(lane < 8, right, jnp.where(lane >= LANES - 8, left, 0))

    def take(value, index):
        return jnp.take_along_axis(value, index, axis=1, mode="promise_in_bounds")

    def spread(slot, ref, p, packed_plane):
        out = []
        for t in range(slabs):
            value = ref[slot, p, :, pl.ds(LANES * (t // 2), LANES)]
            out.append(take(value, 64 * (t % 2) + pair))
        out.append(take(got_p[slot], spread_index(packed_plane)))
        return out

    def shifted(values):
        count = len(values)
        right = [pltpu.roll(v, 1, 1) for v in values]
        left = [pltpu.roll(v, LANES - 1, 1) for v in values]
        before = [jnp.where(first, right[t - 1], right[t]) for t in range(count)]
        after = [jnp.where(last, left[(t + 1) % count], left[t]) for t in range(count)]
        return before, after

    def produce(k, row, values, c_ref, q_ref, w_ref):
        before, after = shifted(values)
        rows = pl.ds(row, SUB)
        for t, value in enumerate(values):
            outer = jnp.where(even, before[t], after[t])
            swap = jnp.where(even, pltpu.roll(outer, LANES - 1, 1), pltpu.roll(outer, 1, 1))
            c_ref[k, t, rows, :] = value
            q_ref[k, t, rows, :] = 0.375 * value + 0.125 * outer
            w_ref[k, t, rows, :] = outer + swap

    def coarse_row(m):
        return pl.multiple_of(COARSE_OFF + SUB * m, SUB)

    def spread_first(slot, carry):
        for k in range(3):
            produce(k, coarse_row(slot - 1), spread(slot, got_c, k, k), c_a, q_a, w_a)
        return carry

    halo_lanes = ((lane < 8) & has_right) | ((lane >= LANES - 8) & has_left)
    halo_lanes_fine = ((lane < EDGE) & has_right) | ((lane >= LANES - EDGE) & has_left)

    def spread_second(slot, carry):
        rows = pl.ds(coarse_row(slot - 1), SUB)
        inside = ((slot > 0) | has_up) & ((slot <= gy) | has_down)
        for k in range(3):
            for t, value in enumerate(spread(slot, got_k, k, 3 + k)):
                ck[k, t, rows, :] = value
        for t, value in enumerate(spread(slot, got_k, 3, 6)):
            diag = value + 1.0
            valid = (halo_lanes if t == halo else (lane >= 0)) & inside
            cd[t, rows, :] = diag
            ci[t, rows, :] = jnp.where(valid, 1.0 / diag, 0.0)
        return carry

    fwd_copies = {}
    for n, ref in enumerate((got_c, got_p, got_k)):
        fwd_copies[n] = (
            remote(ref.at[gy], ref.at[0], fwd_send.at[0, n], fwd_recv.at[0, n], down_i, j),
            remote(ref.at[1], ref.at[gy + 1], fwd_send.at[1, n], fwd_recv.at[1, n], up_i, j),
        )

    def wait_from(kinds, source):
        step = lax.rem(j - source + gy, gy)

        @pl.when(step > 0)
        def _():
            for kind in kinds:
                dst = (got_c, got_p, got_k)[kind].at[source + 1]
                pltpu.make_async_remote_copy(
                    src_ref=dst,
                    dst_ref=dst,
                    send_sem=a_send.at[kind, step],
                    recv_sem=a_recv.at[kind, step],
                    device_id=(i, source),
                    device_id_type=MESH,
                ).wait_recv()

    def pass_on(kinds):
        wait_from(kinds, gy - 1)

        @pl.when(has_down)
        def _():
            for kind in kinds:
                fwd_copies[kind][0].start()

        wait_from(kinds, 0)

        @pl.when(has_up)
        def _():
            for kind in kinds:
                fwd_copies[kind][1].start()

        def rest(source, carry):
            wait_from(kinds, source)
            return carry

        lax.fori_loop(1, gy - 1, rest, 0)

    def passed_on(kinds):
        @pl.when(has_up)
        def _():
            for kind in kinds:
                fwd_copies[kind][0].wait_recv()

        @pl.when(has_down)
        def _():
            for kind in kinds:
                fwd_copies[kind][1].wait_recv()

    pass_on((0, 1))
    lax.fori_loop(1, gy + 1, spread_first, 0)

    @pl.when(has_up)
    def _():
        for copy in rows_down:
            copy.wait_recv()

    @pl.when(has_down)
    def _():
        for copy in rows_up:
            copy.wait_recv()

    low_row = jnp.where(has_up, FINE_OFF - SUB, FINE_OFF)
    high_row = jnp.where(has_down, fine_end + SUB, fine_end)

    def diagonals(step, carry):
        row = pl.multiple_of(SUB * (step + 1), SUB)
        rows = pl.ds(row, SUB)
        inside = (row >= low_row) & (row < high_row)
        for t in range(sh.all_slabs):
            diag = mu[t, rows, :] + 1.0
            valid = (halo_lanes_fine if t == halo else (lane >= 0)) & inside
            fd[t, rows, :] = diag
            fi[t, rows, :] = jnp.where(valid, 1.0 / diag, 0.0)
        return carry

    lax.fori_loop(0, sh.fine_buf // SUB - 2, diagonals, 0)

    passed_on((0, 1))
    spread_first(0, 0)
    spread_first(gy + 1, 0)

    def fine_tile(m, acc, f_in, q_ref, f_out, count, out_off):
        base = FINE_OFF + 16 * m
        upper, lower = pl.ds(base, SUB, stride=2), pl.ds(base + 1, SUB, stride=2)
        above, below = pl.ds(base - 1, SUB, stride=2), pl.ds(base + 2, SUB, stride=2)
        crow = COARSE_OFF + SUB * m
        q_here, q_up, q_down = pl.ds(crow, SUB), pl.ds(crow - 1, SUB), pl.ds(crow + 1, SUB)
        out_upper = pl.ds(base + out_off, SUB, stride=2)
        out_lower = pl.ds(base + 1 + out_off, SUB, stride=2)
        for k in range(3):
            tops = [f_in[k, t, upper, :] for t in range(sh.all_slabs)]
            lows = [f_in[k, t, lower, :] for t in range(sh.all_slabs)]
            top_l, top_r = shifted(tops)
            low_l, low_r = shifted(lows)
            for t in range(count):
                three = 3.0 * q_ref[k, t, q_here, :]
                nb = lows[t] + f_in[k, t, above, :] + top_l[t] + top_r[t]
                nb = nb + (three + q_ref[k, t, q_up, :])
                total = kn[k, t, upper, :] + 0.25 * nb
                res = total - fd[t, upper, :] * tops[t]
                f_out[k, t, out_upper, :] = total * fi[t, upper, :]
                nb2 = tops[t] + f_in[k, t, below, :] + low_l[t] + low_r[t]
                nb2 = nb2 + (three + q_ref[k, t, q_down, :])
                total2 = kn[k, t, lower, :] + 0.25 * nb2
                res2 = total2 - fd[t, lower, :] * lows[t]
                f_out[k, t, out_lower, :] = total2 * fi[t, lower, :]
                if acc is not None and t < slabs:
                    acc = acc + (res * res + res2 * res2)
        return acc

    def coarse_sum(m, k, t, f_in, c_ref, w_ref):
        base = FINE_OFF + 16 * m
        crow = COARSE_OFF + SUB * m
        pairs = f_in[k, t, pl.ds(base, SUB, stride=2), :]
        pairs = pairs + f_in[k, t, pl.ds(base + 1, SUB, stride=2), :]
        swap = jnp.where(even, pltpu.roll(pairs, LANES - 1, 1), pltpu.roll(pairs, 1, 1))
        nb = c_ref[k, t, pl.ds(crow - 1, SUB), :] + c_ref[k, t, pl.ds(crow + 1, SUB), :]
        nb = nb + w_ref[k, t, pl.ds(coarse_row(m), SUB), :]
        return 0.25 * (nb + 0.5 * (pairs + swap))

    def coarse_step(m, k, t, acc, added, c_ref):
        rows = pl.ds(coarse_row(m), SUB)
        total = ck[k, t, rows, :] + added
        res = total - cd[t, rows, :] * c_ref[k, t, rows, :]
        if acc is not None and t < slabs:
            acc = acc + res * res
        return total * ci[t, rows, :], acc

    def first_sum(m, carry):
        rows = pl.ds(coarse_row(m), SUB)
        for k in range(3):
            for t in range(sh.all_slabs):
                pre[k, t, rows, :] = coarse_sum(m, k, t, f_a, c_a, w_a)
        return carry

    def first_coarse(m, acc):
        rows = pl.ds(coarse_row(m), SUB)
        for k in range(3):
            values = []
            for t in range(sh.all_slabs):
                value, acc = coarse_step(m, k, t, acc, pre[k, t, rows, :], c_a)
                values.append(value)
            produce(k, coarse_row(m), values, c_b, q_b, w_b)
        return acc

    def second_coarse(m, acc):
        for k in range(3):
            values = []
            for t in range(sh.all_slabs):
                added = coarse_sum(m, k, t, f_b, c_b, w_b)
                value, acc = coarse_step(m, k, t, acc, added, c_b)
                values.append(value)
            produce(k, coarse_row(m), values, c_a, q_a, w_a)
        return acc

    gather_low = jnp.where(lane < 64, 2 * lane, 0)
    gather_high = jnp.where(lane < 64, 0, 2 * lane - LANES)

    def third_coarse(m, acc):
        for k in range(3):
            values = []
            for t in range(slabs):
                added = coarse_sum(m, k, t, f_a, c_a, w_a)
                value, acc = coarse_step(m, k, t, acc, added, c_a)
                values.append(value)
            for u in range(wide // LANES):
                narrow = jnp.where(
                    lane < 64, take(values[2 * u], gather_low), take(values[2 * u + 1], gather_high)
                )
                fin[m, k, :, pl.ds(LANES * u, LANES)] = narrow
        return acc

    def every_tile(body, acc):
        acc = lax.fori_loop(0, tiles, body, acc)
        body(-1, None)
        body(tiles, None)
        return acc

    def fine_first(m, acc):
        return fine_tile(m, acc, f_a, q_a, f_b, sh.all_slabs, 0)

    def fine_second(m, acc):
        return fine_tile(m, acc, f_b, q_b, f_a, sh.all_slabs, 0)

    def fine_third(m, acc):
        return fine_tile(m, acc, f_a, q_a, f_b, slabs, 0)

    fine_sum1 = every_tile(fine_first, zero)
    every_tile(first_sum, 0)

    pass_on((2,))
    lax.fori_loop(1, gy + 1, spread_second, 0)
    passed_on((2,))
    spread_second(0, 0)
    spread_second(gy + 1, 0)

    coarse_sum1 = every_tile(first_coarse, zero)

    @pl.when(has_down)
    def _():
        for copy in rows_down:
            copy.wait_send()

    @pl.when(has_up)
    def _():
        for copy in rows_up:
            copy.wait_send()

    fine_sum2 = every_tile(fine_second, zero)
    coarse_sum2 = every_tile(second_coarse, zero)
    coarse_sum3 = lax.fori_loop(0, tiles, third_coarse, zero)

    my_cols = pl.ds(pl.multiple_of(j * wide, LANES), wide)
    finals = []
    for step in order:
        to = lax.rem(j + step, gy)
        copy = remote(
            fin.at[to],
            coarse_out.at[:, :, my_cols],
            fin_send.at[step],
            fin_recv.at[step],
            i,
            to,
        )
        copy.start()
        finals.append(copy)
    own_final = pltpu.make_async_copy(fin.at[j], coarse_out.at[:, :, my_cols], out_sem.at[slabs])
    own_final.start()

    fine_sum3 = lax.fori_loop(0, tiles, fine_third, zero)
    fine_stores = []
    for t in range(slabs):
        copy = pltpu.make_async_copy(
            f_b.at[:, t, rows_in, :],
            fine_out.at[:, :, pl.ds(LANES * t, LANES)],
            out_sem.at[t],
        )
        copy.start()
        fine_stores.append(copy)

    row_of = lax.broadcasted_iota(jnp.int32, (SUB, LANES), 0)
    mine = zero
    sums = ((fine_sum1, coarse_sum1), (fine_sum2, coarse_sum2), (fine_sum3, coarse_sum3))
    for s, (fine_part, coarse_part) in enumerate(sums):
        line = jnp.sum(fine_part + 0.5 * coarse_part, axis=0, keepdims=True)
        mine = jnp.where(row_of == s, line, mine)
    part[0] = mine
    norm_y = []
    for step in order:
        copy = remote(
            part.at[0],
            part_gy.at[step],
            norm_send.at[0, step],
            norm_recv_y.at[step],
            i,
            lax.rem(j + step, gy),
        )
        copy.start()
        norm_y.append(copy)
    for copy in norm_y:
        copy.wait_recv()
    for step in order:
        mine = mine + part_gy[step]
    part[1] = mine
    norm_x = []
    for step in range(1, gx):
        copy = remote(
            part.at[1],
            part_gx.at[step],
            norm_send.at[1, step],
            norm_recv_x.at[step],
            lax.rem(i + step, gx),
            j,
        )
        copy.start()
        norm_x.append(copy)
    for copy in norm_x:
        copy.wait_recv()
    for step in range(1, gx):
        mine = mine + part_gx[step]
    norms = jnp.sqrt(jnp.sum(mine, axis=1, keepdims=True) * (1.0 / sh.cells))
    for s in range(SWEEPS):
        norm_out[s] = norms[s, 0]

    @pl.when(has_right)
    def _():
        edge_right.wait_send()

    @pl.when(has_left)
    def _():
        edge_left.wait_send()

    @pl.when(has_down)
    def _():
        for kind in range(3):
            fwd_copies[kind][0].wait_send()

    @pl.when(has_up)
    def _():
        for kind in range(3):
            fwd_copies[kind][1].wait_send()

    for step in order:
        for copy in firsts[step]:
            copy.wait_send()
        seconds[step].wait_send()
    for copy in finals:
        copy.wait()
    own_final.wait()
    for copy in fine_stores:
        copy.wait()
    for copy in norm_y + norm_x:
        copy.wait_send()


def solution(mesh):
    gx, gy = mesh.shape["gx"], mesh.shape["gy"]

    def on_device(fine_start, fine_known, fine_mu, coarse_start, coarse_known, coarse_mu):
        sh = Shape(gx, gy, *fine_mu.shape)
        fine = pltpu.VMEM((3, sh.all_slabs, sh.fine_buf, LANES), F32)
        fine_one = pltpu.VMEM((sh.all_slabs, sh.fine_buf, LANES), F32)
        coarse = pltpu.VMEM((3, sh.all_slabs, sh.coarse_buf, LANES), F32)
        coarse_one = pltpu.VMEM((sh.all_slabs, sh.coarse_buf, LANES), F32)
        dma = pltpu.SemaphoreType.DMA
        anywhere = pl.BlockSpec(memory_space=pl.ANY)
        return pl.pallas_call(
            functools.partial(kernel, sh),
            out_shape=(
                jax.ShapeDtypeStruct(fine_start.shape, F32),
                jax.ShapeDtypeStruct(coarse_start.shape, F32),
                jax.ShapeDtypeStruct((SWEEPS,), F32),
            ),
            in_specs=[anywhere] * 6,
            out_specs=(anywhere, anywhere, pl.BlockSpec(memory_space=pltpu.SMEM)),
            scratch_shapes=[
                fine,
                fine,
                fine,
                fine_one,
                fine_one,
                fine_one,
                coarse,
                coarse,
                coarse,
                coarse,
                coarse,
                coarse,
                coarse,
                coarse_one,
                coarse_one,
                coarse,
                pltpu.VMEM((7, SUB, gy * sh.wide), F32),
                pltpu.VMEM((gy, SUB, LANES), F32),
                pltpu.VMEM((gy + 2, 3, SUB, sh.wide), F32),
                pltpu.VMEM((gy + 2, SUB, LANES), F32),
                pltpu.VMEM((gy + 2, 4, SUB, sh.wide), F32),
                pltpu.VMEM((2, 7, SUB, LANES), F32),
                pltpu.VMEM((2, 7, SUB, LANES), F32),
                pltpu.VMEM((gy, 3, SUB, sh.wide), F32),
                pltpu.VMEM((2, SUB, LANES), F32),
                pltpu.VMEM((gy, SUB, LANES), F32),
                pltpu.VMEM((gx, SUB, LANES), F32),
                dma((3 + 3 * sh.slabs,)),
                dma((2,)),
                dma((2,)),
                dma((2, 3)),
                dma((2, 3)),
                dma((3, gy)),
                dma((3, gy)),
                dma((2, 3)),
                dma((2, 3)),
                dma((gy,)),
                dma((gy,)),
                dma((sh.slabs + 1,)),
                dma((2, max(gx, gy))),
                dma((gy,)),
                dma((gx,)),
            ],
            compiler_params=pltpu.CompilerParams(
                collective_id=0, has_side_effects=True, vmem_limit_bytes=62_000_000
            ),
            name="interface_sweeps",
        )(fine_start, fine_known, fine_mu, coarse_start, coarse_known, coarse_mu)

    return jax.shard_map(
        on_device,
        mesh=mesh,
        in_specs=(
            P(None, "gx", "gy"),
            P(None, "gx", "gy"),
            P("gx", "gy"),
            P(None, ("gx", "gy"), None),
            P(None, ("gx", "gy"), None),
            P(("gx", "gy"), None),
        ),
        out_specs=(P(None, "gx", "gy"), P(None, ("gx", "gy"), None), P(None)),
        check_vma=False,
    )
```

```python
import functools

import jax
import jax.numpy as jnp
from jax import lax
from jax.experimental import pallas as pl
from jax.experimental.pallas import tpu as pltpu
from jax.sharding import PartitionSpec as P

MESH = pl.DeviceIdType.MESH
F32 = jnp.float32
BF16 = jnp.bfloat16
SWEEPS = 3
LANES = 128
SUB = 8
FINE_OFF = 24
COARSE_OFF = 16
EDGE = 4
PLANES = 7


class Shape:
    def __init__(self, gx, gy, fine_rows, fine_cols):
        self.gx, self.gy = gx, gy
        self.fine_rows, self.fine_cols = fine_rows, fine_cols
        self.coarse_rows, self.wide = fine_rows // 2, fine_cols // 2
        self.tiles = self.coarse_rows // SUB
        self.halves = self.wide // LANES
        self.slabs = 2 * self.halves
        self.fine_buf = fine_rows + 2 * FINE_OFF
        self.coarse_buf = self.coarse_rows + 2 * COARSE_OFF
        self.blocks = fine_rows // LANES
        self.cells = 3.0 * gx * gy * fine_rows * fine_cols * 1.25


def lane_iota():
    return lax.broadcasted_iota(jnp.int32, (SUB, LANES), 1)


def exact_dot(values, table):
    high = values.astype(BF16)
    rest = values - high.astype(F32)
    middle = rest.astype(BF16)
    low = (rest - middle.astype(F32)).astype(BF16)
    total = jnp.dot(high, table, preferred_element_type=F32)
    total = total + jnp.dot(middle, table, preferred_element_type=F32)
    return total + jnp.dot(low, table, preferred_element_type=F32)


def kernel(
    sh,
    fine_start,
    fine_known,
    fine_mu,
    coarse_start,
    coarse_known,
    coarse_mu,
    fine_out,
    coarse_out,
    norm_out,
    nat,
    turned,
    swapped,
    f_a,
    f_b,
    fd,
    fi,
    c_a,
    c_b,
    q_a,
    q_b,
    w_a,
    w_b,
    ckh,
    cd,
    ci,
    pre,
    own,
    comb,
    pack,
    got_c,
    got_p,
    got_k,
    edge_out,
    edge_in,
    fin,
    part,
    part_gy,
    part_gx,
    load_sem,
    edge_send,
    edge_recv,
    row_send,
    row_recv,
    a_send,
    a_recv,
    fwd_send,
    fwd_recv,
    fin_send,
    fin_recv,
    norm_send,
    norm_recv_y,
    norm_recv_x,
):
    gx, gy = sh.gx, sh.gy
    i = lax.axis_index("gx")
    j = lax.axis_index("gy")
    halves, slabs, tiles, wide = sh.halves, sh.slabs, sh.tiles, sh.wide
    halo, coarse_halo = slabs, halves
    lane = lane_iota()
    even = lane % 2 == 0
    first = lane == 0
    last = lane == LANES - 1
    has_up, has_down = i > 0, i < gx - 1
    has_left, has_right = j > 0, j < gy - 1

    def remote(src, dst, send, recv, to_i, to_j):
        return pltpu.make_async_remote_copy(
            src_ref=src,
            dst_ref=dst,
            send_sem=send,
            recv_sem=recv,
            device_id=(to_i, to_j),
            device_id_type=MESH,
        )

    loads = []

    def load(src, dst):
        copy = pltpu.make_async_copy(src, dst, load_sem.at[len(loads)])
        copy.start()
        loads.append(copy)
        return copy

    own_loads = [
        load(coarse_start, own.at[pl.ds(0, 3)]),
        load(coarse_known, own.at[pl.ds(3, 3)]),
        load(coarse_mu, own.at[6]),
    ]
    fine_loads = []
    for t in [0, slabs - 1] + list(range(1, slabs - 1)):
        cols = pl.ds(LANES * t, LANES)
        fine_loads.append(load(fine_start.at[:, :, cols], nat.at[pl.ds(0, 3), t]))
        fine_loads.append(load(fine_known.at[:, :, cols], nat.at[pl.ds(3, 3), t]))
        fine_loads.append(load(fine_mu.at[:, cols], nat.at[6, t]))

    zero = jnp.zeros((SUB, LANES), F32)
    fine_end = FINE_OFF + sh.fine_rows

    def zero_fine(step, carry):
        for row in (0, 8, 16, fine_end, fine_end + 8, fine_end + 16):
            rows = pl.ds(row, SUB)
            for p in range(PLANES):
                f_a[p, step, rows, :] = zero
            for k in range(3):
                f_b[k, step, rows, :] = zero
        for row in (0, 8, sh.coarse_buf - 16, sh.coarse_buf - 8):
            rows = pl.ds(row, SUB)
            for k in range(3):
                q_a[k, step, rows, :] = zero
                q_b[k, step, rows, :] = zero
        return carry

    lax.fori_loop(0, slabs + 1, zero_fine, 0)
    for t in range(halves + 1):
        for row in (0, 8, sh.coarse_buf - 16, sh.coarse_buf - 8):
            rows = pl.ds(row, SUB)
            for k in range(3):
                c_a[k, t, rows, :] = zero
                c_b[k, t, rows, :] = zero
    for side in range(2):
        for p in range(PLANES):
            edge_in[side, p] = zero
    for slot in (0, gy + 1):
        got_p[slot] = zero
        for u in range(halves):
            cols = pl.ds(LANES * u, LANES)
            for p in range(3):
                got_c[slot, p, :, cols] = zero
            for p in range(4):
                got_k[slot, p, :, cols] = zero

    barrier = pltpu.get_barrier_semaphore()
    for step in range(1, gy):
        pl.semaphore_signal(
            barrier, inc=1, device_id=(i, lax.rem(j + step, gy)), device_id_type=MESH
        )
    for step in range(1, gx):
        pl.semaphore_signal(
            barrier, inc=1, device_id=(lax.rem(i + step, gx), j), device_id_type=MESH
        )

    for copy in own_loads:
        copy.wait()

    for dest in range(gy):
        for p in range(PLANES):
            after = own[p, :, pl.ds((dest + 1) * wide, LANES)] if dest < gy - 1 else zero
            before = own[p, :, pl.ds(dest * wide - LANES, LANES)] if dest > 0 else zero
            comb[p, pl.ds(SUB * dest, SUB), :] = jnp.where(lane < 64, after, before)
    source = lax.broadcasted_iota(jnp.int32, (LANES, LANES), 0)
    target = lax.broadcasted_iota(jnp.int32, (LANES, LANES), 1)
    inside = target % 16
    wanted = jnp.where(inside < 8, LANES - EDGE + inside // 2, (inside - 8) // 2)
    packed = None
    for p in range(PLANES):
        table = ((source == wanted) & (target // 16 == p)).astype(F32).astype(BF16)
        piece = exact_dot(comb[p], table)
        packed = piece if packed is None else packed + piece
    for dest in range(gy):
        pack[dest] = packed[SUB * dest : SUB * (dest + 1), :]

    for copy in fine_loads:
        copy.wait()

    def turn_edges(p, carry):
        for b in range(sh.blocks):
            rows = pl.ds(LANES * b, LANES)
            low = nat[p, 0, rows, :].T
            high = nat[p, slabs - 1, rows, :].T
            turned[p, b, pl.ds(0, LANES), :] = low
            turned[p, b, pl.ds(LANES * (slabs - 1), LANES), :] = high
            edge_out[0, p, pl.ds(EDGE * b, EDGE), :] = high[LANES - EDGE :, :]
            edge_out[1, p, pl.ds(EDGE * b, EDGE), :] = low[:EDGE, :]
        return carry

    lax.fori_loop(0, PLANES, turn_edges, 0, unroll=PLANES)

    pl.semaphore_wait(barrier, gy + gx - 2)

    edge_right = remote(
        edge_out.at[0], edge_in.at[0], edge_send.at[0], edge_recv.at[0], i, lax.rem(j + 1, gy)
    )
    edge_left = remote(
        edge_out.at[1], edge_in.at[1], edge_send.at[1], edge_recv.at[1], i, lax.rem(j + gy - 1, gy)
    )

    @pl.when(has_right)
    def _():
        edge_right.start()

    @pl.when(has_left)
    def _():
        edge_left.start()

    def sends_of(step):
        to = lax.rem(j + step, gy)
        cols = pl.ds(pl.multiple_of(to * wide, LANES), wide)
        ends = (
            (own.at[pl.ds(0, 3), :, cols], got_c),
            (pack.at[to], got_p),
            (own.at[pl.ds(3, 4), :, cols], got_k),
        )
        return [
            remote(src, dst.at[j + 1], a_send.at[n, step], a_recv.at[n, step], i, to)
            for n, (src, dst) in enumerate(ends)
        ]

    order = list(range(1, gy))
    sends = {step: sends_of(step) for step in order}
    for step in order:
        sends[step][0].start()
        sends[step][1].start()
    for step in order:
        sends[step][2].start()

    got_p[j + 1] = pack[j]
    for u in range(halves):
        cols = pl.ds(pl.multiple_of(j * wide + LANES * u, LANES), LANES)
        for p in range(PLANES):
            piece = own[p, :, cols]
            if p < 3:
                got_c[j + 1, p, :, pl.ds(LANES * u, LANES)] = piece
            else:
                got_k[j + 1, p - 3, :, pl.ds(LANES * u, LANES)] = piece

    def split_columns(p, carry):
        for b in range(sh.blocks):
            rows = pl.ds(LANES * b, LANES)
            for t in range(1, slabs - 1):
                turned[p, b, pl.ds(LANES * t, LANES), :] = nat[p, t, rows, :].T
        for b in range(sh.blocks):
            rows = pl.ds(FINE_OFF + LANES * b, LANES)
            for s in range(slabs):
                begin = 2 * LANES * (s // 2) + s % 2
                f_a[p, s, rows, :] = turned[p, b, pl.ds(begin, LANES, stride=2), :].T
        return carry

    lax.fori_loop(0, PLANES, split_columns, 0)

    @pl.when(has_left)
    def _():
        edge_right.wait_recv()

    @pl.when(has_right)
    def _():
        edge_left.wait_recv()

    between = jnp.zeros((LANES - 2 * EDGE, LANES), F32)

    def unpack_edges(p, carry):
        for b in range(sh.blocks):
            from_left = edge_in[0, p, pl.ds(EDGE * b, EDGE), :]
            from_right = edge_in[1, p, pl.ds(EDGE * b, EDGE), :]
            slab = jnp.concatenate([from_right, between, from_left], axis=0).T
            f_a[p, halo, pl.ds(FINE_OFF + LANES * b, LANES), :] = slab
        return carry

    lax.fori_loop(0, PLANES, unpack_edges, 0, unroll=PLANES)

    down_i, up_i = lax.rem(i + 1, gx), lax.rem(i + gx - 1, gx)
    row_down = remote(
        f_a.at[:, :, pl.ds(fine_end - SUB, SUB), :],
        f_a.at[:, :, pl.ds(FINE_OFF - SUB, SUB), :],
        row_send.at[0],
        row_recv.at[0],
        down_i,
        j,
    )
    row_up = remote(
        f_a.at[:, :, pl.ds(FINE_OFF, SUB), :],
        f_a.at[:, :, pl.ds(fine_end, SUB), :],
        row_send.at[1],
        row_recv.at[1],
        up_i,
        j,
    )

    @pl.when(has_down)
    def _():
        row_down.start()

    @pl.when(has_up)
    def _():
        row_up.start()

    def coarse_row(m):
        return pl.multiple_of(COARSE_OFF + SUB * m, SUB)

    def halo_of(slot, p):
        return pltpu.roll(got_p[slot], (LANES - (16 * p + 8)) % LANES, 1)

    def swapped_pairs(value):
        return jnp.where(even, pltpu.roll(value, LANES - 1, 1), pltpu.roll(value, 1, 1))

    def produce(k, row, values, c_ref, q_ref, w_ref):
        right = [pltpu.roll(v, 1, 1) for v in values]
        left = [pltpu.roll(v, LANES - 1, 1) for v in values]
        rows = pl.ds(row, SUB)
        count = len(values)
        for t, value in enumerate(values):
            before = jnp.where(first, right[t - 1], right[t])
            after = jnp.where(last, left[(t + 1) % count], left[t])
            c_ref[k, t, rows, :] = value
            main = 0.375 * value
            if t == coarse_halo:
                outer = jnp.where(even, before, after)
                q_ref[k, halo, rows, :] = main + 0.125 * outer
                w_ref[k, t, rows, :] = outer + swapped_pairs(outer)
            else:
                q_ref[k, 2 * t, rows, :] = main + 0.125 * before
                q_ref[k, 2 * t + 1, rows, :] = main + 0.125 * after
                w_ref[k, t, rows, :] = before + after

    def spread_first(slot, carry):
        for k in range(3):
            values = [got_c[slot, k, :, pl.ds(LANES * t, LANES)] for t in range(halves)]
            values.append(halo_of(slot, k))
            produce(k, coarse_row(slot - 1), values, c_a, q_a, w_a)
        return carry

    halo_lanes = ((lane < 2 * EDGE) & has_right) | ((lane >= LANES - 2 * EDGE) & has_left)
    halo_lanes_fine = ((lane < EDGE) & has_right) | ((lane >= LANES - EDGE) & has_left)

    def spread_second(slot, carry):
        rows = pl.ds(coarse_row(slot - 1), SUB)
        held = ((slot > 0) | has_up) & ((slot <= gy) | has_down)
        for k in range(3):
            ckh[k, rows, :] = halo_of(slot, 3 + k)
        for t in range(halves + 1):
            if t == coarse_halo:
                value, valid = halo_of(slot, 6), halo_lanes & held
            else:
                value, valid = got_k[slot, 3, :, pl.ds(LANES * t, LANES)], (lane >= 0) & held
            diag = value + 1.0
            cd[t, rows, :] = diag
            ci[t, rows, :] = jnp.where(valid, 1.0 / diag, 0.0)
        return carry

    fwd_copies = {}
    for n, ref in enumerate((got_c, got_p, got_k)):
        fwd_copies[n] = (
            remote(ref.at[gy], ref.at[0], fwd_send.at[0, n], fwd_recv.at[0, n], down_i, j),
            remote(ref.at[1], ref.at[gy + 1], fwd_send.at[1, n], fwd_recv.at[1, n], up_i, j),
        )

    def wait_from(kinds, source):
        step = lax.rem(j - source + gy, gy)

        @pl.when(step > 0)
        def _():
            for kind in kinds:
                dst = (got_c, got_p, got_k)[kind].at[source + 1]
                remote(dst, dst, a_send.at[kind, step], a_recv.at[kind, step], i, source).wait_recv()

    def pass_on(kinds):
        wait_from(kinds, gy - 1)

        @pl.when(has_down)
        def _():
            for kind in kinds:
                fwd_copies[kind][0].start()

        wait_from(kinds, 0)

        @pl.when(has_up)
        def _():
            for kind in kinds:
                fwd_copies[kind][1].start()

        def rest(source, carry):
            wait_from(kinds, source)
            return carry

        lax.fori_loop(1, gy - 1, rest, 0)

    def passed_on(kinds):
        @pl.when(has_up)
        def _():
            for kind in kinds:
                fwd_copies[kind][0].wait_recv()

        @pl.when(has_down)
        def _():
            for kind in kinds:
                fwd_copies[kind][1].wait_recv()

    def diagonal(row, held):
        rows = pl.ds(row, SUB)
        for t in range(slabs + 1):
            diag = f_a[6, t, rows, :] + 1.0
            valid = (halo_lanes_fine if t == halo else (lane >= 0)) & held
            fd[t, rows, :] = diag
            fi[t, rows, :] = jnp.where(valid, 1.0 / diag, 0.0)

    def diagonals(step, carry):
        for n in range(4):
            diagonal(pl.multiple_of(FINE_OFF + SUB * (4 * step + n), SUB), lane >= 0)
        return carry

    lax.fori_loop(0, sh.fine_rows // (4 * SUB), diagonals, 0)

    pass_on((0, 1))
    lax.fori_loop(1, gy + 1, spread_first, 0, unroll=8)

    @pl.when(has_up)
    def _():
        row_down.wait_recv()

    @pl.when(has_down)
    def _():
        row_up.wait_recv()

    for row, held in (
        (FINE_OFF - 16, lane < 0),
        (FINE_OFF - 8, (lane >= 0) & has_up),
        (fine_end, (lane >= 0) & has_down),
        (fine_end + 8, lane < 0),
    ):
        diagonal(row, held)

    passed_on((0, 1))
    lax.fori_loop(0, 2, lambda e, c: spread_first((gy + 1) * e, c), 0, unroll=2)

    def beside(values):
        side = values[halo]
        odd_right = [pltpu.roll(values[2 * h + 1], 1, 1) for h in range(halves)]
        even_left = [pltpu.roll(values[2 * h], LANES - 1, 1) for h in range(halves)]
        side_right, side_left = pltpu.roll(side, 1, 1), pltpu.roll(side, LANES - 1, 1)
        sums = []
        for h in range(halves):
            before = odd_right[h - 1] if h > 0 else side_right
            after = even_left[h + 1] if h < halves - 1 else side_left
            sums.append(jnp.where(first, before, odd_right[h]) + values[2 * h + 1])
            sums.append(values[2 * h] + jnp.where(last, after, even_left[h]))
        sums.append(
            jnp.where(first, odd_right[-1], side_right) + jnp.where(last, even_left[0], side_left)
        )
        return sums

    def fine_tile(m, acc, f_in, q_ref, f_out, count):
        base = FINE_OFF + 16 * m
        upper, lower = pl.ds(base, SUB, stride=2), pl.ds(base + 1, SUB, stride=2)
        above, below = pl.ds(base - 1, SUB, stride=2), pl.ds(base + 2, SUB, stride=2)
        crow = COARSE_OFF + SUB * m
        q_here, q_up, q_down = pl.ds(crow, SUB), pl.ds(crow - 1, SUB), pl.ds(crow + 1, SUB)
        for k in range(3):
            tops = [f_in[k, t, upper, :] for t in range(slabs + 1)]
            lows = [f_in[k, t, lower, :] for t in range(slabs + 1)]
            top_sum, low_sum = beside(tops), beside(lows)
            for t in range(count):
                three = 3.0 * q_ref[k, t, q_here, :]
                nb = (lows[t] + f_in[k, t, above, :]) + (top_sum[t] + q_ref[k, t, q_up, :])
                total = f_a[3 + k, t, upper, :] + 0.25 * (nb + three)
                res = total - fd[t, upper, :] * tops[t]
                f_out[k, t, upper, :] = total * fi[t, upper, :]
                nb2 = (tops[t] + f_in[k, t, below, :]) + (low_sum[t] + q_ref[k, t, q_down, :])
                total2 = f_a[3 + k, t, lower, :] + 0.25 * (nb2 + three)
                res2 = total2 - fd[t, lower, :] * lows[t]
                f_out[k, t, lower, :] = total2 * fi[t, lower, :]
                if acc is not None and t < slabs:
                    acc = acc + (res * res + res2 * res2)
        return acc

    def coarse_sum(m, k, t, f_in, c_ref, w_ref):
        base = FINE_OFF + 16 * m
        crow = COARSE_OFF + SUB * m
        upper, lower = pl.ds(base, SUB, stride=2), pl.ds(base + 1, SUB, stride=2)
        if t == coarse_halo:
            four = f_in[k, halo, upper, :] + f_in[k, halo, lower, :]
            four = four + swapped_pairs(four)
        else:
            four = (f_in[k, 2 * t, upper, :] + f_in[k, 2 * t, lower, :]) + (
                f_in[k, 2 * t + 1, upper, :] + f_in[k, 2 * t + 1, lower, :]
            )
        nb = c_ref[k, t, pl.ds(crow - 1, SUB), :] + c_ref[k, t, pl.ds(crow + 1, SUB), :]
        nb = nb + w_ref[k, t, pl.ds(coarse_row(m), SUB), :]
        return 0.25 * (nb + 0.5 * four)

    def coarse_step(m, k, t, acc, added, c_ref):
        rows = pl.ds(coarse_row(m), SUB)
        if t == coarse_halo:
            known = ckh[k, rows, :]
        else:
            known = got_k[m + 1, k, :, pl.ds(LANES * t, LANES)]
        total = known + added
        if acc is not None and t < halves:
            res = total - cd[t, rows, :] * c_ref[k, t, rows, :]
            acc = acc + res * res
        return total * ci[t, rows, :], acc

    def first_sum(m, carry):
        rows = pl.ds(coarse_row(m), SUB)
        for k in range(3):
            for t in range(halves + 1):
                pre[k, t, rows, :] = coarse_sum(m, k, t, f_a, c_a, w_a)
        return zero

    def first_coarse(m, acc):
        rows = pl.ds(coarse_row(m), SUB)
        for k in range(3):
            values = []
            for t in range(halves + 1):
                value, acc = coarse_step(m, k, t, acc, pre[k, t, rows, :], c_a)
                values.append(value)
            produce(k, coarse_row(m), values, c_b, q_b, w_b)
        return acc

    def second_coarse(m, acc):
        for k in range(3):
            values = []
            for t in range(halves + 1):
                added = coarse_sum(m, k, t, f_b, c_b, w_b)
                value, acc = coarse_step(m, k, t, acc, added, c_b)
                values.append(value)
            produce(k, coarse_row(m), values, c_a, q_a, w_a)
        return acc

    def third_coarse(m, acc):
        for k in range(3):
            for t in range(halves):
                added = coarse_sum(m, k, t, f_a, c_a, w_a)
                value, acc = coarse_step(m, k, t, acc, added, c_a)
                fin[m, k, :, pl.ds(LANES * t, LANES)] = value
        return acc

    def every_tile(body, acc, unroll=6):
        def step(n, acc):
            m = n - 1
            part_sum = body(m, zero)
            inner = jnp.where((n > 0) & (n <= tiles), 1.0, 0.0).astype(F32)
            return acc + part_sum * inner

        return lax.fori_loop(0, tiles + 2, step, acc, unroll=unroll)

    def fine_first(m, acc):
        return fine_tile(m, acc, f_a, q_a, f_b, slabs + 1)

    def fine_second(m, acc):
        return fine_tile(m, acc, f_b, q_b, f_a, slabs + 1)

    def fine_third(m, acc):
        return fine_tile(m, acc, f_a, q_a, f_b, slabs)

    fine_sum1 = every_tile(fine_first, zero)
    every_tile(first_sum, zero)

    pass_on((2,))
    lax.fori_loop(1, gy + 1, spread_second, 0, unroll=8)
    passed_on((2,))
    lax.fori_loop(0, 2, lambda e, c: spread_second((gy + 1) * e, c), 0, unroll=2)

    coarse_sum1 = every_tile(first_coarse, zero)

    @pl.when(has_down)
    def _():
        row_down.wait_send()

    @pl.when(has_up)
    def _():
        row_up.wait_send()

    fine_sum2 = every_tile(fine_second, zero)
    coarse_sum2 = every_tile(second_coarse, zero)
    coarse_sum3 = lax.fori_loop(0, tiles, third_coarse, zero, unroll=4)

    my_cols = pl.ds(pl.multiple_of(j * wide, LANES), wide)
    finals = []
    for step in order:
        to = lax.rem(j + step, gy)
        copy = remote(
            fin.at[to], coarse_out.at[:, :, my_cols], fin_send.at[step], fin_recv.at[step], i, to
        )
        copy.start()
        finals.append(copy)
    for k in range(3):
        for t in range(halves):
            cols = pl.ds(pl.multiple_of(j * wide + LANES * t, LANES), LANES)
            coarse_out[k, :, cols] = fin[j, k, :, pl.ds(LANES * t, LANES)]

    fine_sum3 = lax.fori_loop(0, tiles, fine_third, zero, unroll=8)

    row_of = lax.broadcasted_iota(jnp.int32, (SUB, LANES), 0)
    mine = zero
    sums = ((fine_sum1, coarse_sum1), (fine_sum2, coarse_sum2), (fine_sum3, coarse_sum3))
    for s, (fine_part, coarse_part) in enumerate(sums):
        line = jnp.sum(fine_part + coarse_part, axis=0, keepdims=True)
        mine = jnp.where(row_of == s, line, mine)
    part[0] = mine
    norm_x = []
    for step in range(1, gx):
        copy = remote(
            part.at[0],
            part_gx.at[step],
            norm_send.at[0, step],
            norm_recv_x.at[step],
            lax.rem(i + step, gx),
            j,
        )
        copy.start()
        norm_x.append(copy)

    def join_columns(k, carry):
        for b in range(sh.blocks):
            rows = pl.ds(FINE_OFF + LANES * b, LANES)
            for s in range(slabs):
                begin = 2 * LANES * (s // 2) + s % 2
                swapped[b, pl.ds(begin, LANES, stride=2), :] = f_b[k, s, rows, :].T
            for t in range(slabs):
                natural = swapped[b, pl.ds(LANES * t, LANES), :].T
                fine_out[k, pl.ds(LANES * b, LANES), pl.ds(LANES * t, LANES)] = natural
        return carry

    lax.fori_loop(0, 3, join_columns, 0)

    for copy in norm_x:
        copy.wait_recv()
    for step in range(1, gx):
        mine = mine + part_gx[step]
    part[1] = mine
    norm_y = []
    for step in order:
        copy = remote(
            part.at[1],
            part_gy.at[step],
            norm_send.at[1, step],
            norm_recv_y.at[step],
            i,
            lax.rem(j + step, gy),
        )
        copy.start()
        norm_y.append(copy)
    for copy in norm_y:
        copy.wait_recv()
    for step in order:
        mine = mine + part_gy[step]
    total = jnp.sum(mine, axis=1, keepdims=True) * (1.0 / sh.cells)
    norms = jnp.sqrt(total)
    for s in range(SWEEPS):
        norm_out[s] = norms[s, 0]

    @pl.when(has_right)
    def _():
        edge_right.wait_send()

    @pl.when(has_left)
    def _():
        edge_left.wait_send()

    @pl.when(has_down)
    def _():
        for kind in range(3):
            fwd_copies[kind][0].wait_send()

    @pl.when(has_up)
    def _():
        for kind in range(3):
            fwd_copies[kind][1].wait_send()

    for step in order:
        for copy in sends[step]:
            copy.wait_send()
    for copy in finals:
        copy.wait()
    for copy in norm_y + norm_x:
        copy.wait_send()


def solution(mesh):
    gx, gy = mesh.shape["gx"], mesh.shape["gy"]

    def on_device(fine_start, fine_known, fine_mu, coarse_start, coarse_known, coarse_mu):
        sh = Shape(gx, gy, *fine_mu.shape)
        dma = pltpu.SemaphoreType.DMA
        in_hbm = pl.BlockSpec(memory_space=pltpu.HBM)
        on_chip = pl.BlockSpec(memory_space=pltpu.VMEM)

        def fine(*lead):
            return pltpu.VMEM((*lead, sh.slabs + 1, sh.fine_buf, LANES), F32)

        def coarse(*lead):
            return pltpu.VMEM((*lead, sh.coarse_buf, LANES), F32)

        few = sh.halves + 1
        return pl.pallas_call(
            functools.partial(kernel, sh),
            out_shape=(
                pltpu.VMEM(fine_start.shape, F32),
                pltpu.VMEM(coarse_start.shape, F32),
                jax.ShapeDtypeStruct((SWEEPS,), F32),
            ),
            in_specs=[in_hbm] * 6,
            out_specs=(on_chip, on_chip, pl.BlockSpec(memory_space=pltpu.SMEM)),
            scratch_shapes=[
                pltpu.VMEM((PLANES, sh.slabs, sh.fine_rows, LANES), F32),
                pltpu.VMEM((PLANES, sh.blocks, sh.slabs * LANES, LANES), F32),
                pltpu.VMEM((sh.blocks, sh.slabs * LANES, LANES), F32),
                fine(PLANES),
                fine(3),
                fine(),
                fine(),
                coarse(3, few),
                coarse(3, few),
                coarse(3, sh.slabs + 1),
                coarse(3, sh.slabs + 1),
                coarse(3, few),
                coarse(3, few),
                coarse(3),
                coarse(few),
                coarse(few),
                coarse(3, few),
                pltpu.VMEM((PLANES, SUB, gy * sh.wide), F32),
                pltpu.VMEM((PLANES, gy * SUB, LANES), F32),
                pltpu.VMEM((gy, SUB, LANES), F32),
                pltpu.VMEM((gy + 2, 3, SUB, sh.wide), F32),
                pltpu.VMEM((gy + 2, SUB, LANES), F32),
                pltpu.VMEM((gy + 2, 4, SUB, sh.wide), F32),
                pltpu.VMEM((2, PLANES, SUB, LANES), F32),
                pltpu.VMEM((2, PLANES, SUB, LANES), F32),
                pltpu.VMEM((gy, 3, SUB, sh.wide), F32),
                pltpu.VMEM((2, SUB, LANES), F32),
                pltpu.VMEM((gy, SUB, LANES), F32),
                pltpu.VMEM((gx, SUB, LANES), F32),
                dma((3 + 3 * sh.slabs,)),
                dma((2,)),
                dma((2,)),
                dma((2,)),
                dma((2,)),
                dma((3, gy)),
                dma((3, gy)),
                dma((2, 3)),
                dma((2, 3)),
                dma((gy,)),
                dma((gy,)),
                dma((2, max(gx, gy))),
                dma((gy,)),
                dma((gx,)),
            ],
            compiler_params=pltpu.CompilerParams(
                collective_id=0, has_side_effects=True, vmem_limit_bytes=64_500_000
            ),
            name="interface_sweeps",
        )(fine_start, fine_known, fine_mu, coarse_start, coarse_known, coarse_mu)

    return jax.shard_map(
        on_device,
        mesh=mesh,
        in_specs=(
            P(None, "gx", "gy"),
            P(None, "gx", "gy"),
            P("gx", "gy"),
            P(None, ("gx", "gy"), None),
            P(None, ("gx", "gy"), None),
            P(("gx", "gy"), None),
        ),
        out_specs=(P(None, "gx", "gy"), P(None, ("gx", "gy"), None), P(None)),
        check_vma=False,
    )
```

```python
import functools

import jax
import jax.numpy as jnp
from jax import lax
from jax.experimental import pallas as pl
from jax.experimental.pallas import tpu as pltpu
from jax.sharding import PartitionSpec as P

MESH = pl.DeviceIdType.MESH
F32 = jnp.float32
BF16 = jnp.bfloat16
SWEEPS = 3
LANES = 128
SUB = 8
FINE_OFF = 24
COARSE_OFF = 16
EDGE = 4
PLANES = 7


class Shape:
    def __init__(self, gx, gy, fine_rows, fine_cols):
        self.gx, self.gy = gx, gy
        self.fine_rows, self.fine_cols = fine_rows, fine_cols
        self.coarse_rows, self.wide = fine_rows // 2, fine_cols // 2
        self.tiles = self.coarse_rows // SUB
        self.halves = self.wide // LANES
        self.slabs = 2 * self.halves
        self.fine_buf = fine_rows + 2 * FINE_OFF
        self.coarse_buf = self.coarse_rows + 2 * COARSE_OFF + SUB
        self.blocks = fine_rows // LANES
        self.cells = 3.0 * gx * gy * fine_rows * fine_cols * 1.25


def far_first(count):
    return sorted(range(1, count), key=lambda step: -min(step, count - step))


def lane_iota():
    return lax.broadcasted_iota(jnp.int32, (SUB, LANES), 1)


def exact_dot(values, table):
    high = values.astype(BF16)
    rest = values - high.astype(F32)
    middle = rest.astype(BF16)
    low = (rest - middle.astype(F32)).astype(BF16)
    total = jnp.dot(high, table, preferred_element_type=F32)
    total = total + jnp.dot(middle, table, preferred_element_type=F32)
    return total + jnp.dot(low, table, preferred_element_type=F32)


def kernel(
    sh,
    fine_start,
    fine_known,
    fine_mu,
    coarse_start,
    coarse_known,
    coarse_mu,
    fine_out,
    coarse_out,
    norm_out,
    nat,
    turned,
    swapped,
    f_a,
    f_b,
    fd,
    fi,
    c_a,
    c_b,
    q_a,
    q_b,
    w_a,
    w_b,
    ckh,
    cd,
    ci,
    pre,
    pre_b,
    near,
    own,
    comb,
    pack,
    got_c,
    got_p,
    got_k,
    strip_out,
    strip_in,
    strip_far,
    edge_out,
    edge_in,
    fin,
    part,
    part_gy,
    part_gx,
    load_sem,
    edge_send,
    edge_recv,
    row_send,
    row_recv,
    a_send,
    a_recv,
    fwd_send,
    fwd_recv,
    strip_send,
    strip_recv,
    fin_send,
    fin_recv,
    norm_send,
    norm_recv_y,
    norm_recv_x,
):
    gx, gy = sh.gx, sh.gy
    i = lax.axis_index("gx")
    j = lax.axis_index("gy")
    halves, slabs, tiles, wide = sh.halves, sh.slabs, sh.tiles, sh.wide
    halo, coarse_halo = slabs, halves
    lane = lane_iota()
    even = lane % 2 == 0
    first = lane == 0
    last = lane == LANES - 1
    has_up, has_down = i > 0, i < gx - 1
    has_left, has_right = j > 0, j < gy - 1

    def remote(src, dst, send, recv, to_i, to_j):
        return pltpu.make_async_remote_copy(
            src_ref=src,
            dst_ref=dst,
            send_sem=send,
            recv_sem=recv,
            device_id=(to_i, to_j),
            device_id_type=MESH,
        )

    loads = []

    def load(src, dst):
        copy = pltpu.make_async_copy(src, dst, load_sem.at[len(loads)])
        copy.start()
        loads.append(copy)
        return copy

    own_loads = [
        load(coarse_start, own.at[pl.ds(0, 3)]),
        load(coarse_known, own.at[pl.ds(3, 3)]),
        load(coarse_mu, own.at[6]),
    ]
    fine_loads = []
    for t in [0, slabs - 1] + list(range(1, slabs - 1)):
        cols = pl.ds(LANES * t, LANES)
        fine_loads.append(load(fine_start.at[:, :, cols], nat.at[pl.ds(0, 3), t]))
        fine_loads.append(load(fine_known.at[:, :, cols], nat.at[pl.ds(3, 3), t]))
        fine_loads.append(load(fine_mu.at[:, cols], nat.at[6, t]))

    barrier = pltpu.get_barrier_semaphore()
    for step in far_first(gy):
        pl.semaphore_signal(
            barrier, inc=1, device_id=(i, lax.rem(j + step, gy)), device_id_type=MESH
        )
    for step in far_first(gx):
        pl.semaphore_signal(
            barrier, inc=1, device_id=(lax.rem(i + step, gx), j), device_id_type=MESH
        )

    zero = jnp.zeros((SUB, LANES), F32)
    fine_end = FINE_OFF + sh.fine_rows
    for t in range(slabs + 1):
        for row in (0, 8, fine_end + 8, fine_end + 16):
            for p in range(PLANES):
                f_a[p, t, pl.ds(row, SUB), :] = zero
        for k in range(3):
            for row in (0, fine_end + 16):
                f_b[k, t, pl.ds(row, SUB), :] = zero
            for row in (0, sh.coarse_buf - 8):
                q_a[k, t, pl.ds(row, SUB), :] = zero
                q_b[k, t, pl.ds(row, SUB), :] = zero
                if t <= halves:
                    c_a[k, t, pl.ds(row, SUB), :] = zero
                    c_b[k, t, pl.ds(row, SUB), :] = zero

    for slot in (0, gy + 1):
        for u in range(halves):
            for p in range(4):
                got_k[slot, p, :, pl.ds(LANES * u, LANES)] = zero

    def clear_rows(row, slot):
        for p in range(PLANES):
            for t in range(slabs + 1):
                f_a[p, t, pl.ds(row, SUB), :] = zero
        got_p[slot] = zero
        for u in range(halves):
            for p in range(3):
                got_c[slot, p, :, pl.ds(LANES * u, LANES)] = zero

    def clear_columns(side):
        for p in range(PLANES):
            edge_in[side, p] = zero

    pl.when(i == 0)(lambda: clear_rows(FINE_OFF - SUB, 0))
    pl.when(i == gx - 1)(lambda: clear_rows(fine_end, gy + 1))
    pl.when(j == 0)(lambda: clear_columns(0))
    pl.when(j == gy - 1)(lambda: clear_columns(1))

    for copy in own_loads:
        copy.wait()

    for dest in range(gy):
        for p in range(PLANES):
            after = own[p, :, pl.ds((dest + 1) * wide, LANES)] if dest < gy - 1 else zero
            before = own[p, :, pl.ds(dest * wide - LANES, LANES)] if dest > 0 else zero
            comb[p, pl.ds(SUB * dest, SUB), :] = jnp.where(lane < 64, after, before)
    source = lax.broadcasted_iota(jnp.int32, (LANES, LANES), 0)
    target = lax.broadcasted_iota(jnp.int32, (LANES, LANES), 1)
    inside = target % 16
    wanted = jnp.where(inside < 8, LANES - EDGE + inside // 2, (inside - 8) // 2)
    packed = None
    for p in range(PLANES):
        table = ((source == wanted) & (target // 16 == p)).astype(F32).astype(BF16)
        piece = exact_dot(comb[p], table)
        packed = piece if packed is None else packed + piece
    for dest in range(gy):
        pack[dest] = packed[SUB * dest : SUB * (dest + 1), :]

    def pack_strip(begin):
        for dest in range(gy):
            for p in range(4):
                piece = own[3 + p, begin : begin + 2, pl.ds(dest * wide, wide)]
                strip_out[dest, pl.ds(2 * p, 2), :] = piece

    pl.when(j == gy - 1)(lambda: pack_strip(SUB - 2))
    pl.when(j == 0)(lambda: pack_strip(0))

    for copy in fine_loads:
        copy.wait()

    def turn_edges(p, carry):
        for b in range(sh.blocks):
            rows = pl.ds(LANES * b, LANES)
            low = nat[p, 0, rows, :].T
            high = nat[p, slabs - 1, rows, :].T
            turned[p, b, pl.ds(0, LANES), :] = low
            turned[p, b, pl.ds(LANES * (slabs - 1), LANES), :] = high
            edge_out[0, p, pl.ds(EDGE * b, EDGE), :] = high[LANES - EDGE :, :]
            edge_out[1, p, pl.ds(EDGE * b, EDGE), :] = low[:EDGE, :]
        return carry

    lax.fori_loop(0, PLANES, turn_edges, 0, unroll=PLANES)

    pl.semaphore_wait(barrier, gy + gx - 2)

    edge_right = remote(
        edge_out.at[0], edge_in.at[0], edge_send.at[0], edge_recv.at[0], i, lax.rem(j + 1, gy)
    )
    edge_left = remote(
        edge_out.at[1], edge_in.at[1], edge_send.at[1], edge_recv.at[1], i, lax.rem(j + gy - 1, gy)
    )

    @pl.when(has_right)
    def _():
        edge_right.start()

    @pl.when(has_left)
    def _():
        edge_left.start()

    def sends_of(step):
        to = lax.rem(j + step, gy)
        cols = pl.ds(pl.multiple_of(to * wide, LANES), wide)
        ends = (
            (own.at[pl.ds(0, 3), :, cols], got_c),
            (pack.at[to], got_p),
            (own.at[pl.ds(3, 4), :, cols], got_k),
        )
        return [
            remote(src, dst.at[j + 1], a_send.at[n, step], a_recv.at[n, step], i, to)
            for n, (src, dst) in enumerate(ends)
        ]

    order = list(range(1, gy))
    sends = {step: sends_of(step) for step in order}
    def strip_of(step, side):
        to = lax.rem(j + step, gy)
        return remote(
            strip_out.at[to], strip_in.at[side], strip_send.at[step], strip_recv.at[side], i, to
        )

    for step in order:
        sends[step][0].start()
        sends[step][1].start()

    def send_strips(side):
        for step in order:
            strip_of(step, side).start()
        strip_in[side] = strip_out[j]

    pl.when(j == gy - 1)(lambda: send_strips(0))
    pl.when(j == 0)(lambda: send_strips(1))
    for step in order:
        sends[step][2].start()

    got_p[j + 1] = pack[j]
    for u in range(halves):
        cols = pl.ds(pl.multiple_of(j * wide + LANES * u, LANES), LANES)
        for p in range(PLANES):
            piece = own[p, :, cols]
            if p < 3:
                got_c[j + 1, p, :, pl.ds(LANES * u, LANES)] = piece
            else:
                got_k[j + 1, p - 3, :, pl.ds(LANES * u, LANES)] = piece

    def split_columns(p, carry):
        for b in range(sh.blocks):
            rows = pl.ds(LANES * b, LANES)
            for t in range(1, slabs - 1):
                turned[p, b, pl.ds(LANES * t, LANES), :] = nat[p, t, rows, :].T
        for b in range(sh.blocks):
            rows = pl.ds(FINE_OFF + LANES * b, LANES)
            for s in range(slabs):
                begin = 2 * LANES * (s // 2) + s % 2
                f_a[p, s, rows, :] = turned[p, b, pl.ds(begin, LANES, stride=2), :].T
        return carry

    lax.fori_loop(0, PLANES, split_columns, 0)

    @pl.when(has_left)
    def _():
        edge_right.wait_recv()

    @pl.when(has_right)
    def _():
        edge_left.wait_recv()

    between = jnp.zeros((LANES - 2 * EDGE, LANES), F32)

    def unpack_edges(p, carry):
        for b in range(sh.blocks):
            from_left = edge_in[0, p, pl.ds(EDGE * b, EDGE), :]
            from_right = edge_in[1, p, pl.ds(EDGE * b, EDGE), :]
            slab = jnp.concatenate([from_right, between, from_left], axis=0).T
            f_a[p, halo, pl.ds(FINE_OFF + LANES * b, LANES), :] = slab
        return carry

    lax.fori_loop(0, PLANES, unpack_edges, 0, unroll=PLANES)

    down_i, up_i = lax.rem(i + 1, gx), lax.rem(i + gx - 1, gx)
    row_down = remote(
        f_a.at[:, :, pl.ds(fine_end - SUB, SUB), :],
        f_a.at[:, :, pl.ds(FINE_OFF - SUB, SUB), :],
        row_send.at[0],
        row_recv.at[0],
        down_i,
        j,
    )
    row_up = remote(
        f_a.at[:, :, pl.ds(FINE_OFF, SUB), :],
        f_a.at[:, :, pl.ds(fine_end, SUB), :],
        row_send.at[1],
        row_recv.at[1],
        up_i,
        j,
    )

    @pl.when(has_down)
    def _():
        row_down.start()

    @pl.when(has_up)
    def _():
        row_up.start()

    def coarse_row(m):
        return pl.multiple_of(COARSE_OFF + SUB * m, SUB)

    def halo_of(slot, p):
        return pltpu.roll(got_p[slot], (LANES - (16 * p + 8)) % LANES, 1)

    def swapped_pairs(value):
        return jnp.where(even, pltpu.roll(value, LANES - 1, 1), pltpu.roll(value, 1, 1))

    def produce(k, row, values, c_ref, q_ref, w_ref):
        right = [pltpu.roll(v, 1, 1) for v in values]
        left = [pltpu.roll(v, LANES - 1, 1) for v in values]
        rows = pl.ds(row, SUB)
        count = len(values)
        for t, value in enumerate(values):
            before = jnp.where(first, right[t - 1], right[t])
            after = jnp.where(last, left[(t + 1) % count], left[t])
            c_ref[k, t, rows, :] = value
            main = 0.375 * value
            if t == coarse_halo:
                outer = jnp.where(even, before, after)
                q_ref[k, halo, rows, :] = main + 0.125 * outer
                w_ref[k, t, rows, :] = outer + swapped_pairs(outer)
            else:
                q_ref[k, 2 * t, rows, :] = main + 0.125 * before
                q_ref[k, 2 * t + 1, rows, :] = main + 0.125 * after
                w_ref[k, t, rows, :] = before + after

    def spread_first(slot, carry):
        for k in range(3):
            values = [got_c[slot, k, :, pl.ds(LANES * t, LANES)] for t in range(halves)]
            values.append(halo_of(slot, k))
            produce(k, coarse_row(slot - 1), values, c_a, q_a, w_a)
        return carry

    halo_lanes = ((lane < 2 * EDGE) & has_right) | ((lane >= LANES - 2 * EDGE) & has_left)
    halo_lanes_fine = ((lane < EDGE) & has_right) | ((lane >= LANES - EDGE) & has_left)

    def spread_second(slot, carry):
        rows = pl.ds(coarse_row(slot - 1), SUB)
        held = ((slot > 0) | has_up) & ((slot <= gy) | has_down)
        for k in range(3):
            ckh[k, rows, :] = halo_of(slot, 3 + k)
        for t in range(halves + 1):
            if t == coarse_halo:
                value, valid = halo_of(slot, 6), halo_lanes & held
            else:
                value, valid = got_k[slot, 3, :, pl.ds(LANES * t, LANES)], (lane >= 0) & held
            diag = value + 1.0
            cd[t, rows, :] = diag
            ci[t, rows, :] = jnp.where(valid, 1.0 / diag, 0.0)
        return carry

    fwd_copies = {}
    for n, ref in enumerate((got_c, got_p)):
        fwd_copies[n] = (
            remote(ref.at[gy], ref.at[0], fwd_send.at[0, n], fwd_recv.at[0, n], down_i, j),
            remote(ref.at[1], ref.at[gy + 1], fwd_send.at[1, n], fwd_recv.at[1, n], up_i, j),
        )

    strip_copies = (
        remote(strip_in.at[0], strip_far.at[0], fwd_send.at[0, 2], fwd_recv.at[0, 2], down_i, j),
        remote(strip_in.at[1], strip_far.at[1], fwd_send.at[1, 2], fwd_recv.at[1, 2], up_i, j),
    )

    def pass_strips_on():
        pl.when(j < gy - 1)(lambda: strip_of(1, 0).wait_recv())
        pl.when(has_down)(lambda: strip_copies[0].start())
        pl.when(j > 0)(lambda: strip_of(1, 1).wait_recv())
        pl.when(has_up)(lambda: strip_copies[1].start())

    def strips_passed_on():
        @pl.when(has_up)
        def _():
            strip_copies[0].wait_recv()
            for p in range(4):
                got_k[0, p, pl.ds(SUB - 2, 2), :] = strip_far[0, pl.ds(2 * p, 2), :]

        @pl.when(has_down)
        def _():
            strip_copies[1].wait_recv()
            for p in range(4):
                got_k[gy + 1, p, pl.ds(0, 2), :] = strip_far[1, pl.ds(2 * p, 2), :]

    def wait_from(kinds, source):
        step = lax.rem(j - source + gy, gy)

        @pl.when(step > 0)
        def _():
            for kind in kinds:
                dst = (got_c, got_p, got_k)[kind].at[source + 1]
                remote(dst, dst, a_send.at[kind, step], a_recv.at[kind, step], i, source).wait_recv()

    def pass_on(kinds):
        wait_from(kinds, gy - 1)

        @pl.when(has_down)
        def _():
            for kind in kinds:
                fwd_copies[kind][0].start()

        wait_from(kinds, 0)

        @pl.when(has_up)
        def _():
            for kind in kinds:
                fwd_copies[kind][1].start()

    def wait_rest(kinds):
        def rest(source, carry):
            wait_from(kinds, source)
            return carry

        lax.fori_loop(1, gy - 1, rest, 0)

    def passed_on(kinds):
        @pl.when(has_up)
        def _():
            for kind in kinds:
                fwd_copies[kind][0].wait_recv()

        @pl.when(has_down)
        def _():
            for kind in kinds:
                fwd_copies[kind][1].wait_recv()

    def diagonal(row, held):
        rows = pl.ds(row, SUB)
        for t in range(slabs + 1):
            diag = f_a[6, t, rows, :] + 1.0
            valid = (halo_lanes_fine if t == halo else (lane >= 0)) & held
            fd[t, rows, :] = diag
            fi[t, rows, :] = jnp.where(valid, 1.0 / diag, 0.0)

    def diagonals(step, carry):
        for n in range(4):
            diagonal(pl.multiple_of(FINE_OFF + SUB * (4 * step + n), SUB), lane >= 0)
        return carry

    lax.fori_loop(0, sh.fine_rows // (4 * SUB), diagonals, 0)

    pass_on((0, 1))
    wait_rest((0, 1))
    lax.fori_loop(1, gy + 1, spread_first, 0, unroll=4)

    pass_strips_on()
    @pl.when(has_up)
    def _():
        row_down.wait_recv()

    @pl.when(has_down)
    def _():
        row_up.wait_recv()

    for row, held in (
        (FINE_OFF - 16, lane < 0),
        (FINE_OFF - 8, (lane >= 0) & has_up),
        (fine_end, (lane >= 0) & has_down),
        (fine_end + 8, lane < 0),
    ):
        diagonal(row, held)

    passed_on((0, 1))
    lax.fori_loop(0, 2, lambda e, c: spread_first((gy + 1) * e, c), 0, unroll=2)

    def beside(values):
        side = values[halo]
        odd_right = [pltpu.roll(values[2 * h + 1], 1, 1) for h in range(halves)]
        even_left = [pltpu.roll(values[2 * h], LANES - 1, 1) for h in range(halves)]
        side_right, side_left = pltpu.roll(side, 1, 1), pltpu.roll(side, LANES - 1, 1)
        sums = []
        for h in range(halves):
            before = odd_right[h - 1] if h > 0 else side_right
            after = even_left[h + 1] if h < halves - 1 else side_left
            sums.append(jnp.where(first, before, odd_right[h]) + values[2 * h + 1])
            sums.append(values[2 * h] + jnp.where(last, after, even_left[h]))
        sums.append(
            jnp.where(first, odd_right[-1], side_right) + jnp.where(last, even_left[0], side_left)
        )
        return sums

    def fine_tile(m, acc, f_in, q_ref, f_out, count):
        base = FINE_OFF + 16 * m
        upper, lower = pl.ds(base, SUB, stride=2), pl.ds(base + 1, SUB, stride=2)
        above, below = pl.ds(base - 1, SUB, stride=2), pl.ds(base + 2, SUB, stride=2)
        crow = COARSE_OFF + SUB * m
        q_here, q_up, q_down = pl.ds(crow, SUB), pl.ds(crow - 1, SUB), pl.ds(crow + 1, SUB)
        for k in range(3):
            tops = [f_in[k, t, upper, :] for t in range(slabs + 1)]
            lows = [f_in[k, t, lower, :] for t in range(slabs + 1)]
            top_sum, low_sum = beside(tops), beside(lows)
            for t in range(count):
                three = 3.0 * q_ref[k, t, q_here, :]
                nb = (lows[t] + f_in[k, t, above, :]) + (top_sum[t] + q_ref[k, t, q_up, :])
                total = f_a[3 + k, t, upper, :] + 0.25 * (nb + three)
                res = total - fd[t, upper, :] * tops[t]
                f_out[k, t, upper, :] = total * fi[t, upper, :]
                nb2 = (tops[t] + f_in[k, t, below, :]) + (low_sum[t] + q_ref[k, t, q_down, :])
                total2 = f_a[3 + k, t, lower, :] + 0.25 * (nb2 + three)
                res2 = total2 - fd[t, lower, :] * lows[t]
                f_out[k, t, lower, :] = total2 * fi[t, lower, :]
                if acc is not None and t < slabs:
                    acc = acc + (res * res + res2 * res2)
        return acc

    def coarse_sum(m, k, t, f_in, c_ref, w_ref):
        base = FINE_OFF + 16 * m
        upper, lower = pl.ds(base, SUB, stride=2), pl.ds(base + 1, SUB, stride=2)
        if t == coarse_halo:
            four = f_in[k, halo, upper, :] + f_in[k, halo, lower, :]
            four = four + swapped_pairs(four)
        else:
            four = (f_in[k, 2 * t, upper, :] + f_in[k, 2 * t, lower, :]) + (
                f_in[k, 2 * t + 1, upper, :] + f_in[k, 2 * t + 1, lower, :]
            )
        return 0.25 * (coarse_near(m, k, t, c_ref, w_ref) + 0.5 * four)

    def coarse_step(m, k, t, acc, added, c_ref):
        rows = pl.ds(coarse_row(m), SUB)
        if t == coarse_halo:
            known = ckh[k, rows, :]
        else:
            known = got_k[m + 1, k, :, pl.ds(LANES * t, LANES)]
        total = known + added
        if acc is not None and t < halves:
            res = total - cd[t, rows, :] * c_ref[k, t, rows, :]
            acc = acc + res * res
        return total * ci[t, rows, :], acc

    def near_sum(m, carry):
        base = FINE_OFF + 16 * m
        upper, lower = pl.ds(base, SUB, stride=2), pl.ds(base + 1, SUB, stride=2)
        above, below = pl.ds(base - 1, SUB, stride=2), pl.ds(base + 2, SUB, stride=2)
        for k in range(3):
            tops = [f_b[k, t, upper, :] for t in range(slabs + 1)]
            lows = [f_b[k, t, lower, :] for t in range(slabs + 1)]
            top_sum, low_sum = beside(tops), beside(lows)
            both = [tops[t] + lows[t] for t in range(slabs + 1)]
            for t in range(slabs + 1):
                nb = (lows[t] + f_b[k, t, above, :]) + top_sum[t]
                near[k, t, upper, :] = f_a[3 + k, t, upper, :] + 0.25 * nb
                nb2 = (tops[t] + f_b[k, t, below, :]) + low_sum[t]
                near[k, t, lower, :] = f_a[3 + k, t, lower, :] + 0.25 * nb2
            rows = pl.ds(coarse_row(m), SUB)
            for t in range(halves):
                pre_b[k, t, rows, :] = 0.125 * (both[2 * t] + both[2 * t + 1])
            side = both[halo]
            pre_b[k, coarse_halo, rows, :] = 0.125 * (side + swapped_pairs(side))
        return zero

    def second_fine(m, acc):
        base = FINE_OFF + 16 * m
        upper, lower = pl.ds(base, SUB, stride=2), pl.ds(base + 1, SUB, stride=2)
        crow = COARSE_OFF + SUB * m
        q_here, q_up, q_down = pl.ds(crow, SUB), pl.ds(crow - 1, SUB), pl.ds(crow + 1, SUB)
        for k in range(3):
            for t in range(slabs + 1):
                three = 0.75 * q_b[k, t, q_here, :]
                total = near[k, t, upper, :] + (three + 0.25 * q_b[k, t, q_up, :])
                res = total - fd[t, upper, :] * f_b[k, t, upper, :]
                f_a[k, t, upper, :] = total * fi[t, upper, :]
                total2 = near[k, t, lower, :] + (three + 0.25 * q_b[k, t, q_down, :])
                res2 = total2 - fd[t, lower, :] * f_b[k, t, lower, :]
                f_a[k, t, lower, :] = total2 * fi[t, lower, :]
                if t < slabs:
                    acc = acc + (res * res + res2 * res2)
        return acc

    def coarse_near(m, k, t, c_ref, w_ref):
        crow = COARSE_OFF + SUB * m
        nb = c_ref[k, t, pl.ds(crow - 1, SUB), :] + c_ref[k, t, pl.ds(crow + 1, SUB), :]
        return nb + w_ref[k, t, pl.ds(coarse_row(m), SUB), :]

    def first_sum(m, carry):
        rows = pl.ds(coarse_row(m), SUB)
        for k in range(3):
            for t in range(halves + 1):
                pre[k, t, rows, :] = coarse_sum(m, k, t, f_a, c_a, w_a)
        return zero

    def first_coarse(m, acc):
        rows = pl.ds(coarse_row(m), SUB)
        for k in range(3):
            values = []
            for t in range(halves + 1):
                value, acc = coarse_step(m, k, t, acc, pre[k, t, rows, :], c_a)
                values.append(value)
            produce(k, coarse_row(m), values, c_b, q_b, w_b)
        return acc

    def second_coarse(m, acc):
        for k in range(3):
            values = []
            for t in range(halves + 1):
                added = pre_b[k, t, pl.ds(coarse_row(m), SUB), :]
                added = added + 0.25 * coarse_near(m, k, t, c_b, w_b)
                value, acc = coarse_step(m, k, t, acc, added, c_b)
                values.append(value)
            produce(k, coarse_row(m), values, c_a, q_a, w_a)
        return acc

    def third_coarse(m, acc):
        for k in range(3):
            for t in range(halves):
                added = coarse_sum(m, k, t, f_a, c_a, w_a)
                value, acc = coarse_step(m, k, t, acc, added, c_a)
                fin[m, k, :, pl.ds(LANES * t, LANES)] = value
        return acc

    def every_tile(body, acc, unroll=6):
        def step(n, acc):
            m = n - 1
            part_sum = body(m, zero)
            inner = jnp.where((n > 0) & (n <= tiles), 1.0, 0.0).astype(F32)
            return acc + part_sum * inner

        return lax.fori_loop(0, tiles + 2, step, acc, unroll=unroll)

    def fine_first(m, acc):
        return fine_tile(m, acc, f_a, q_a, f_b, slabs + 1)

    def fine_third(m, acc):
        return fine_tile(m, acc, f_a, q_a, f_b, slabs)

    fine_sum1 = every_tile(fine_first, zero)
    every_tile(first_sum, zero)
    every_tile(near_sum, zero)

    wait_from((2,), 0)
    wait_from((2,), gy - 1)
    wait_rest((2,))
    lax.fori_loop(1, gy + 1, spread_second, 0, unroll=8)
    strips_passed_on()
    lax.fori_loop(0, 2, lambda e, c: spread_second((gy + 1) * e, c), 0, unroll=2)

    coarse_sum1 = every_tile(first_coarse, zero, unroll=6)

    @pl.when(has_down)
    def _():
        row_down.wait_send()

    @pl.when(has_up)
    def _():
        row_up.wait_send()

    fine_sum2 = every_tile(second_fine, zero, unroll=3)
    coarse_sum2 = every_tile(second_coarse, zero, unroll=6)
    coarse_sum3 = lax.fori_loop(0, tiles, third_coarse, zero, unroll=4)

    my_cols = pl.ds(pl.multiple_of(j * wide, LANES), wide)
    finals = []
    for step in order:
        to = lax.rem(j + step, gy)
        copy = remote(
            fin.at[to], coarse_out.at[:, :, my_cols], fin_send.at[step], fin_recv.at[step], i, to
        )
        copy.start()
        finals.append(copy)
    for k in range(3):
        for t in range(halves):
            cols = pl.ds(pl.multiple_of(j * wide + LANES * t, LANES), LANES)
            coarse_out[k, :, cols] = fin[j, k, :, pl.ds(LANES * t, LANES)]

    fine_sum3 = lax.fori_loop(0, tiles, fine_third, zero, unroll=8)

    row_of = lax.broadcasted_iota(jnp.int32, (SUB, LANES), 0)
    mine = zero
    sums = ((fine_sum1, coarse_sum1), (fine_sum2, coarse_sum2), (fine_sum3, coarse_sum3))
    for s, (fine_part, coarse_part) in enumerate(sums):
        line = jnp.sum(fine_part + coarse_part, axis=0, keepdims=True)
        mine = jnp.where(row_of == s, line, mine)
    part[0] = mine
    norm_x = []
    for step in range(1, gx):
        copy = remote(
            part.at[0],
            part_gx.at[step],
            norm_send.at[0, step],
            norm_recv_x.at[step],
            lax.rem(i + step, gx),
            j,
        )
        copy.start()
        norm_x.append(copy)

    def join_columns(k, carry):
        for b in range(sh.blocks):
            rows = pl.ds(FINE_OFF + LANES * b, LANES)
            for s in range(slabs):
                begin = 2 * LANES * (s // 2) + s % 2
                swapped[b, pl.ds(begin, LANES, stride=2), :] = f_b[k, s, rows, :].T
            for t in range(slabs):
                natural = swapped[b, pl.ds(LANES * t, LANES), :].T
                fine_out[k, pl.ds(LANES * b, LANES), pl.ds(LANES * t, LANES)] = natural
        return carry

    lax.fori_loop(0, 3, join_columns, 0)

    for copy in norm_x:
        copy.wait_recv()
    for step in range(1, gx):
        mine = mine + part_gx[step]
    part[1] = mine
    norm_y = []
    for step in order:
        copy = remote(
            part.at[1],
            part_gy.at[step],
            norm_send.at[1, step],
            norm_recv_y.at[step],
            i,
            lax.rem(j + step, gy),
        )
        copy.start()
        norm_y.append(copy)
    for copy in norm_y:
        copy.wait_recv()
    for step in order:
        mine = mine + part_gy[step]
    total = jnp.sum(mine, axis=1, keepdims=True) * (1.0 / sh.cells)
    norm_out[...] = jnp.broadcast_to(jnp.sqrt(total), (SUB, LANES))

    @pl.when(has_right)
    def _():
        edge_right.wait_send()

    @pl.when(has_left)
    def _():
        edge_left.wait_send()

    @pl.when(has_down)
    def _():
        for kind in range(2):
            fwd_copies[kind][0].wait_send()
        strip_copies[0].wait_send()

    @pl.when(has_up)
    def _():
        for kind in range(2):
            fwd_copies[kind][1].wait_send()
        strip_copies[1].wait_send()

    for step in order:
        for copy in sends[step]:
            copy.wait_send()

    @pl.when((j == 0) | (j == gy - 1))
    def _():
        for step in order:
            strip_of(step, 0).wait_send()

    for copy in finals:
        copy.wait()
    for copy in norm_y + norm_x:
        copy.wait_send()


def store_kernel(fine, coarse, norms, fine_out, coarse_out, norm_out, scalars, sem):
    stores = [
        pltpu.make_async_copy(fine, fine_out, sem.at[0]),
        pltpu.make_async_copy(coarse, coarse_out, sem.at[1]),
        pltpu.make_async_copy(scalars, norm_out, sem.at[2]),
    ]
    stores[0].start()
    stores[1].start()
    for s in range(SWEEPS):
        scalars[s] = norms[s, 0]
    stores[2].start()
    for copy in stores:
        copy.wait()


def solution(mesh):
    gx, gy = mesh.shape["gx"], mesh.shape["gy"]

    def on_device(fine_start, fine_known, fine_mu, coarse_start, coarse_known, coarse_mu):
        sh = Shape(gx, gy, *fine_mu.shape)
        dma = pltpu.SemaphoreType.DMA
        in_hbm = pl.BlockSpec(memory_space=pltpu.HBM)
        on_chip = pl.BlockSpec(memory_space=pltpu.VMEM)

        def fine(*lead):
            return pltpu.VMEM((*lead, sh.slabs + 1, sh.fine_buf, LANES), F32)

        def coarse(*lead):
            return pltpu.VMEM((*lead, sh.coarse_buf, LANES), F32)

        few = sh.halves + 1
        fine_v, coarse_v, norm_v = pl.pallas_call(
            functools.partial(kernel, sh),
            out_shape=(
                pltpu.VMEM(fine_start.shape, F32),
                pltpu.VMEM(coarse_start.shape, F32),
                pltpu.VMEM((SUB, LANES), F32),
            ),
            in_specs=[in_hbm] * 6,
            out_specs=(on_chip, on_chip, on_chip),
            scratch_shapes=[
                pltpu.VMEM((PLANES, sh.slabs, sh.fine_rows, LANES), F32),
                pltpu.VMEM((PLANES, sh.blocks, sh.slabs * LANES, LANES), F32),
                pltpu.VMEM((sh.blocks, sh.slabs * LANES, LANES), F32),
                fine(PLANES),
                fine(3),
                fine(),
                fine(),
                coarse(3, few),
                coarse(3, few),
                coarse(3, sh.slabs + 1),
                coarse(3, sh.slabs + 1),
                coarse(3, few),
                coarse(3, few),
                coarse(3),
                coarse(few),
                coarse(few),
                coarse(3, few),
                coarse(3, few),
                fine(3),
                pltpu.VMEM((PLANES, SUB, gy * sh.wide), F32),
                pltpu.VMEM((PLANES, gy * SUB, LANES), F32),
                pltpu.VMEM((gy, SUB, LANES), F32),
                pltpu.VMEM((gy + 2, 3, SUB, sh.wide), F32),
                pltpu.VMEM((gy + 2, SUB, LANES), F32),
                pltpu.VMEM((gy + 2, 4, SUB, sh.wide), F32),
                pltpu.VMEM((gy, SUB, sh.wide), F32),
                pltpu.VMEM((2, SUB, sh.wide), F32),
                pltpu.VMEM((2, SUB, sh.wide), F32),
                pltpu.VMEM((2, PLANES, SUB, LANES), F32),
                pltpu.VMEM((2, PLANES, SUB, LANES), F32),
                pltpu.VMEM((gy, 3, SUB, sh.wide), F32),
                pltpu.VMEM((2, SUB, LANES), F32),
                pltpu.VMEM((gy, SUB, LANES), F32),
                pltpu.VMEM((gx, SUB, LANES), F32),
                dma((3 + 3 * sh.slabs,)),
                dma((2,)),
                dma((2,)),
                dma((2,)),
                dma((2,)),
                dma((3, gy)),
                dma((3, gy)),
                dma((2, 3)),
                dma((2, 3)),
                dma((gy,)),
                dma((2,)),
                dma((gy,)),
                dma((gy,)),
                dma((2, max(gx, gy))),
                dma((gy,)),
                dma((gx,)),
            ],
            compiler_params=pltpu.CompilerParams(
                collective_id=0, has_side_effects=True, vmem_limit_bytes=64_500_000
            ),
            name="interface_sweeps",
        )(fine_start, fine_known, fine_mu, coarse_start, coarse_known, coarse_mu)
        anywhere = pl.BlockSpec(memory_space=pl.ANY)
        return pl.pallas_call(
            store_kernel,
            out_shape=(
                jax.ShapeDtypeStruct(fine_start.shape, F32),
                jax.ShapeDtypeStruct(coarse_start.shape, F32),
                jax.ShapeDtypeStruct((SWEEPS,), F32),
            ),
            in_specs=[anywhere, anywhere, on_chip],
            out_specs=(in_hbm, in_hbm, in_hbm),
            scratch_shapes=[pltpu.SMEM((SWEEPS,), F32), dma((3,))],
            compiler_params=pltpu.CompilerParams(vmem_limit_bytes=1_000_000),
            name="store_results",
        )(fine_v, coarse_v, norm_v)

    return jax.shard_map(
        on_device,
        mesh=mesh,
        in_specs=(
            P(None, "gx", "gy"),
            P(None, "gx", "gy"),
            P("gx", "gy"),
            P(None, ("gx", "gy"), None),
            P(None, ("gx", "gy"), None),
            P(("gx", "gy"), None),
        ),
        out_specs=(P(None, "gx", "gy"), P(None, ("gx", "gy"), None), P(None)),
        check_vma=False,
    )
```

```python
import functools

import jax
import jax.numpy as jnp
from jax import lax
from jax.experimental import pallas as pl
from jax.experimental.pallas import tpu as pltpu
from jax.sharding import PartitionSpec as P

MESH = pl.DeviceIdType.MESH
F32 = jnp.float32
BF16 = jnp.bfloat16
SWEEPS = 3
LANES = 128
SUB = 8
FINE_OFF = 24
COARSE_OFF = 16
EDGE = 4
PLANES = 7


class Shape:
    def __init__(self, gx, gy, fine_rows, fine_cols):
        self.gx, self.gy = gx, gy
        self.fine_rows, self.fine_cols = fine_rows, fine_cols
        self.coarse_rows, self.wide = fine_rows // 2, fine_cols // 2
        self.tiles = self.coarse_rows // SUB
        self.halves = self.wide // LANES
        self.slabs = 2 * self.halves
        self.fine_buf = fine_rows + 2 * FINE_OFF
        self.coarse_buf = self.coarse_rows + 2 * COARSE_OFF + SUB
        self.blocks = fine_rows // LANES
        self.cells = 3.0 * gx * gy * fine_rows * fine_cols * 1.25


RING = 4


def hops(step):
    return sum(min(d, RING - d) for d in divmod(step, RING))


def far_first(count):
    return sorted(range(1, count), key=lambda step: -hops(step))


def torus_add(at, step):
    row, column = at // RING + step // RING, lax.rem(at, RING) + step % RING
    return lax.rem(row, RING) * RING + lax.rem(column, RING)


def torus_back(at, step):
    row, column = at // RING + RING - step // RING, lax.rem(at, RING) + RING - step % RING
    return lax.rem(row, RING) * RING + lax.rem(column, RING)


def lane_iota():
    return lax.broadcasted_iota(jnp.int32, (SUB, LANES), 1)


def exact_dot(values, table):
    high = values.astype(BF16)
    rest = values - high.astype(F32)
    middle = rest.astype(BF16)
    low = (rest - middle.astype(F32)).astype(BF16)
    total = jnp.dot(high, table, preferred_element_type=F32)
    total = total + jnp.dot(middle, table, preferred_element_type=F32)
    return total + jnp.dot(low, table, preferred_element_type=F32)


def kernel(
    sh,
    fine_start,
    fine_known,
    fine_mu,
    coarse_start,
    coarse_known,
    coarse_mu,
    fine_out,
    coarse_out,
    norm_out,
    nat,
    turned,
    swapped,
    f_a,
    f_b,
    fd,
    fi,
    c_a,
    c_b,
    q_a,
    q_b,
    w_a,
    w_b,
    ckh,
    cd,
    ci,
    pre,
    pre_b,
    near,
    own,
    comb,
    pack,
    got_c,
    got_p,
    got_k,
    strip_out,
    strip_in,
    strip_far,
    edge_out,
    edge_in,
    fin,
    part,
    part_gy,
    part_gx,
    load_sem,
    edge_send,
    edge_recv,
    row_send,
    row_recv,
    a_send,
    a_recv,
    fwd_send,
    fwd_recv,
    strip_send,
    strip_recv,
    fin_send,
    fin_recv,
    norm_send,
    norm_recv_y,
    norm_recv_x,
):
    gx, gy = sh.gx, sh.gy
    i = lax.axis_index("gx")
    j = lax.axis_index("gy")
    halves, slabs, tiles, wide = sh.halves, sh.slabs, sh.tiles, sh.wide
    halo, coarse_halo = slabs, halves
    lane = lane_iota()
    even = lane % 2 == 0
    first = lane == 0
    last = lane == LANES - 1
    has_up, has_down = i > 0, i < gx - 1
    has_left, has_right = j > 0, j < gy - 1

    def remote(src, dst, send, recv, to_i, to_j):
        return pltpu.make_async_remote_copy(
            src_ref=src,
            dst_ref=dst,
            send_sem=send,
            recv_sem=recv,
            device_id=(to_i, to_j),
            device_id_type=MESH,
        )

    loads = []

    def load(src, dst):
        copy = pltpu.make_async_copy(src, dst, load_sem.at[len(loads)])
        copy.start()
        loads.append(copy)
        return copy

    own_loads = [
        load(coarse_start, own.at[pl.ds(0, 3)]),
        load(coarse_known, own.at[pl.ds(3, 3)]),
        load(coarse_mu, own.at[6]),
    ]
    fine_loads = []
    for t in [0, slabs - 1] + list(range(1, slabs - 1)):
        cols = pl.ds(LANES * t, LANES)
        fine_loads.append(load(fine_start.at[:, :, cols], nat.at[pl.ds(0, 3), t]))
        fine_loads.append(load(fine_known.at[:, :, cols], nat.at[pl.ds(3, 3), t]))
        fine_loads.append(load(fine_mu.at[:, cols], nat.at[6, t]))

    barrier = pltpu.get_barrier_semaphore()
    for step in far_first(gy):
        pl.semaphore_signal(
            barrier, inc=1, device_id=(i, torus_add(j, step)), device_id_type=MESH
        )
    for step in range(1, gx):
        pl.semaphore_signal(
            barrier, inc=1, device_id=(lax.rem(i + step, gx), j), device_id_type=MESH
        )

    zero = jnp.zeros((SUB, LANES), F32)
    fine_end = FINE_OFF + sh.fine_rows
    for t in range(slabs + 1):
        for row in (0, 8, fine_end + 8, fine_end + 16):
            for p in range(PLANES):
                f_a[p, t, pl.ds(row, SUB), :] = zero
        for k in range(3):
            for row in (0, fine_end + 16):
                f_b[k, t, pl.ds(row, SUB), :] = zero
            for row in (0, sh.coarse_buf - 8):
                q_a[k, t, pl.ds(row, SUB), :] = zero
                q_b[k, t, pl.ds(row, SUB), :] = zero
                if t <= halves:
                    c_a[k, t, pl.ds(row, SUB), :] = zero
                    c_b[k, t, pl.ds(row, SUB), :] = zero

    for slot in (0, gy + 1):
        for u in range(halves):
            for p in range(4):
                got_k[slot, p, :, pl.ds(LANES * u, LANES)] = zero

    def clear_rows(row, slot):
        for p in range(PLANES):
            for t in range(slabs + 1):
                f_a[p, t, pl.ds(row, SUB), :] = zero
        got_p[slot] = zero
        for u in range(halves):
            for p in range(3):
                got_c[slot, p, :, pl.ds(LANES * u, LANES)] = zero

    def clear_columns(side):
        for p in range(PLANES):
            edge_in[side, p] = zero

    pl.when(i == 0)(lambda: clear_rows(FINE_OFF - SUB, 0))
    pl.when(i == gx - 1)(lambda: clear_rows(fine_end, gy + 1))
    pl.when(j == 0)(lambda: clear_columns(0))
    pl.when(j == gy - 1)(lambda: clear_columns(1))

    for copy in own_loads:
        copy.wait()

    for dest in range(gy):
        for p in range(PLANES):
            after = own[p, :, pl.ds((dest + 1) * wide, LANES)] if dest < gy - 1 else zero
            before = own[p, :, pl.ds(dest * wide - LANES, LANES)] if dest > 0 else zero
            comb[p, pl.ds(SUB * dest, SUB), :] = jnp.where(lane < 64, after, before)
    source = lax.broadcasted_iota(jnp.int32, (LANES, LANES), 0)
    target = lax.broadcasted_iota(jnp.int32, (LANES, LANES), 1)
    inside = target % 16
    wanted = jnp.where(inside < 8, LANES - EDGE + inside // 2, (inside - 8) // 2)
    packed = None
    for p in range(PLANES):
        table = ((source == wanted) & (target // 16 == p)).astype(F32).astype(BF16)
        piece = exact_dot(comb[p], table)
        packed = piece if packed is None else packed + piece
    for dest in range(gy):
        pack[dest] = packed[SUB * dest : SUB * (dest + 1), :]

    def pack_strip(begin):
        for dest in range(gy):
            for p in range(4):
                piece = own[3 + p, begin : begin + 2, pl.ds(dest * wide, wide)]
                strip_out[dest, pl.ds(2 * p, 2), :] = piece

    pl.when(j == gy - 1)(lambda: pack_strip(SUB - 2))
    pl.when(j == 0)(lambda: pack_strip(0))

    for copy in fine_loads:
        copy.wait()

    def turn_edges(p, carry):
        for b in range(sh.blocks):
            rows = pl.ds(LANES * b, LANES)
            low = nat[p, 0, rows, :].T
            high = nat[p, slabs - 1, rows, :].T
            turned[p, b, pl.ds(0, LANES), :] = low
            turned[p, b, pl.ds(LANES * (slabs - 1), LANES), :] = high
            edge_out[0, p, pl.ds(EDGE * b, EDGE), :] = high[LANES - EDGE :, :]
            edge_out[1, p, pl.ds(EDGE * b, EDGE), :] = low[:EDGE, :]
        return carry

    lax.fori_loop(0, PLANES, turn_edges, 0, unroll=PLANES)

    pl.semaphore_wait(barrier, gy + gx - 2)

    edge_right = remote(
        edge_out.at[0], edge_in.at[0], edge_send.at[0], edge_recv.at[0], i, lax.rem(j + 1, gy)
    )
    edge_left = remote(
        edge_out.at[1], edge_in.at[1], edge_send.at[1], edge_recv.at[1], i, lax.rem(j + gy - 1, gy)
    )

    @pl.when(has_right)
    def _():
        edge_right.start()

    @pl.when(has_left)
    def _():
        edge_left.start()

    def sends_of(step):
        to = torus_add(j, step)
        cols = pl.ds(pl.multiple_of(to * wide, LANES), wide)
        ends = (
            (own.at[pl.ds(0, 3), :, cols], got_c),
            (pack.at[to], got_p),
            (own.at[pl.ds(3, 4), :, cols], got_k),
        )
        return [
            remote(src, dst.at[j + 1], a_send.at[n, step], a_recv.at[n, step], i, to)
            for n, (src, dst) in enumerate(ends)
        ]

    order = far_first(gy)
    sends = {step: sends_of(step) for step in order}
    def strip_of(step, side):
        to = torus_add(j, step)
        return remote(
            strip_out.at[to], strip_in.at[side], strip_send.at[step], strip_recv.at[side], i, to
        )

    for step in order:
        sends[step][0].start()
        sends[step][1].start()

    def send_strips(side):
        for step in order:
            strip_of(step, side).start()
        strip_in[side] = strip_out[j]

    pl.when(j == gy - 1)(lambda: send_strips(0))
    pl.when(j == 0)(lambda: send_strips(1))
    for step in order:
        sends[step][2].start()

    got_p[j + 1] = pack[j]
    for u in range(halves):
        cols = pl.ds(pl.multiple_of(j * wide + LANES * u, LANES), LANES)
        for p in range(PLANES):
            piece = own[p, :, cols]
            if p < 3:
                got_c[j + 1, p, :, pl.ds(LANES * u, LANES)] = piece
            else:
                got_k[j + 1, p - 3, :, pl.ds(LANES * u, LANES)] = piece

    def scale_of(p):
        return jnp.where((p >= 3) & (p < 6), 4.0, 1.0).astype(F32)

    def split_columns(p, carry):
        scale = scale_of(p)
        for b in range(sh.blocks):
            rows = pl.ds(LANES * b, LANES)
            for t in range(1, slabs - 1):
                turned[p, b, pl.ds(LANES * t, LANES), :] = nat[p, t, rows, :].T
        for b in range(sh.blocks):
            rows = pl.ds(FINE_OFF + LANES * b, LANES)
            for s in range(slabs):
                begin = 2 * LANES * (s // 2) + s % 2
                f_a[p, s, rows, :] = turned[p, b, pl.ds(begin, LANES, stride=2), :].T * scale
        return carry

    lax.fori_loop(0, PLANES, split_columns, 0)

    @pl.when(has_left)
    def _():
        edge_right.wait_recv()

    @pl.when(has_right)
    def _():
        edge_left.wait_recv()

    between = jnp.zeros((LANES - 2 * EDGE, LANES), F32)

    def unpack_edges(p, carry):
        for b in range(sh.blocks):
            from_left = edge_in[0, p, pl.ds(EDGE * b, EDGE), :]
            from_right = edge_in[1, p, pl.ds(EDGE * b, EDGE), :]
            slab = jnp.concatenate([from_right, between, from_left], axis=0).T * scale_of(p)
            f_a[p, halo, pl.ds(FINE_OFF + LANES * b, LANES), :] = slab
        return carry

    lax.fori_loop(0, PLANES, unpack_edges, 0, unroll=PLANES)

    down_i, up_i = lax.rem(i + 1, gx), lax.rem(i + gx - 1, gx)
    row_down = remote(
        f_a.at[:, :, pl.ds(fine_end - SUB, SUB), :],
        f_a.at[:, :, pl.ds(FINE_OFF - SUB, SUB), :],
        row_send.at[0],
        row_recv.at[0],
        down_i,
        j,
    )
    row_up = remote(
        f_a.at[:, :, pl.ds(FINE_OFF, SUB), :],
        f_a.at[:, :, pl.ds(fine_end, SUB), :],
        row_send.at[1],
        row_recv.at[1],
        up_i,
        j,
    )

    @pl.when(has_down)
    def _():
        row_down.start()

    @pl.when(has_up)
    def _():
        row_up.start()

    def coarse_row(m):
        return pl.multiple_of(COARSE_OFF + SUB * m, SUB)

    def halo_of(slot, p):
        return pltpu.roll(got_p[slot], (LANES - (16 * p + 8)) % LANES, 1)

    def swapped_pairs(value):
        return jnp.where(even, pltpu.roll(value, LANES - 1, 1), pltpu.roll(value, 1, 1))

    def produce(k, row, values, c_ref, q_ref, w_ref, inner=False):
        right = [pltpu.roll(v, 1, 1) for v in values]
        left = [pltpu.roll(v, LANES - 1, 1) for v in values]
        rows = pl.ds(row, SUB)
        count = len(values)
        for t, value in enumerate(values):
            if t == coarse_halo and inner:
                continue
            before = jnp.where(first, right[t - 1], right[t])
            after = jnp.where(last, left[(t + 1) % count], left[t])
            c_ref[k, t, rows, :] = value
            main = 0.375 * value
            if t == coarse_halo:
                outer = jnp.where(even, before, after)
                q_ref[k, halo, rows, :] = main + 0.125 * outer
                w_ref[k, t, rows, :] = outer + swapped_pairs(outer)
            else:
                q_ref[k, 2 * t, rows, :] = main + 0.125 * before
                q_ref[k, 2 * t + 1, rows, :] = main + 0.125 * after
                w_ref[k, t, rows, :] = before + after

    def spread_first(slot, carry):
        for k in range(3):
            values = [got_c[slot, k, :, pl.ds(LANES * t, LANES)] for t in range(halves)]
            values.append(halo_of(slot, k))
            produce(k, coarse_row(slot - 1), values, c_a, q_a, w_a)
        return carry

    halo_lanes = ((lane < 2 * EDGE) & has_right) | ((lane >= LANES - 2 * EDGE) & has_left)
    halo_lanes_fine = ((lane < EDGE) & has_right) | ((lane >= LANES - EDGE) & has_left)

    def spread_second(slot, carry):
        rows = pl.ds(coarse_row(slot - 1), SUB)
        held = ((slot > 0) | has_up) & ((slot <= gy) | has_down)
        for k in range(3):
            ckh[k, rows, :] = 4.0 * halo_of(slot, 3 + k)
        for t in range(halves + 1):
            if t == coarse_halo:
                value, valid = halo_of(slot, 6), halo_lanes & held
            else:
                value, valid = got_k[slot, 3, :, pl.ds(LANES * t, LANES)], (lane >= 0) & held
            diag = value + 1.0
            cd[t, rows, :] = diag * diag
            ci[t, rows, :] = jnp.where(valid, 0.25 * (1.0 / diag), 0.0)
        return carry

    fwd_copies = {}
    for n, ref in enumerate((got_c, got_p)):
        fwd_copies[n] = (
            remote(ref.at[gy], ref.at[0], fwd_send.at[0, n], fwd_recv.at[0, n], down_i, j),
            remote(ref.at[1], ref.at[gy + 1], fwd_send.at[1, n], fwd_recv.at[1, n], up_i, j),
        )

    strip_copies = (
        remote(strip_in.at[0], strip_far.at[0], fwd_send.at[0, 2], fwd_recv.at[0, 2], down_i, j),
        remote(strip_in.at[1], strip_far.at[1], fwd_send.at[1, 2], fwd_recv.at[1, 2], up_i, j),
    )

    def pass_strips_on():
        pl.when(j < gy - 1)(lambda: strip_of(1, 0).wait_recv())
        pl.when(has_down)(lambda: strip_copies[0].start())
        pl.when(j > 0)(lambda: strip_of(1, 1).wait_recv())
        pl.when(has_up)(lambda: strip_copies[1].start())

    def strips_passed_on():
        @pl.when(has_up)
        def _():
            strip_copies[0].wait_recv()
            for p in range(4):
                got_k[0, p, pl.ds(SUB - 2, 2), :] = strip_far[0, pl.ds(2 * p, 2), :]

        @pl.when(has_down)
        def _():
            strip_copies[1].wait_recv()
            for p in range(4):
                got_k[gy + 1, p, pl.ds(0, 2), :] = strip_far[1, pl.ds(2 * p, 2), :]

    def wait_step(kinds, step):
        source = torus_back(j, step)
        for kind in kinds:
            dst = (got_c, got_p, got_k)[kind].at[source + 1]
            remote(dst, dst, a_send.at[kind, step], a_recv.at[kind, step], i, source).wait_recv()

    def wait_source(kinds, source):
        step = RING * lax.rem(j // RING + RING - source // RING, RING)
        step = step + lax.rem(lax.rem(j, RING) + RING - source % RING, RING)

        @pl.when(step > 0)
        def _():
            for kind in kinds:
                dst = (got_c, got_p, got_k)[kind].at[source + 1]
                remote(dst, dst, a_send.at[kind, step], a_recv.at[kind, step], i, source).wait_recv()

    def pass_on(source):
        wait_source((0, 1), source)
        side, there = (0, has_down) if source else (1, has_up)

        @pl.when(there)
        def _():
            fwd_copies[0][side].start()
            fwd_copies[1][side].start()

    def passed_on():
        @pl.when(has_up)
        def _():
            fwd_copies[0][0].wait_recv()
            fwd_copies[1][0].wait_recv()

        @pl.when(has_down)
        def _():
            fwd_copies[0][1].wait_recv()
            fwd_copies[1][1].wait_recv()

    def diagonal(row, held):
        rows = pl.ds(row, SUB)
        for t in range(slabs + 1):
            diag = f_a[6, t, rows, :] + 1.0
            valid = (halo_lanes_fine if t == halo else (lane >= 0)) & held
            fd[t, rows, :] = diag * diag
            fi[t, rows, :] = jnp.where(valid, 0.25 * (1.0 / diag), 0.0)

    def diagonals(step, carry):
        for n in range(4):
            diagonal(pl.multiple_of(FINE_OFF + SUB * (4 * step + n), SUB), lane >= 0)
        return carry

    lax.fori_loop(0, sh.fine_rows // (4 * SUB), diagonals, 0)

    pass_on(gy - 1)
    pass_on(0)
    group = 4
    for begin in range(0, gy, group):
        if begin == gy // 2:
            pass_strips_on()
        sources = []
        for step in ([0] + order)[begin : begin + group]:
            source = torus_back(j, step) if step else j
            if step:
                pl.when((source > 0) & (source < gy - 1))(lambda: wait_step((0, 1), step))
            sources.append(source)
        for source in sources:
            spread_first(source + 1, 0)

    def beside(values):
        side = values[halo]
        odd_right = [pltpu.roll(values[2 * h + 1], 1, 1) for h in range(halves)]
        even_left = [pltpu.roll(values[2 * h], LANES - 1, 1) for h in range(halves)]
        side_right, side_left = pltpu.roll(side, 1, 1), pltpu.roll(side, LANES - 1, 1)
        sums = []
        for h in range(halves):
            before = odd_right[h - 1] if h > 0 else side_right
            after = even_left[h + 1] if h < halves - 1 else side_left
            sums.append(jnp.where(first, before, odd_right[h]) + values[2 * h + 1])
            sums.append(values[2 * h] + jnp.where(last, after, even_left[h]))
        sums.append(
            jnp.where(first, odd_right[-1], side_right) + jnp.where(last, even_left[0], side_left)
        )
        return sums

    def squares(parts, scales, acc):
        for part_sum, scale in zip(parts, scales):
            acc = acc + part_sum * scale
        return acc

    def grown(total, new, old):
        step = new - old
        return step * step if total is None else total + step * step

    def fine_tile(m, acc, f_in, q_ref, f_out, count):
        base = FINE_OFF + 16 * m
        upper, lower = pl.ds(base, SUB, stride=2), pl.ds(base + 1, SUB, stride=2)
        above, below = pl.ds(base - 1, SUB, stride=2), pl.ds(base + 2, SUB, stride=2)
        crow = COARSE_OFF + SUB * m
        q_here, q_up, q_down = pl.ds(crow, SUB), pl.ds(crow - 1, SUB), pl.ds(crow + 1, SUB)
        inv_top = [fi[t, upper, :] for t in range(count)]
        inv_low = [fi[t, lower, :] for t in range(count)]
        part_top, part_low = [None] * slabs, [None] * slabs
        for k in range(3):
            tops = [f_in[k, t, upper, :] for t in range(slabs + 1)]
            lows = [f_in[k, t, lower, :] for t in range(slabs + 1)]
            top_sum, low_sum = beside(tops), beside(lows)
            for t in range(count):
                three = 3.0 * q_ref[k, t, q_here, :]
                nb = (lows[t] + f_in[k, t, above, :]) + (top_sum[t] + q_ref[k, t, q_up, :])
                new = (f_a[3 + k, t, upper, :] + (nb + three)) * inv_top[t]
                f_out[k, t, upper, :] = new
                nb2 = (tops[t] + f_in[k, t, below, :]) + (low_sum[t] + q_ref[k, t, q_down, :])
                new2 = (f_a[3 + k, t, lower, :] + (nb2 + three)) * inv_low[t]
                f_out[k, t, lower, :] = new2
                if t < slabs:
                    part_top[t] = grown(part_top[t], new, tops[t])
                    part_low[t] = grown(part_low[t], new2, lows[t])
        acc = squares(part_top, [fd[t, upper, :] for t in range(slabs)], acc)
        return squares(part_low, [fd[t, lower, :] for t in range(slabs)], acc)

    def coarse_sum(m, k, t, f_in, c_ref, w_ref):
        base = FINE_OFF + 16 * m
        upper, lower = pl.ds(base, SUB, stride=2), pl.ds(base + 1, SUB, stride=2)
        if t == coarse_halo:
            four = f_in[k, halo, upper, :] + f_in[k, halo, lower, :]
            four = four + swapped_pairs(four)
        else:
            four = (f_in[k, 2 * t, upper, :] + f_in[k, 2 * t, lower, :]) + (
                f_in[k, 2 * t + 1, upper, :] + f_in[k, 2 * t + 1, lower, :]
            )
        return coarse_near(m, k, t, c_ref, w_ref) + 0.5 * four

    def coarse_step(m, k, t, added, inv):
        rows = pl.ds(coarse_row(m), SUB)
        if t == coarse_halo:
            known = ckh[k, rows, :]
        else:
            known = 4.0 * got_k[m + 1, k, :, pl.ds(LANES * t, LANES)]
        return (known + added) * inv

    def coarse_tile(m, acc, added_of, c_ref, count, use):
        rows = pl.ds(coarse_row(m), SUB)
        inv = [ci[t, rows, :] for t in range(count)]
        parts = [None] * halves
        for k in range(3):
            values = []
            for t in range(count):
                value = coarse_step(m, k, t, added_of(k, t), inv[t])
                values.append(value)
                if t < halves:
                    parts[t] = grown(parts[t], value, c_ref[k, t, rows, :])
            use(k, values)
        return squares(parts, [cd[t, rows, :] for t in range(halves)], acc)

    def near_sum(m, carry):
        base = FINE_OFF + 16 * m
        upper, lower = pl.ds(base, SUB, stride=2), pl.ds(base + 1, SUB, stride=2)
        above, below = pl.ds(base - 1, SUB, stride=2), pl.ds(base + 2, SUB, stride=2)
        for k in range(3):
            tops = [f_b[k, t, upper, :] for t in range(slabs + 1)]
            lows = [f_b[k, t, lower, :] for t in range(slabs + 1)]
            top_sum, low_sum = beside(tops), beside(lows)
            both = [tops[t] + lows[t] for t in range(slabs + 1)]
            for t in range(slabs + 1):
                nb = (lows[t] + f_b[k, t, above, :]) + top_sum[t]
                near[k, t, upper, :] = f_a[3 + k, t, upper, :] + nb
                nb2 = (tops[t] + f_b[k, t, below, :]) + low_sum[t]
                near[k, t, lower, :] = f_a[3 + k, t, lower, :] + nb2
            rows = pl.ds(coarse_row(m), SUB)
            for t in range(halves):
                pre_b[k, t, rows, :] = 0.5 * (both[2 * t] + both[2 * t + 1])
            side = both[halo]
            pre_b[k, coarse_halo, rows, :] = 0.5 * (side + swapped_pairs(side))
        return zero

    def second_fine(m, acc):
        base = FINE_OFF + 16 * m
        upper, lower = pl.ds(base, SUB, stride=2), pl.ds(base + 1, SUB, stride=2)
        crow = COARSE_OFF + SUB * m
        q_here, q_up, q_down = pl.ds(crow, SUB), pl.ds(crow - 1, SUB), pl.ds(crow + 1, SUB)
        for t in range(slabs + 1):
            inv_top, inv_low = fi[t, upper, :], fi[t, lower, :]
            part_top, part_low = None, None
            for k in range(3):
                three = 3.0 * q_b[k, t, q_here, :]
                new = (near[k, t, upper, :] + (three + q_b[k, t, q_up, :])) * inv_top
                f_a[k, t, upper, :] = new
                new2 = (near[k, t, lower, :] + (three + q_b[k, t, q_down, :])) * inv_low
                f_a[k, t, lower, :] = new2
                if t < slabs:
                    part_top = grown(part_top, new, f_b[k, t, upper, :])
                    part_low = grown(part_low, new2, f_b[k, t, lower, :])
            if t < slabs:
                acc = acc + (part_top * fd[t, upper, :] + part_low * fd[t, lower, :])
        return acc

    def coarse_near(m, k, t, c_ref, w_ref):
        crow = COARSE_OFF + SUB * m
        nb = c_ref[k, t, pl.ds(crow - 1, SUB), :] + c_ref[k, t, pl.ds(crow + 1, SUB), :]
        return nb + w_ref[k, t, pl.ds(coarse_row(m), SUB), :]

    def first_sum(m, carry):
        rows = pl.ds(coarse_row(m), SUB)
        for k in range(3):
            for t in range(halves + 1):
                pre[k, t, rows, :] = coarse_sum(m, k, t, f_a, c_a, w_a)
        return zero

    def first_coarse(m, acc):
        rows = pl.ds(coarse_row(m), SUB)

        def use(k, values):
            produce(k, coarse_row(m), values, c_b, q_b, w_b)

        return coarse_tile(m, acc, lambda k, t: pre[k, t, rows, :], c_a, halves + 1, use)

    def second_coarse(m, acc):
        rows = pl.ds(coarse_row(m), SUB)

        def added_of(k, t):
            return pre_b[k, t, rows, :] + coarse_near(m, k, t, c_b, w_b)

        def use(k, values):
            produce(k, coarse_row(m), values, c_a, q_a, w_a, inner=True)

        return coarse_tile(m, acc, added_of, c_b, halves + 1, use)

    def third_coarse(m, acc):
        def added_of(k, t):
            return coarse_sum(m, k, t, f_a, c_a, w_a)

        def use(k, values):
            for t, value in enumerate(values):
                fin[m, k, :, pl.ds(LANES * t, LANES)] = value

        return coarse_tile(m, acc, added_of, c_a, halves, use)

    def every_tile(body, acc, unroll=6):
        def step(n, acc):
            m = n - 1
            part_sum = body(m, zero)
            inner = jnp.where((n > 0) & (n <= tiles), 1.0, 0.0).astype(F32)
            return acc + part_sum * inner

        return lax.fori_loop(0, tiles + 2, step, acc, unroll=unroll)

    def fine_first(m, acc):
        return fine_tile(m, acc, f_a, q_a, f_b, slabs + 1)

    def fine_third(m, acc):
        return fine_tile(m, acc, f_a, q_a, f_b, slabs)

    def both_first(m, acc):
        first_sum(m, 0)
        return fine_first(m, acc)

    fine_sum1 = lax.fori_loop(1, tiles - 1, fine_first, zero, unroll=7)
    lax.fori_loop(1, tiles - 1, first_sum, zero, unroll=7)

    @pl.when(has_up)
    def _():
        row_down.wait_recv()

    @pl.when(has_down)
    def _():
        row_up.wait_recv()

    for row, held in (
        (FINE_OFF - 16, lane < 0),
        (FINE_OFF - 8, (lane >= 0) & has_up),
        (fine_end, (lane >= 0) & has_down),
        (fine_end + 8, lane < 0),
    ):
        diagonal(row, held)

    passed_on()
    lax.fori_loop(0, 2, lambda e, c: spread_first((gy + 1) * e, c), 0, unroll=2)

    def outer_first(e, acc):
        for n in range(2):
            m = jnp.where(e == 0, n - 1, tiles - 1 + n)
            part_sum = both_first(m, zero)
            if n == 0:
                acc = acc + jnp.where(e == 1, 1.0, 0.0).astype(F32) * part_sum
            else:
                acc = acc + jnp.where(e == 0, 1.0, 0.0).astype(F32) * part_sum
        return acc

    fine_sum1 = lax.fori_loop(0, 2, outer_first, fine_sum1, unroll=2)
    every_tile(near_sum, zero)

    for step in order:
        wait_step((2,), step)
    lax.fori_loop(1, gy + 1, spread_second, 0, unroll=8)
    strips_passed_on()
    lax.fori_loop(0, 2, lambda e, c: spread_second((gy + 1) * e, c), 0, unroll=2)

    coarse_sum1 = every_tile(first_coarse, zero, unroll=6)

    @pl.when(has_down)
    def _():
        row_down.wait_send()

    @pl.when(has_up)
    def _():
        row_up.wait_send()

    fine_sum2 = every_tile(second_fine, zero, unroll=3)
    coarse_sum2 = every_tile(second_coarse, zero, unroll=6)
    coarse_sum3 = lax.fori_loop(0, tiles, third_coarse, zero, unroll=4)

    my_cols = pl.ds(pl.multiple_of(j * wide, LANES), wide)
    finals = []
    for step in order:
        to = torus_add(j, step)
        copy = remote(
            fin.at[to], coarse_out.at[:, :, my_cols], fin_send.at[step], fin_recv.at[step], i, to
        )
        copy.start()
        finals.append(copy)
    for k in range(3):
        for t in range(halves):
            cols = pl.ds(pl.multiple_of(j * wide + LANES * t, LANES), LANES)
            coarse_out[k, :, cols] = fin[j, k, :, pl.ds(LANES * t, LANES)]

    fine_sum3 = lax.fori_loop(0, tiles, fine_third, zero, unroll=8)

    row_of = lax.broadcasted_iota(jnp.int32, (SUB, LANES), 0)
    mine = zero
    sums = ((fine_sum1, coarse_sum1), (fine_sum2, coarse_sum2), (fine_sum3, coarse_sum3))
    for s, (fine_part, coarse_part) in enumerate(sums):
        line = jnp.sum(fine_part + coarse_part, axis=0, keepdims=True)
        mine = jnp.where(row_of == s, line, mine)
    part[0] = mine
    norm_x = []
    for step in range(1, gx):
        copy = remote(
            part.at[0],
            part_gx.at[step],
            norm_send.at[0, step],
            norm_recv_x.at[step],
            lax.rem(i + step, gx),
            j,
        )
        copy.start()
        norm_x.append(copy)

    def join_columns(k, carry):
        for b in range(sh.blocks):
            rows = pl.ds(FINE_OFF + LANES * b, LANES)
            for s in range(slabs):
                begin = 2 * LANES * (s // 2) + s % 2
                swapped[b, pl.ds(begin, LANES, stride=2), :] = f_b[k, s, rows, :].T
            for t in range(slabs):
                natural = swapped[b, pl.ds(LANES * t, LANES), :].T
                fine_out[k, pl.ds(LANES * b, LANES), pl.ds(LANES * t, LANES)] = natural
        return carry

    lax.fori_loop(0, 3, join_columns, 0)

    for copy in norm_x:
        copy.wait_recv()
    for step in range(1, gx):
        mine = mine + part_gx[step]
    part[1] = mine
    norm_y = []
    for step in order:
        copy = remote(
            part.at[1],
            part_gy.at[step],
            norm_send.at[1, step],
            norm_recv_y.at[step],
            i,
            torus_add(j, step),
        )
        copy.start()
        norm_y.append(copy)
    for copy in norm_y:
        copy.wait_recv()
    for step in order:
        mine = mine + part_gy[step]
    total = jnp.sum(mine, axis=1, keepdims=True) * (1.0 / sh.cells)
    norm_out[...] = jnp.broadcast_to(jnp.sqrt(total), (SUB, LANES))

    @pl.when(has_right)
    def _():
        edge_right.wait_send()

    @pl.when(has_left)
    def _():
        edge_left.wait_send()

    @pl.when(has_down)
    def _():
        for kind in range(2):
            fwd_copies[kind][0].wait_send()
        strip_copies[0].wait_send()

    @pl.when(has_up)
    def _():
        for kind in range(2):
            fwd_copies[kind][1].wait_send()
        strip_copies[1].wait_send()

    for step in order:
        for copy in sends[step]:
            copy.wait_send()

    @pl.when((j == 0) | (j == gy - 1))
    def _():
        for step in order:
            strip_of(step, 0).wait_send()

    for copy in finals:
        copy.wait()
    for copy in norm_y + norm_x:
        copy.wait_send()


def store_kernel(fine, coarse, norms, fine_out, coarse_out, norm_out, scalars, sem):
    stores = [
        pltpu.make_async_copy(fine, fine_out, sem.at[0]),
        pltpu.make_async_copy(coarse, coarse_out, sem.at[1]),
        pltpu.make_async_copy(scalars, norm_out, sem.at[2]),
    ]
    stores[0].start()
    stores[1].start()
    for s in range(SWEEPS):
        scalars[s] = norms[s, 0]
    stores[2].start()
    for copy in stores:
        copy.wait()


def solution(mesh):
    gx, gy = mesh.shape["gx"], mesh.shape["gy"]

    def on_device(fine_start, fine_known, fine_mu, coarse_start, coarse_known, coarse_mu):
        sh = Shape(gx, gy, *fine_mu.shape)
        dma = pltpu.SemaphoreType.DMA
        in_hbm = pl.BlockSpec(memory_space=pltpu.HBM)
        on_chip = pl.BlockSpec(memory_space=pltpu.VMEM)

        def fine(*lead):
            return pltpu.VMEM((*lead, sh.slabs + 1, sh.fine_buf, LANES), F32)

        def coarse(*lead):
            return pltpu.VMEM((*lead, sh.coarse_buf, LANES), F32)

        few = sh.halves + 1
        fine_v, coarse_v, norm_v = pl.pallas_call(
            functools.partial(kernel, sh),
            out_shape=(
                pltpu.VMEM(fine_start.shape, F32),
                pltpu.VMEM(coarse_start.shape, F32),
                pltpu.VMEM((SUB, LANES), F32),
            ),
            in_specs=[in_hbm] * 6,
            out_specs=(on_chip, on_chip, on_chip),
            scratch_shapes=[
                pltpu.VMEM((PLANES, sh.slabs, sh.fine_rows, LANES), F32),
                pltpu.VMEM((PLANES, sh.blocks, sh.slabs * LANES, LANES), F32),
                pltpu.VMEM((sh.blocks, sh.slabs * LANES, LANES), F32),
                fine(PLANES),
                fine(3),
                fine(),
                fine(),
                coarse(3, few),
                coarse(3, few),
                coarse(3, sh.slabs + 1),
                coarse(3, sh.slabs + 1),
                coarse(3, few),
                coarse(3, few),
                coarse(3),
                coarse(few),
                coarse(few),
                coarse(3, few),
                coarse(3, few),
                fine(3),
                pltpu.VMEM((PLANES, SUB, gy * sh.wide), F32),
                pltpu.VMEM((PLANES, gy * SUB, LANES), F32),
                pltpu.VMEM((gy, SUB, LANES), F32),
                pltpu.VMEM((gy + 2, 3, SUB, sh.wide), F32),
                pltpu.VMEM((gy + 2, SUB, LANES), F32),
                pltpu.VMEM((gy + 2, 4, SUB, sh.wide), F32),
                pltpu.VMEM((gy, SUB, sh.wide), F32),
                pltpu.VMEM((2, SUB, sh.wide), F32),
                pltpu.VMEM((2, SUB, sh.wide), F32),
                pltpu.VMEM((2, PLANES, SUB, LANES), F32),
                pltpu.VMEM((2, PLANES, SUB, LANES), F32),
                pltpu.VMEM((gy, 3, SUB, sh.wide), F32),
                pltpu.VMEM((2, SUB, LANES), F32),
                pltpu.VMEM((gy, SUB, LANES), F32),
                pltpu.VMEM((gx, SUB, LANES), F32),
                dma((3 + 3 * sh.slabs,)),
                dma((2,)),
                dma((2,)),
                dma((2,)),
                dma((2,)),
                dma((3, gy)),
                dma((3, gy)),
                dma((2, 3)),
                dma((2, 3)),
                dma((gy,)),
                dma((2,)),
                dma((gy,)),
                dma((gy,)),
                dma((2, max(gx, gy))),
                dma((gy,)),
                dma((gx,)),
            ],
            compiler_params=pltpu.CompilerParams(
                collective_id=0, has_side_effects=True, vmem_limit_bytes=64_500_000
            ),
            name="interface_sweeps",
        )(fine_start, fine_known, fine_mu, coarse_start, coarse_known, coarse_mu)
        anywhere = pl.BlockSpec(memory_space=pl.ANY)
        return pl.pallas_call(
            store_kernel,
            out_shape=(
                jax.ShapeDtypeStruct(fine_start.shape, F32),
                jax.ShapeDtypeStruct(coarse_start.shape, F32),
                jax.ShapeDtypeStruct((SWEEPS,), F32),
            ),
            in_specs=[anywhere, anywhere, on_chip],
            out_specs=(in_hbm, in_hbm, in_hbm),
            scratch_shapes=[pltpu.SMEM((SWEEPS,), F32), dma((3,))],
            compiler_params=pltpu.CompilerParams(vmem_limit_bytes=1_000_000),
            name="store_results",
        )(fine_v, coarse_v, norm_v)

    return jax.shard_map(
        on_device,
        mesh=mesh,
        in_specs=(
            P(None, "gx", "gy"),
            P(None, "gx", "gy"),
            P("gx", "gy"),
            P(None, ("gx", "gy"), None),
            P(None, ("gx", "gy"), None),
            P(("gx", "gy"), None),
        ),
        out_specs=(P(None, "gx", "gy"), P(None, ("gx", "gy"), None), P(None)),
        check_vma=False,
    )
```

```python
import functools

import jax
import jax.numpy as jnp
from jax import lax
from jax.experimental import pallas as pl
from jax.experimental.pallas import tpu as pltpu
from jax.sharding import PartitionSpec as P

MESH = pl.DeviceIdType.MESH
F32 = jnp.float32
BF16 = jnp.bfloat16
SWEEPS = 3
LANES = 128
SUB = 8
FINE_OFF = 24
COARSE_OFF = 16
EDGE = 4
PLANES = 7


class Shape:
    def __init__(self, gx, gy, fine_rows, fine_cols):
        self.gx, self.gy = gx, gy
        self.fine_rows, self.fine_cols = fine_rows, fine_cols
        self.coarse_rows, self.wide = fine_rows // 2, fine_cols // 2
        self.tiles = self.coarse_rows // SUB
        self.halves = self.wide // LANES
        self.slabs = 2 * self.halves
        self.fine_buf = fine_rows + 2 * FINE_OFF
        self.coarse_buf = self.coarse_rows + 2 * COARSE_OFF + SUB
        self.blocks = fine_rows // LANES
        self.cells = 3.0 * gx * gy * fine_rows * fine_cols * 1.25


RING = 4


def hops(step):
    return sum(min(d, RING - d) for d in divmod(step, RING))


def far_first(count):
    return sorted(range(1, count), key=lambda step: -hops(step))


def torus_add(at, step):
    row, column = at // RING + step // RING, lax.rem(at, RING) + step % RING
    return lax.rem(row, RING) * RING + lax.rem(column, RING)


def torus_back(at, step):
    row, column = at // RING + RING - step // RING, lax.rem(at, RING) + RING - step % RING
    return lax.rem(row, RING) * RING + lax.rem(column, RING)


def lane_iota():
    return lax.broadcasted_iota(jnp.int32, (SUB, LANES), 1)


def exact_dot(values, table):
    high = values.astype(BF16)
    rest = values - high.astype(F32)
    middle = rest.astype(BF16)
    low = (rest - middle.astype(F32)).astype(BF16)
    total = jnp.dot(high, table, preferred_element_type=F32)
    total = total + jnp.dot(middle, table, preferred_element_type=F32)
    return total + jnp.dot(low, table, preferred_element_type=F32)


def kernel(
    sh,
    fine_start,
    fine_known,
    fine_mu,
    coarse_start,
    coarse_known,
    coarse_mu,
    fine_out,
    coarse_out,
    norm_out,
    nat,
    turned,
    swapped,
    f_a,
    f_b,
    fd,
    fi,
    c_a,
    c_b,
    q_a,
    q_b,
    w_a,
    w_b,
    ckh,
    cd,
    ci,
    pre,
    pre_b,
    near,
    own,
    comb,
    pack,
    got_c,
    got_p,
    got_k,
    strip_out,
    strip_in,
    strip_far,
    edge_out,
    edge_in,
    fin,
    part,
    part_gy,
    part_gx,
    load_sem,
    edge_send,
    edge_recv,
    row_send,
    row_recv,
    a_send,
    a_recv,
    fwd_send,
    fwd_recv,
    strip_send,
    strip_recv,
    fin_send,
    fin_recv,
    norm_send,
    norm_recv_y,
    norm_recv_x,
):
    gx, gy = sh.gx, sh.gy
    i = lax.axis_index("gx")
    j = lax.axis_index("gy")
    halves, slabs, tiles, wide = sh.halves, sh.slabs, sh.tiles, sh.wide
    halo, coarse_halo = slabs, halves
    lane = lane_iota()
    even = lane % 2 == 0
    first = lane == 0
    last = lane == LANES - 1
    has_up, has_down = i > 0, i < gx - 1
    has_left, has_right = j > 0, j < gy - 1

    def remote(src, dst, send, recv, to_i, to_j):
        return pltpu.make_async_remote_copy(
            src_ref=src,
            dst_ref=dst,
            send_sem=send,
            recv_sem=recv,
            device_id=(to_i, to_j),
            device_id_type=MESH,
        )

    loads = []

    def load(src, dst):
        copy = pltpu.make_async_copy(src, dst, load_sem.at[len(loads)])
        copy.start()
        loads.append(copy)
        return copy

    own_loads = [
        load(coarse_start, own.at[pl.ds(0, 3)]),
        load(coarse_known, own.at[pl.ds(3, 3)]),
        load(coarse_mu, own.at[6]),
    ]
    fine_loads = []
    for t in [0, slabs - 1] + list(range(1, slabs - 1)):
        cols = pl.ds(LANES * t, LANES)
        fine_loads.append(load(fine_start.at[:, :, cols], nat.at[pl.ds(0, 3), t]))
        fine_loads.append(load(fine_known.at[:, :, cols], nat.at[pl.ds(3, 3), t]))
        fine_loads.append(load(fine_mu.at[:, cols], nat.at[6, t]))

    barrier = pltpu.get_barrier_semaphore()
    for step in far_first(gy):
        pl.semaphore_signal(
            barrier, inc=1, device_id=(i, torus_add(j, step)), device_id_type=MESH
        )
    for step in range(1, gx):
        pl.semaphore_signal(
            barrier, inc=1, device_id=(lax.rem(i + step, gx), j), device_id_type=MESH
        )

    zero = jnp.zeros((SUB, LANES), F32)
    fine_end = FINE_OFF + sh.fine_rows
    for t in range(slabs + 1):
        for row in (0, 8, fine_end + 8, fine_end + 16):
            for p in range(PLANES):
                f_a[p, t, pl.ds(row, SUB), :] = zero
        for k in range(3):
            for row in (0, fine_end + 16):
                f_b[k, t, pl.ds(row, SUB), :] = zero
            for row in (0, sh.coarse_buf - 8):
                q_a[k, t, pl.ds(row, SUB), :] = zero
                q_b[k, t, pl.ds(row, SUB), :] = zero
                if t <= halves:
                    c_a[k, t, pl.ds(row, SUB), :] = zero
                    c_b[k, t, pl.ds(row, SUB), :] = zero

    for slot in (0, gy + 1):
        for u in range(halves):
            for p in range(4):
                got_k[slot, p, :, pl.ds(LANES * u, LANES)] = zero

    def clear_rows(row, slot):
        for p in range(PLANES):
            for t in range(slabs + 1):
                f_a[p, t, pl.ds(row, SUB), :] = zero
        got_p[slot] = zero
        for u in range(halves):
            for p in range(3):
                got_c[slot, p, :, pl.ds(LANES * u, LANES)] = zero

    def clear_columns(side):
        for p in range(PLANES):
            edge_in[side, p] = zero

    pl.when(i == 0)(lambda: clear_rows(FINE_OFF - SUB, 0))
    pl.when(i == gx - 1)(lambda: clear_rows(fine_end, gy + 1))
    pl.when(j == 0)(lambda: clear_columns(0))
    pl.when(j == gy - 1)(lambda: clear_columns(1))

    for copy in own_loads:
        copy.wait()

    for dest in range(gy):
        for p in range(PLANES):
            after = own[p, :, pl.ds((dest + 1) * wide, LANES)] if dest < gy - 1 else zero
            before = own[p, :, pl.ds(dest * wide - LANES, LANES)] if dest > 0 else zero
            comb[p, pl.ds(SUB * dest, SUB), :] = jnp.where(lane < 64, after, before)
    source = lax.broadcasted_iota(jnp.int32, (LANES, LANES), 0)
    target = lax.broadcasted_iota(jnp.int32, (LANES, LANES), 1)
    inside = target % 16
    wanted = jnp.where(inside < 8, LANES - EDGE + inside // 2, (inside - 8) // 2)
    packed = None
    for p in range(PLANES):
        table = ((source == wanted) & (target // 16 == p)).astype(F32).astype(BF16)
        piece = exact_dot(comb[p], table)
        packed = piece if packed is None else packed + piece
    for dest in range(gy):
        pack[dest] = packed[SUB * dest : SUB * (dest + 1), :]

    def pack_strip(begin):
        for dest in range(gy):
            for p in range(4):
                piece = own[3 + p, begin : begin + 2, pl.ds(dest * wide, wide)]
                strip_out[dest, pl.ds(2 * p, 2), :] = piece

    pl.when(j == gy - 1)(lambda: pack_strip(SUB - 2))
    pl.when(j == 0)(lambda: pack_strip(0))

    for copy in fine_loads:
        copy.wait()

    def turn_edges(p, carry):
        for b in range(sh.blocks):
            rows = pl.ds(LANES * b, LANES)
            low = nat[p, 0, rows, :].T
            high = nat[p, slabs - 1, rows, :].T
            turned[p, b, pl.ds(0, LANES), :] = low
            turned[p, b, pl.ds(LANES * (slabs - 1), LANES), :] = high
            edge_out[0, p, pl.ds(EDGE * b, EDGE), :] = high[LANES - EDGE :, :]
            edge_out[1, p, pl.ds(EDGE * b, EDGE), :] = low[:EDGE, :]
        return carry

    lax.fori_loop(0, PLANES, turn_edges, 0, unroll=PLANES)

    pl.semaphore_wait(barrier, gy + gx - 2)

    edge_right = remote(
        edge_out.at[0], edge_in.at[0], edge_send.at[0], edge_recv.at[0], i, lax.rem(j + 1, gy)
    )
    edge_left = remote(
        edge_out.at[1], edge_in.at[1], edge_send.at[1], edge_recv.at[1], i, lax.rem(j + gy - 1, gy)
    )

    @pl.when(has_right)
    def _():
        edge_right.start()

    @pl.when(has_left)
    def _():
        edge_left.start()

    def sends_of(step):
        to = torus_add(j, step)
        cols = pl.ds(pl.multiple_of(to * wide, LANES), wide)
        ends = (
            (own.at[pl.ds(0, 3), :, cols], got_c),
            (pack.at[to], got_p),
            (own.at[pl.ds(3, 4), :, cols], got_k),
        )
        return [
            remote(src, dst.at[j + 1], a_send.at[n, step], a_recv.at[n, step], i, to)
            for n, (src, dst) in enumerate(ends)
        ]

    order = far_first(gy)
    sends = {step: sends_of(step) for step in order}
    def strip_of(step, side):
        to = torus_add(j, step)
        return remote(
            strip_out.at[to], strip_in.at[side], strip_send.at[step], strip_recv.at[side], i, to
        )

    for step in order:
        sends[step][0].start()
        sends[step][1].start()

    def send_strips(side):
        for step in order:
            strip_of(step, side).start()
        strip_in[side] = strip_out[j]

    pl.when(j == gy - 1)(lambda: send_strips(0))
    pl.when(j == 0)(lambda: send_strips(1))

    got_p[j + 1] = pack[j]
    for u in range(halves):
        cols = pl.ds(pl.multiple_of(j * wide + LANES * u, LANES), LANES)
        for p in range(PLANES):
            piece = own[p, :, cols]
            if p < 3:
                got_c[j + 1, p, :, pl.ds(LANES * u, LANES)] = piece
            else:
                got_k[j + 1, p - 3, :, pl.ds(LANES * u, LANES)] = piece

    def scale_of(p):
        return jnp.where((p >= 3) & (p < 6), 4.0, 1.0).astype(F32)

    def split_columns(p, carry):
        scale = scale_of(p)
        for b in range(sh.blocks):
            rows = pl.ds(LANES * b, LANES)
            for t in range(1, slabs - 1):
                turned[p, b, pl.ds(LANES * t, LANES), :] = nat[p, t, rows, :].T
        for b in range(sh.blocks):
            rows = pl.ds(FINE_OFF + LANES * b, LANES)
            for s in range(slabs):
                begin = 2 * LANES * (s // 2) + s % 2
                f_a[p, s, rows, :] = turned[p, b, pl.ds(begin, LANES, stride=2), :].T * scale
        return carry

    lax.fori_loop(0, PLANES, split_columns, 0)

    @pl.when(has_left)
    def _():
        edge_right.wait_recv()

    @pl.when(has_right)
    def _():
        edge_left.wait_recv()

    between = jnp.zeros((LANES - 2 * EDGE, LANES), F32)

    def unpack_edges(p, carry):
        for b in range(sh.blocks):
            from_left = edge_in[0, p, pl.ds(EDGE * b, EDGE), :]
            from_right = edge_in[1, p, pl.ds(EDGE * b, EDGE), :]
            slab = jnp.concatenate([from_right, between, from_left], axis=0).T * scale_of(p)
            f_a[p, halo, pl.ds(FINE_OFF + LANES * b, LANES), :] = slab
        return carry

    lax.fori_loop(0, PLANES, unpack_edges, 0, unroll=PLANES)

    down_i, up_i = lax.rem(i + 1, gx), lax.rem(i + gx - 1, gx)
    row_down = remote(
        f_a.at[:, :, pl.ds(fine_end - SUB, SUB), :],
        f_a.at[:, :, pl.ds(FINE_OFF - SUB, SUB), :],
        row_send.at[0],
        row_recv.at[0],
        down_i,
        j,
    )
    row_up = remote(
        f_a.at[:, :, pl.ds(FINE_OFF, SUB), :],
        f_a.at[:, :, pl.ds(fine_end, SUB), :],
        row_send.at[1],
        row_recv.at[1],
        up_i,
        j,
    )

    @pl.when(has_down)
    def _():
        row_down.start()

    @pl.when(has_up)
    def _():
        row_up.start()

    def coarse_row(m):
        return pl.multiple_of(COARSE_OFF + SUB * m, SUB)

    def halo_of(slot, p):
        return pltpu.roll(got_p[slot], (LANES - (16 * p + 8)) % LANES, 1)

    def swapped_pairs(value):
        return jnp.where(even, pltpu.roll(value, LANES - 1, 1), pltpu.roll(value, 1, 1))

    def produce(k, row, values, c_ref, q_ref, w_ref, inner=False):
        right = [pltpu.roll(v, 1, 1) for v in values]
        left = [pltpu.roll(v, LANES - 1, 1) for v in values]
        rows = pl.ds(row, SUB)
        count = len(values)
        for t, value in enumerate(values):
            if t == coarse_halo and inner:
                continue
            before = jnp.where(first, right[t - 1], right[t])
            after = jnp.where(last, left[(t + 1) % count], left[t])
            c_ref[k, t, rows, :] = value
            main = 0.375 * value
            if t == coarse_halo:
                outer = jnp.where(even, before, after)
                q_ref[k, halo, rows, :] = main + 0.125 * outer
                w_ref[k, t, rows, :] = outer + swapped_pairs(outer)
            else:
                q_ref[k, 2 * t, rows, :] = main + 0.125 * before
                q_ref[k, 2 * t + 1, rows, :] = main + 0.125 * after
                w_ref[k, t, rows, :] = before + after

    def spread_first(slot, carry):
        for k in range(3):
            values = [got_c[slot, k, :, pl.ds(LANES * t, LANES)] for t in range(halves)]
            values.append(halo_of(slot, k))
            produce(k, coarse_row(slot - 1), values, c_a, q_a, w_a)
        return carry

    halo_lanes = ((lane < 2 * EDGE) & has_right) | ((lane >= LANES - 2 * EDGE) & has_left)
    halo_lanes_fine = ((lane < EDGE) & has_right) | ((lane >= LANES - EDGE) & has_left)

    def spread_second(slot, carry):
        rows = pl.ds(coarse_row(slot - 1), SUB)
        held = ((slot > 0) | has_up) & ((slot <= gy) | has_down)
        for k in range(3):
            ckh[k, rows, :] = 4.0 * halo_of(slot, 3 + k)
        for t in range(halves + 1):
            if t == coarse_halo:
                value, valid = halo_of(slot, 6), halo_lanes & held
            else:
                value, valid = got_k[slot, 3, :, pl.ds(LANES * t, LANES)], (lane >= 0) & held
            diag = value + 1.0
            cd[t, rows, :] = diag * diag
            ci[t, rows, :] = jnp.where(valid, 0.25 * (1.0 / diag), 0.0)
        return carry

    fwd_copies = {}
    for n, ref in enumerate((got_c, got_p)):
        fwd_copies[n] = (
            remote(ref.at[gy], ref.at[0], fwd_send.at[0, n], fwd_recv.at[0, n], down_i, j),
            remote(ref.at[1], ref.at[gy + 1], fwd_send.at[1, n], fwd_recv.at[1, n], up_i, j),
        )

    strip_copies = (
        remote(strip_in.at[0], strip_far.at[0], fwd_send.at[0, 2], fwd_recv.at[0, 2], down_i, j),
        remote(strip_in.at[1], strip_far.at[1], fwd_send.at[1, 2], fwd_recv.at[1, 2], up_i, j),
    )

    def pass_strips_on():
        pl.when(j < gy - 1)(lambda: strip_of(1, 0).wait_recv())
        pl.when(has_down)(lambda: strip_copies[0].start())
        pl.when(j > 0)(lambda: strip_of(1, 1).wait_recv())
        pl.when(has_up)(lambda: strip_copies[1].start())

    def strips_passed_on():
        @pl.when(has_up)
        def _():
            strip_copies[0].wait_recv()
            for p in range(4):
                got_k[0, p, pl.ds(SUB - 2, 2), :] = strip_far[0, pl.ds(2 * p, 2), :]

        @pl.when(has_down)
        def _():
            strip_copies[1].wait_recv()
            for p in range(4):
                got_k[gy + 1, p, pl.ds(0, 2), :] = strip_far[1, pl.ds(2 * p, 2), :]

    def wait_step(kinds, step):
        source = torus_back(j, step)
        for kind in kinds:
            dst = (got_c, got_p, got_k)[kind].at[source + 1]
            remote(dst, dst, a_send.at[kind, step], a_recv.at[kind, step], i, source).wait_recv()

    def pass_on(source):
        @pl.when((source == gy - 1) & has_down)
        def _():
            fwd_copies[0][0].start()
            fwd_copies[1][0].start()

        @pl.when((source == 0) & has_up)
        def _():
            fwd_copies[0][1].start()
            fwd_copies[1][1].start()

    def passed_on():
        @pl.when(has_up)
        def _():
            fwd_copies[0][0].wait_recv()
            fwd_copies[1][0].wait_recv()

        @pl.when(has_down)
        def _():
            fwd_copies[0][1].wait_recv()
            fwd_copies[1][1].wait_recv()

    def diagonal(row, held):
        rows = pl.ds(row, SUB)
        for t in range(slabs + 1):
            diag = f_a[6, t, rows, :] + 1.0
            valid = (halo_lanes_fine if t == halo else (lane >= 0)) & held
            fd[t, rows, :] = diag * diag
            fi[t, rows, :] = jnp.where(valid, 0.25 * (1.0 / diag), 0.0)

    def diagonals(step, carry):
        for n in range(4):
            diagonal(pl.multiple_of(FINE_OFF + SUB * (4 * step + n), SUB), lane >= 0)
        return carry

    lax.fori_loop(0, sh.fine_rows // (4 * SUB), diagonals, 0)

    group = 4
    for begin in range(0, gy, group):
        if begin == gy // 2:
            for step in order:
                sends[step][2].start()
        sources = []
        for step in ([0] + order)[begin : begin + group]:
            source = torus_back(j, step) if step else j
            if step:
                wait_step((0, 1), step)
            pass_on(source)
            sources.append(source)
        for source in sources:
            spread_first(source + 1, 0)
    pass_strips_on()

    def beside(values):
        side = values[halo]
        odd_right = [pltpu.roll(values[2 * h + 1], 1, 1) for h in range(halves)]
        even_left = [pltpu.roll(values[2 * h], LANES - 1, 1) for h in range(halves)]
        side_right, side_left = pltpu.roll(side, 1, 1), pltpu.roll(side, LANES - 1, 1)
        sums = []
        for h in range(halves):
            before = odd_right[h - 1] if h > 0 else side_right
            after = even_left[h + 1] if h < halves - 1 else side_left
            sums.append(jnp.where(first, before, odd_right[h]) + values[2 * h + 1])
            sums.append(values[2 * h] + jnp.where(last, after, even_left[h]))
        sums.append(
            jnp.where(first, odd_right[-1], side_right) + jnp.where(last, even_left[0], side_left)
        )
        return sums

    def squares(parts, scales, acc):
        for part_sum, scale in zip(parts, scales):
            acc = acc + part_sum * scale
        return acc

    def grown(total, new, old):
        step = new - old
        return step * step if total is None else total + step * step

    def fine_tile(m, acc, f_in, q_ref, f_out, count):
        base = FINE_OFF + 16 * m
        upper, lower = pl.ds(base, SUB, stride=2), pl.ds(base + 1, SUB, stride=2)
        above, below = pl.ds(base - 1, SUB, stride=2), pl.ds(base + 2, SUB, stride=2)
        crow = COARSE_OFF + SUB * m
        q_here, q_up, q_down = pl.ds(crow, SUB), pl.ds(crow - 1, SUB), pl.ds(crow + 1, SUB)
        inv_top = [fi[t, upper, :] for t in range(count)]
        inv_low = [fi[t, lower, :] for t in range(count)]
        part_top, part_low = [None] * slabs, [None] * slabs
        for k in range(3):
            tops = [f_in[k, t, upper, :] for t in range(slabs + 1)]
            lows = [f_in[k, t, lower, :] for t in range(slabs + 1)]
            top_sum, low_sum = beside(tops), beside(lows)
            for t in range(count):
                three = 3.0 * q_ref[k, t, q_here, :]
                nb = (lows[t] + f_in[k, t, above, :]) + (top_sum[t] + q_ref[k, t, q_up, :])
                new = (f_a[3 + k, t, upper, :] + (nb + three)) * inv_top[t]
                f_out[k, t, upper, :] = new
                nb2 = (tops[t] + f_in[k, t, below, :]) + (low_sum[t] + q_ref[k, t, q_down, :])
                new2 = (f_a[3 + k, t, lower, :] + (nb2 + three)) * inv_low[t]
                f_out[k, t, lower, :] = new2
                if t < slabs:
                    part_top[t] = grown(part_top[t], new, tops[t])
                    part_low[t] = grown(part_low[t], new2, lows[t])
        acc = squares(part_top, [fd[t, upper, :] for t in range(slabs)], acc)
        return squares(part_low, [fd[t, lower, :] for t in range(slabs)], acc)

    def coarse_sum(m, k, t, f_in, c_ref, w_ref):
        base = FINE_OFF + 16 * m
        upper, lower = pl.ds(base, SUB, stride=2), pl.ds(base + 1, SUB, stride=2)
        if t == coarse_halo:
            four = f_in[k, halo, upper, :] + f_in[k, halo, lower, :]
            four = four + swapped_pairs(four)
        else:
            four = (f_in[k, 2 * t, upper, :] + f_in[k, 2 * t, lower, :]) + (
                f_in[k, 2 * t + 1, upper, :] + f_in[k, 2 * t + 1, lower, :]
            )
        return coarse_near(m, k, t, c_ref, w_ref) + 0.5 * four

    def coarse_step(m, k, t, added, inv):
        rows = pl.ds(coarse_row(m), SUB)
        if t == coarse_halo:
            known = ckh[k, rows, :]
        else:
            known = 4.0 * got_k[m + 1, k, :, pl.ds(LANES * t, LANES)]
        return (known + added) * inv

    def coarse_tile(m, acc, added_of, c_ref, count, use):
        rows = pl.ds(coarse_row(m), SUB)
        inv = [ci[t, rows, :] for t in range(count)]
        parts = [None] * halves
        for k in range(3):
            values = []
            for t in range(count):
                value = coarse_step(m, k, t, added_of(k, t), inv[t])
                values.append(value)
                if t < halves:
                    parts[t] = grown(parts[t], value, c_ref[k, t, rows, :])
            use(k, values)
        return squares(parts, [cd[t, rows, :] for t in range(halves)], acc)

    def near_sum(m, carry):
        base = FINE_OFF + 16 * m
        upper, lower = pl.ds(base, SUB, stride=2), pl.ds(base + 1, SUB, stride=2)
        above, below = pl.ds(base - 1, SUB, stride=2), pl.ds(base + 2, SUB, stride=2)
        for k in range(3):
            tops = [f_b[k, t, upper, :] for t in range(slabs + 1)]
            lows = [f_b[k, t, lower, :] for t in range(slabs + 1)]
            top_sum, low_sum = beside(tops), beside(lows)
            both = [tops[t] + lows[t] for t in range(slabs + 1)]
            for t in range(slabs + 1):
                nb = (lows[t] + f_b[k, t, above, :]) + top_sum[t]
                near[k, t, upper, :] = f_a[3 + k, t, upper, :] + nb
                nb2 = (tops[t] + f_b[k, t, below, :]) + low_sum[t]
                near[k, t, lower, :] = f_a[3 + k, t, lower, :] + nb2
            rows = pl.ds(coarse_row(m), SUB)
            for t in range(halves):
                pre_b[k, t, rows, :] = 0.5 * (both[2 * t] + both[2 * t + 1])
            side = both[halo]
            pre_b[k, coarse_halo, rows, :] = 0.5 * (side + swapped_pairs(side))
        return zero

    def second_fine(m, acc):
        base = FINE_OFF + 16 * m
        upper, lower = pl.ds(base, SUB, stride=2), pl.ds(base + 1, SUB, stride=2)
        crow = COARSE_OFF + SUB * m
        q_here, q_up, q_down = pl.ds(crow, SUB), pl.ds(crow - 1, SUB), pl.ds(crow + 1, SUB)
        for t in range(slabs + 1):
            inv_top, inv_low = fi[t, upper, :], fi[t, lower, :]
            part_top, part_low = None, None
            for k in range(3):
                three = 3.0 * q_b[k, t, q_here, :]
                new = (near[k, t, upper, :] + (three + q_b[k, t, q_up, :])) * inv_top
                f_a[k, t, upper, :] = new
                new2 = (near[k, t, lower, :] + (three + q_b[k, t, q_down, :])) * inv_low
                f_a[k, t, lower, :] = new2
                if t < slabs:
                    part_top = grown(part_top, new, f_b[k, t, upper, :])
                    part_low = grown(part_low, new2, f_b[k, t, lower, :])
            if t < slabs:
                acc = acc + (part_top * fd[t, upper, :] + part_low * fd[t, lower, :])
        return acc

    def coarse_near(m, k, t, c_ref, w_ref):
        crow = COARSE_OFF + SUB * m
        nb = c_ref[k, t, pl.ds(crow - 1, SUB), :] + c_ref[k, t, pl.ds(crow + 1, SUB), :]
        return nb + w_ref[k, t, pl.ds(coarse_row(m), SUB), :]

    def first_sum(m, carry):
        rows = pl.ds(coarse_row(m), SUB)
        for k in range(3):
            for t in range(halves + 1):
                pre[k, t, rows, :] = coarse_sum(m, k, t, f_a, c_a, w_a)
        return zero

    def first_coarse(m, acc):
        rows = pl.ds(coarse_row(m), SUB)

        def use(k, values):
            produce(k, coarse_row(m), values, c_b, q_b, w_b)

        return coarse_tile(m, acc, lambda k, t: pre[k, t, rows, :], c_a, halves + 1, use)

    def second_coarse(m, acc):
        rows = pl.ds(coarse_row(m), SUB)

        def added_of(k, t):
            return pre_b[k, t, rows, :] + coarse_near(m, k, t, c_b, w_b)

        def use(k, values):
            produce(k, coarse_row(m), values, c_a, q_a, w_a, inner=True)

        return coarse_tile(m, acc, added_of, c_b, halves + 1, use)

    def third_coarse(m, acc):
        def added_of(k, t):
            return coarse_sum(m, k, t, f_a, c_a, w_a)

        def use(k, values):
            for t, value in enumerate(values):
                fin[m, k, :, pl.ds(LANES * t, LANES)] = value

        return coarse_tile(m, acc, added_of, c_a, halves, use)

    def every_tile(body, acc, unroll=6):
        def step(n, acc):
            m = n - 1
            part_sum = body(m, zero)
            inner = jnp.where((n > 0) & (n <= tiles), 1.0, 0.0).astype(F32)
            return acc + part_sum * inner

        return lax.fori_loop(0, tiles + 2, step, acc, unroll=unroll)

    def fine_first(m, acc):
        return fine_tile(m, acc, f_a, q_a, f_b, slabs + 1)

    def fine_third(m, acc):
        return fine_tile(m, acc, f_a, q_a, f_b, slabs)

    def both_first(m, acc):
        first_sum(m, 0)
        return fine_first(m, acc)

    fine_sum1 = lax.fori_loop(1, tiles - 1, fine_first, zero, unroll=7)
    lax.fori_loop(1, tiles - 1, first_sum, zero, unroll=7)

    @pl.when(has_up)
    def _():
        row_down.wait_recv()

    @pl.when(has_down)
    def _():
        row_up.wait_recv()

    for row, held in (
        (FINE_OFF - 16, lane < 0),
        (FINE_OFF - 8, (lane >= 0) & has_up),
        (fine_end, (lane >= 0) & has_down),
        (fine_end + 8, lane < 0),
    ):
        diagonal(row, held)

    passed_on()
    lax.fori_loop(0, 2, lambda e, c: spread_first((gy + 1) * e, c), 0, unroll=2)

    def outer_first(e, acc):
        for n in range(2):
            m = jnp.where(e == 0, n - 1, tiles - 1 + n)
            part_sum = both_first(m, zero)
            if n == 0:
                acc = acc + jnp.where(e == 1, 1.0, 0.0).astype(F32) * part_sum
            else:
                acc = acc + jnp.where(e == 0, 1.0, 0.0).astype(F32) * part_sum
        return acc

    fine_sum1 = lax.fori_loop(0, 2, outer_first, fine_sum1, unroll=2)
    every_tile(near_sum, zero)

    for step in order:
        wait_step((2,), step)
    lax.fori_loop(1, gy + 1, spread_second, 0, unroll=8)
    strips_passed_on()
    lax.fori_loop(0, 2, lambda e, c: spread_second((gy + 1) * e, c), 0, unroll=2)

    @pl.when(has_down)
    def _():
        row_down.wait_send()

    @pl.when(has_up)
    def _():
        row_up.wait_send()

    def inner_share(m):
        return jnp.where((m >= 0) & (m < tiles), 1.0, 0.0).astype(F32)

    def lead(m, sums):
        share = inner_share(m)
        return (sums[0] + share * first_coarse(m, zero), sums[1], sums[2])

    def follow(m, sums):
        share = inner_share(m)
        fine_part = second_fine(m, zero)
        coarse_part = second_coarse(m, zero)
        return (sums[0], sums[1] + share * fine_part, sums[2] + share * coarse_part)

    def lead_and_follow(m, sums):
        return lead(m + 1, follow(m - 1, sums))

    sums = lax.fori_loop(-1, 1, lead, (zero, zero, zero), unroll=2)
    sums = lax.fori_loop(0, tiles, lead_and_follow, sums, unroll=4)
    sums = lax.fori_loop(tiles - 1, tiles + 1, follow, sums, unroll=2)
    coarse_sum1, fine_sum2, coarse_sum2 = sums
    coarse_sum3 = lax.fori_loop(0, tiles, third_coarse, zero, unroll=4)

    my_cols = pl.ds(pl.multiple_of(j * wide, LANES), wide)
    finals = []
    for step in order:
        to = torus_add(j, step)
        copy = remote(
            fin.at[to], coarse_out.at[:, :, my_cols], fin_send.at[step], fin_recv.at[step], i, to
        )
        copy.start()
        finals.append(copy)
    for k in range(3):
        for t in range(halves):
            cols = pl.ds(pl.multiple_of(j * wide + LANES * t, LANES), LANES)
            coarse_out[k, :, cols] = fin[j, k, :, pl.ds(LANES * t, LANES)]

    fine_sum3 = lax.fori_loop(0, tiles, fine_third, zero, unroll=8)

    row_of = lax.broadcasted_iota(jnp.int32, (SUB, LANES), 0)
    mine = zero
    sums = ((fine_sum1, coarse_sum1), (fine_sum2, coarse_sum2), (fine_sum3, coarse_sum3))
    for s, (fine_part, coarse_part) in enumerate(sums):
        line = jnp.sum(fine_part + coarse_part, axis=0, keepdims=True)
        mine = jnp.where(row_of == s, line, mine)
    part[0] = mine
    norm_x = []
    for step in range(1, gx):
        copy = remote(
            part.at[0],
            part_gx.at[step],
            norm_send.at[0, step],
            norm_recv_x.at[step],
            lax.rem(i + step, gx),
            j,
        )
        copy.start()
        norm_x.append(copy)

    def join_columns(k, carry):
        for b in range(sh.blocks):
            rows = pl.ds(FINE_OFF + LANES * b, LANES)
            for s in range(slabs):
                begin = 2 * LANES * (s // 2) + s % 2
                swapped[b, pl.ds(begin, LANES, stride=2), :] = f_b[k, s, rows, :].T
            for t in range(slabs):
                natural = swapped[b, pl.ds(LANES * t, LANES), :].T
                fine_out[k, pl.ds(LANES * b, LANES), pl.ds(LANES * t, LANES)] = natural
        return carry

    lax.fori_loop(0, 3, join_columns, 0)

    for copy in norm_x:
        copy.wait_recv()
    for step in range(1, gx):
        mine = mine + part_gx[step]
    part[1] = mine
    norm_y = []
    for step in order:
        copy = remote(
            part.at[1],
            part_gy.at[step],
            norm_send.at[1, step],
            norm_recv_y.at[step],
            i,
            torus_add(j, step),
        )
        copy.start()
        norm_y.append(copy)
    for copy in norm_y:
        copy.wait_recv()
    for step in order:
        mine = mine + part_gy[step]
    total = jnp.sum(mine, axis=1, keepdims=True) * (1.0 / sh.cells)
    norm_out[...] = jnp.broadcast_to(jnp.sqrt(total), (SUB, LANES))

    @pl.when(has_right)
    def _():
        edge_right.wait_send()

    @pl.when(has_left)
    def _():
        edge_left.wait_send()

    @pl.when(has_down)
    def _():
        for kind in range(2):
            fwd_copies[kind][0].wait_send()
        strip_copies[0].wait_send()

    @pl.when(has_up)
    def _():
        for kind in range(2):
            fwd_copies[kind][1].wait_send()
        strip_copies[1].wait_send()

    for step in order:
        for copy in sends[step]:
            copy.wait_send()

    @pl.when((j == 0) | (j == gy - 1))
    def _():
        for step in order:
            strip_of(step, 0).wait_send()

    for copy in finals:
        copy.wait()
    for copy in norm_y + norm_x:
        copy.wait_send()


def store_kernel(fine, coarse, norms, fine_out, coarse_out, norm_out, scalars, sem):
    stores = [
        pltpu.make_async_copy(fine, fine_out, sem.at[0]),
        pltpu.make_async_copy(coarse, coarse_out, sem.at[1]),
        pltpu.make_async_copy(scalars, norm_out, sem.at[2]),
    ]
    stores[0].start()
    stores[1].start()
    for s in range(SWEEPS):
        scalars[s] = norms[s, 0]
    stores[2].start()
    for copy in stores:
        copy.wait()


def solution(mesh):
    gx, gy = mesh.shape["gx"], mesh.shape["gy"]

    def on_device(fine_start, fine_known, fine_mu, coarse_start, coarse_known, coarse_mu):
        sh = Shape(gx, gy, *fine_mu.shape)
        dma = pltpu.SemaphoreType.DMA
        in_hbm = pl.BlockSpec(memory_space=pltpu.HBM)
        on_chip = pl.BlockSpec(memory_space=pltpu.VMEM)

        def fine(*lead):
            return pltpu.VMEM((*lead, sh.slabs + 1, sh.fine_buf, LANES), F32)

        def coarse(*lead):
            return pltpu.VMEM((*lead, sh.coarse_buf, LANES), F32)

        few = sh.halves + 1
        fine_v, coarse_v, norm_v = pl.pallas_call(
            functools.partial(kernel, sh),
            out_shape=(
                pltpu.VMEM(fine_start.shape, F32),
                pltpu.VMEM(coarse_start.shape, F32),
                pltpu.VMEM((SUB, LANES), F32),
            ),
            in_specs=[in_hbm] * 6,
            out_specs=(on_chip, on_chip, on_chip),
            scratch_shapes=[
                pltpu.VMEM((PLANES, sh.slabs, sh.fine_rows, LANES), F32),
                pltpu.VMEM((PLANES, sh.blocks, sh.slabs * LANES, LANES), F32),
                pltpu.VMEM((sh.blocks, sh.slabs * LANES, LANES), F32),
                fine(PLANES),
                fine(3),
                fine(),
                fine(),
                coarse(3, few),
                coarse(3, few),
                coarse(3, sh.slabs + 1),
                coarse(3, sh.slabs + 1),
                coarse(3, few),
                coarse(3, few),
                coarse(3),
                coarse(few),
                coarse(few),
                coarse(3, few),
                coarse(3, few),
                fine(3),
                pltpu.VMEM((PLANES, SUB, gy * sh.wide), F32),
                pltpu.VMEM((PLANES, gy * SUB, LANES), F32),
                pltpu.VMEM((gy, SUB, LANES), F32),
                pltpu.VMEM((gy + 2, 3, SUB, sh.wide), F32),
                pltpu.VMEM((gy + 2, SUB, LANES), F32),
                pltpu.VMEM((gy + 2, 4, SUB, sh.wide), F32),
                pltpu.VMEM((gy, SUB, sh.wide), F32),
                pltpu.VMEM((2, SUB, sh.wide), F32),
                pltpu.VMEM((2, SUB, sh.wide), F32),
                pltpu.VMEM((2, PLANES, SUB, LANES), F32),
                pltpu.VMEM((2, PLANES, SUB, LANES), F32),
                pltpu.VMEM((gy, 3, SUB, sh.wide), F32),
                pltpu.VMEM((2, SUB, LANES), F32),
                pltpu.VMEM((gy, SUB, LANES), F32),
                pltpu.VMEM((gx, SUB, LANES), F32),
                dma((3 + 3 * sh.slabs,)),
                dma((2,)),
                dma((2,)),
                dma((2,)),
                dma((2,)),
                dma((3, gy)),
                dma((3, gy)),
                dma((2, 3)),
                dma((2, 3)),
                dma((gy,)),
                dma((2,)),
                dma((gy,)),
                dma((gy,)),
                dma((2, max(gx, gy))),
                dma((gy,)),
                dma((gx,)),
            ],
            compiler_params=pltpu.CompilerParams(
                collective_id=0, has_side_effects=True, vmem_limit_bytes=64_500_000
            ),
            name="interface_sweeps",
        )(fine_start, fine_known, fine_mu, coarse_start, coarse_known, coarse_mu)
        anywhere = pl.BlockSpec(memory_space=pl.ANY)
        return pl.pallas_call(
            store_kernel,
            out_shape=(
                jax.ShapeDtypeStruct(fine_start.shape, F32),
                jax.ShapeDtypeStruct(coarse_start.shape, F32),
                jax.ShapeDtypeStruct((SWEEPS,), F32),
            ),
            in_specs=[anywhere, anywhere, on_chip],
            out_specs=(in_hbm, in_hbm, in_hbm),
            scratch_shapes=[pltpu.SMEM((SWEEPS,), F32), dma((3,))],
            compiler_params=pltpu.CompilerParams(vmem_limit_bytes=1_000_000),
            name="store_results",
        )(fine_v, coarse_v, norm_v)

    return jax.shard_map(
        on_device,
        mesh=mesh,
        in_specs=(
            P(None, "gx", "gy"),
            P(None, "gx", "gy"),
            P("gx", "gy"),
            P(None, ("gx", "gy"), None),
            P(None, ("gx", "gy"), None),
            P(("gx", "gy"), None),
        ),
        out_specs=(P(None, "gx", "gy"), P(None, ("gx", "gy"), None), P(None)),
        check_vma=False,
    )
```

```python
import functools

import jax
import jax.numpy as jnp
from jax import lax
from jax.experimental import pallas as pl
from jax.experimental.pallas import tpu as pltpu
from jax.sharding import PartitionSpec as P

MESH = pl.DeviceIdType.MESH
F32 = jnp.float32
BF16 = jnp.bfloat16
SWEEPS = 3
LANES = 128
SUB = 8
FINE_OFF = 24
COARSE_OFF = 16
EDGE = 4
PLANES = 7


class Shape:
    def __init__(self, gx, gy, fine_rows, fine_cols):
        self.gx, self.gy = gx, gy
        self.fine_rows, self.fine_cols = fine_rows, fine_cols
        self.coarse_rows, self.wide = fine_rows // 2, fine_cols // 2
        self.tiles = self.coarse_rows // SUB
        self.halves = self.wide // LANES
        self.slabs = 2 * self.halves
        self.fine_buf = fine_rows + 2 * FINE_OFF
        self.coarse_buf = self.coarse_rows + 2 * COARSE_OFF + SUB
        self.blocks = fine_rows // LANES
        self.cells = 3.0 * gx * gy * fine_rows * fine_cols * 1.25


RING = 4


def hops(step):
    return sum(min(d, RING - d) for d in divmod(step, RING))


def far_first(count):
    return sorted(range(1, count), key=lambda step: -hops(step))


def torus_add(at, step):
    row, column = at // RING + step // RING, lax.rem(at, RING) + step % RING
    return lax.rem(row, RING) * RING + lax.rem(column, RING)


def torus_back(at, step):
    row, column = at // RING + RING - step // RING, lax.rem(at, RING) + RING - step % RING
    return lax.rem(row, RING) * RING + lax.rem(column, RING)


def lane_iota():
    return lax.broadcasted_iota(jnp.int32, (SUB, LANES), 1)


def exact_dot(values, table):
    high = values.astype(BF16)
    rest = values - high.astype(F32)
    middle = rest.astype(BF16)
    low = (rest - middle.astype(F32)).astype(BF16)
    total = jnp.dot(high, table, preferred_element_type=F32)
    total = total + jnp.dot(middle, table, preferred_element_type=F32)
    return total + jnp.dot(low, table, preferred_element_type=F32)


def kernel(
    sh,
    fine_start,
    fine_known,
    fine_mu,
    coarse_start,
    coarse_known,
    coarse_mu,
    fine_out,
    coarse_out,
    norm_out,
    nat,
    turned,
    swapped,
    f_a,
    f_b,
    fd,
    fi,
    c_a,
    c_b,
    q_a,
    q_b,
    w_a,
    w_b,
    ckh,
    cd,
    ci,
    pre,
    pre_b,
    near,
    own,
    comb,
    pack,
    got_c,
    got_p,
    got_k,
    strip_out,
    strip_in,
    strip_far,
    edge_out,
    edge_in,
    fin,
    part,
    part_gy,
    part_gx,
    load_sem,
    edge_send,
    edge_recv,
    row_send,
    row_recv,
    a_send,
    a_recv,
    fwd_send,
    fwd_recv,
    strip_send,
    strip_recv,
    fin_sem,
    norm_sem,
):
    gx, gy = sh.gx, sh.gy
    i = lax.axis_index("gx")
    j = lax.axis_index("gy")
    halves, slabs, tiles, wide = sh.halves, sh.slabs, sh.tiles, sh.wide
    halo, coarse_halo = slabs, halves
    lane = lane_iota()
    even = lane % 2 == 0
    first = lane == 0
    last = lane == LANES - 1
    has_up, has_down = i > 0, i < gx - 1
    has_left, has_right = j > 0, j < gy - 1

    def remote(src, dst, send, recv, to_i, to_j):
        return pltpu.make_async_remote_copy(
            src_ref=src,
            dst_ref=dst,
            send_sem=send,
            recv_sem=recv,
            device_id=(to_i, to_j),
            device_id_type=MESH,
        )

    def load(src, dst, kind):
        pltpu.make_async_copy(src, dst, load_sem.at[kind]).start()

    load(coarse_start, own.at[pl.ds(0, 3)], 0)
    load(coarse_known, own.at[pl.ds(3, 3)], 0)
    load(coarse_mu, own.at[6], 0)
    for t in [0, slabs - 1] + list(range(1, slabs - 1)):
        cols = pl.ds(LANES * t, LANES)
        load(fine_start.at[:, :, cols], nat.at[pl.ds(0, 3), t], 1)
        load(fine_known.at[:, :, cols], nat.at[pl.ds(3, 3), t], 1)
        load(fine_mu.at[:, cols], nat.at[6, t], 1)

    barrier = pltpu.get_barrier_semaphore()
    for step in far_first(gy):
        pl.semaphore_signal(
            barrier, inc=1, device_id=(i, torus_add(j, step)), device_id_type=MESH
        )
    for step in range(1, gx):
        pl.semaphore_signal(
            barrier, inc=1, device_id=(lax.rem(i + step, gx), j), device_id_type=MESH
        )

    zero = jnp.zeros((SUB, LANES), F32)
    fine_end = FINE_OFF + sh.fine_rows
    for t in range(slabs + 1):
        for row in (0, 8, fine_end + 8, fine_end + 16):
            for p in range(PLANES):
                f_a[p, t, pl.ds(row, SUB), :] = zero
        for k in range(3):
            for row in (0, fine_end + 16):
                f_b[k, t, pl.ds(row, SUB), :] = zero
            for row in (0, sh.coarse_buf - 8):
                q_a[k, t, pl.ds(row, SUB), :] = zero
                q_b[k, t, pl.ds(row, SUB), :] = zero
                if t <= halves:
                    c_a[k, t, pl.ds(row, SUB), :] = zero
                    c_b[k, t, pl.ds(row, SUB), :] = zero

    for slot in (0, gy + 1):
        for u in range(halves):
            for p in range(4):
                got_k[slot, p, :, pl.ds(LANES * u, LANES)] = zero

    def clear_rows(row, slot):
        for p in range(PLANES):
            for t in range(slabs + 1):
                f_a[p, t, pl.ds(row, SUB), :] = zero
        got_p[slot] = zero
        for u in range(halves):
            for p in range(3):
                got_c[slot, p, :, pl.ds(LANES * u, LANES)] = zero

    def clear_columns(side):
        for p in range(PLANES):
            edge_in[side, p] = zero

    pl.when(i == 0)(lambda: clear_rows(FINE_OFF - SUB, 0))
    pl.when(i == gx - 1)(lambda: clear_rows(fine_end, gy + 1))
    pl.when(j == 0)(lambda: clear_columns(0))
    pl.when(j == gy - 1)(lambda: clear_columns(1))

    pltpu.make_async_copy(own, own, load_sem.at[0]).wait()

    for dest in range(gy):
        for p in range(PLANES):
            after = own[p, :, pl.ds((dest + 1) * wide, LANES)] if dest < gy - 1 else zero
            before = own[p, :, pl.ds(dest * wide - LANES, LANES)] if dest > 0 else zero
            comb[p, pl.ds(SUB * dest, SUB), :] = jnp.where(lane < 64, after, before)
    source = lax.broadcasted_iota(jnp.int32, (LANES, LANES), 0)
    target = lax.broadcasted_iota(jnp.int32, (LANES, LANES), 1)
    inside = target % 16
    wanted = jnp.where(inside < 8, LANES - EDGE + inside // 2, (inside - 8) // 2)
    packed = None
    for p in range(PLANES):
        table = ((source == wanted) & (target // 16 == p)).astype(F32).astype(BF16)
        piece = exact_dot(comb[p], table)
        packed = piece if packed is None else packed + piece
    for dest in range(gy):
        pack[dest] = packed[SUB * dest : SUB * (dest + 1), :]

    def pack_strip(begin):
        for dest in range(gy):
            for p in range(4):
                piece = own[3 + p, begin : begin + 2, pl.ds(dest * wide, wide)]
                strip_out[dest, pl.ds(2 * p, 2), :] = piece

    pl.when(j == gy - 1)(lambda: pack_strip(SUB - 2))
    pl.when(j == 0)(lambda: pack_strip(0))

    pltpu.make_async_copy(nat, nat, load_sem.at[1]).wait()

    def turn_edges(p, carry):
        for b in range(sh.blocks):
            rows = pl.ds(LANES * b, LANES)
            low = nat[p, 0, rows, :].T
            high = nat[p, slabs - 1, rows, :].T
            turned[p, b, pl.ds(0, LANES), :] = low
            turned[p, b, pl.ds(LANES * (slabs - 1), LANES), :] = high
            edge_out[0, p, pl.ds(EDGE * b, EDGE), :] = high[LANES - EDGE :, :]
            edge_out[1, p, pl.ds(EDGE * b, EDGE), :] = low[:EDGE, :]
        return carry

    lax.fori_loop(0, PLANES, turn_edges, 0, unroll=PLANES)

    pl.semaphore_wait(barrier, gy + gx - 2)

    edge_right = remote(
        edge_out.at[0], edge_in.at[0], edge_send.at[0], edge_recv.at[0], i, lax.rem(j + 1, gy)
    )
    edge_left = remote(
        edge_out.at[1], edge_in.at[1], edge_send.at[1], edge_recv.at[1], i, lax.rem(j + gy - 1, gy)
    )

    @pl.when(has_right)
    def _():
        edge_right.start()

    @pl.when(has_left)
    def _():
        edge_left.start()

    def sends_of(step):
        to = torus_add(j, step)
        cols = pl.ds(pl.multiple_of(to * wide, LANES), wide)
        ends = (
            (own.at[pl.ds(0, 3), :, cols], got_c),
            (pack.at[to], got_p),
            (own.at[pl.ds(3, 4), :, cols], got_k),
        )
        return [
            remote(src, dst.at[j + 1], a_send.at[n], a_recv.at[n, group_of(n, step)], i, to)
            for n, (src, dst) in enumerate(ends)
        ]

    order = far_first(gy)
    peers = gy - 1
    group = 4

    def group_of(kind, step):
        return 0 if kind == 2 else (1 + order.index(step)) // group

    def all_sent(ref, sem):
        remote(ref, ref, sem, sem, i, j).wait_send()

    def all_here(ref, sem):
        remote(ref, ref, sem, sem, i, j).wait_recv()

    sends = {step: sends_of(step) for step in order}
    def strip_of(step, side):
        to = torus_add(j, step)
        return remote(
            strip_out.at[to], strip_in.at[side], strip_send.at[0], strip_recv.at[side], i, to
        )

    for step in order:
        sends[step][0].start()
        sends[step][1].start()

    def send_strips(side):
        for step in order:
            strip_of(step, side).start()
        strip_in[side] = strip_out[j]

    pl.when(j == gy - 1)(lambda: send_strips(0))
    pl.when(j == 0)(lambda: send_strips(1))

    got_p[j + 1] = pack[j]
    for u in range(halves):
        cols = pl.ds(pl.multiple_of(j * wide + LANES * u, LANES), LANES)
        for p in range(PLANES):
            piece = own[p, :, cols]
            if p < 3:
                got_c[j + 1, p, :, pl.ds(LANES * u, LANES)] = piece
            else:
                got_k[j + 1, p - 3, :, pl.ds(LANES * u, LANES)] = piece

    def scale_of(p):
        return jnp.where((p >= 3) & (p < 6), 4.0, 1.0).astype(F32)

    def split_columns(p, carry):
        scale = scale_of(p)
        for b in range(sh.blocks):
            rows = pl.ds(LANES * b, LANES)
            for t in range(1, slabs - 1):
                turned[p, b, pl.ds(LANES * t, LANES), :] = nat[p, t, rows, :].T
        for b in range(sh.blocks):
            rows = pl.ds(FINE_OFF + LANES * b, LANES)
            for s in range(slabs):
                begin = 2 * LANES * (s // 2) + s % 2
                f_a[p, s, rows, :] = turned[p, b, pl.ds(begin, LANES, stride=2), :].T * scale
        return carry

    lax.fori_loop(0, PLANES, split_columns, 0)

    @pl.when(has_left)
    def _():
        edge_right.wait_recv()

    @pl.when(has_right)
    def _():
        edge_left.wait_recv()

    between = jnp.zeros((LANES - 2 * EDGE, LANES), F32)

    def unpack_edges(p, carry):
        for b in range(sh.blocks):
            from_left = edge_in[0, p, pl.ds(EDGE * b, EDGE), :]
            from_right = edge_in[1, p, pl.ds(EDGE * b, EDGE), :]
            slab = jnp.concatenate([from_right, between, from_left], axis=0).T * scale_of(p)
            f_a[p, halo, pl.ds(FINE_OFF + LANES * b, LANES), :] = slab
        return carry

    lax.fori_loop(0, PLANES, unpack_edges, 0, unroll=PLANES)

    down_i, up_i = lax.rem(i + 1, gx), lax.rem(i + gx - 1, gx)
    row_down = remote(
        f_a.at[:, :, pl.ds(fine_end - SUB, SUB), :],
        f_a.at[:, :, pl.ds(FINE_OFF - SUB, SUB), :],
        row_send.at[0],
        row_recv.at[0],
        down_i,
        j,
    )
    row_up = remote(
        f_a.at[:, :, pl.ds(FINE_OFF, SUB), :],
        f_a.at[:, :, pl.ds(fine_end, SUB), :],
        row_send.at[1],
        row_recv.at[1],
        up_i,
        j,
    )

    @pl.when(has_down)
    def _():
        row_down.start()

    @pl.when(has_up)
    def _():
        row_up.start()

    def coarse_row(m):
        return pl.multiple_of(COARSE_OFF + SUB * m, SUB)

    def halo_of(slot, p):
        return pltpu.roll(got_p[slot], (LANES - (16 * p + 8)) % LANES, 1)

    def swapped_pairs(value):
        return jnp.where(even, pltpu.roll(value, LANES - 1, 1), pltpu.roll(value, 1, 1))

    def produce(k, row, values, c_ref, q_ref, w_ref, inner=False):
        right = [pltpu.roll(v, 1, 1) for v in values]
        left = [pltpu.roll(v, LANES - 1, 1) for v in values]
        rows = pl.ds(row, SUB)
        count = len(values)
        for t, value in enumerate(values):
            if t == coarse_halo and inner:
                continue
            before = jnp.where(first, right[t - 1], right[t])
            after = jnp.where(last, left[(t + 1) % count], left[t])
            c_ref[k, t, rows, :] = value
            main = 0.375 * value
            if t == coarse_halo:
                outer = jnp.where(even, before, after)
                q_ref[k, halo, rows, :] = main + 0.125 * outer
                w_ref[k, t, rows, :] = outer + swapped_pairs(outer)
            else:
                q_ref[k, 2 * t, rows, :] = main + 0.125 * before
                q_ref[k, 2 * t + 1, rows, :] = main + 0.125 * after
                w_ref[k, t, rows, :] = before + after

    def spread_first(slot, carry):
        for k in range(3):
            values = [got_c[slot, k, :, pl.ds(LANES * t, LANES)] for t in range(halves)]
            values.append(halo_of(slot, k))
            produce(k, coarse_row(slot - 1), values, c_a, q_a, w_a)
        return carry

    halo_lanes = ((lane < 2 * EDGE) & has_right) | ((lane >= LANES - 2 * EDGE) & has_left)
    halo_lanes_fine = ((lane < EDGE) & has_right) | ((lane >= LANES - EDGE) & has_left)

    def spread_second(slot, carry):
        rows = pl.ds(coarse_row(slot - 1), SUB)
        held = ((slot > 0) | has_up) & ((slot <= gy) | has_down)
        for k in range(3):
            ckh[k, rows, :] = 4.0 * halo_of(slot, 3 + k)
        for t in range(halves + 1):
            if t == coarse_halo:
                value, valid = halo_of(slot, 6), halo_lanes & held
            else:
                value, valid = got_k[slot, 3, :, pl.ds(LANES * t, LANES)], (lane >= 0) & held
            diag = value + 1.0
            cd[t, rows, :] = diag * diag
            ci[t, rows, :] = jnp.where(valid, 0.25 * (1.0 / diag), 0.0)
        return carry

    fwd_copies = {}
    for n, ref in enumerate((got_c, got_p)):
        fwd_copies[n] = (
            remote(ref.at[gy], ref.at[0], fwd_send.at[0, n], fwd_recv.at[0, n], down_i, j),
            remote(ref.at[1], ref.at[gy + 1], fwd_send.at[1, n], fwd_recv.at[1, n], up_i, j),
        )

    strip_copies = (
        remote(strip_in.at[0], strip_far.at[0], fwd_send.at[0, 2], fwd_recv.at[0, 2], down_i, j),
        remote(strip_in.at[1], strip_far.at[1], fwd_send.at[1, 2], fwd_recv.at[1, 2], up_i, j),
    )

    def pass_strips_on():
        pl.when(j < gy - 1)(lambda: strip_of(1, 0).wait_recv())
        pl.when(has_down)(lambda: strip_copies[0].start())
        pl.when(j > 0)(lambda: strip_of(1, 1).wait_recv())
        pl.when(has_up)(lambda: strip_copies[1].start())

    def strips_passed_on():
        @pl.when(has_up)
        def _():
            strip_copies[0].wait_recv()
            for p in range(4):
                got_k[0, p, pl.ds(SUB - 2, 2), :] = strip_far[0, pl.ds(2 * p, 2), :]

        @pl.when(has_down)
        def _():
            strip_copies[1].wait_recv()
            for p in range(4):
                got_k[gy + 1, p, pl.ds(0, 2), :] = strip_far[1, pl.ds(2 * p, 2), :]

    def pass_on(source):
        @pl.when((source == gy - 1) & has_down)
        def _():
            fwd_copies[0][0].start()
            fwd_copies[1][0].start()

        @pl.when((source == 0) & has_up)
        def _():
            fwd_copies[0][1].start()
            fwd_copies[1][1].start()

    def passed_on():
        @pl.when(has_up)
        def _():
            fwd_copies[0][0].wait_recv()
            fwd_copies[1][0].wait_recv()

        @pl.when(has_down)
        def _():
            fwd_copies[0][1].wait_recv()
            fwd_copies[1][1].wait_recv()

    def diagonal(row, held):
        rows = pl.ds(row, SUB)
        for t in range(slabs + 1):
            diag = f_a[6, t, rows, :] + 1.0
            valid = (halo_lanes_fine if t == halo else (lane >= 0)) & held
            fd[t, rows, :] = diag * diag
            fi[t, rows, :] = jnp.where(valid, 0.25 * (1.0 / diag), 0.0)

    def diagonals(step, carry):
        for n in range(4):
            diagonal(pl.multiple_of(FINE_OFF + SUB * (4 * step + n), SUB), lane >= 0)
        return carry

    lax.fori_loop(0, sh.fine_rows // (4 * SUB), diagonals, 0)

    for begin in range(0, gy, group):
        if begin == gy // 2:
            for step in order:
                sends[step][2].start()
        steps = ([0] + order)[begin : begin + group]
        count = len(steps) - steps.count(0)
        all_here(got_c.at[pl.ds(0, count)], a_recv.at[0, begin // group])
        all_here(got_p.at[pl.ds(0, count)], a_recv.at[1, begin // group])
        sources = [torus_back(j, step) if step else j for step in steps]
        for source in sources:
            pass_on(source)
        for source in sources:
            spread_first(source + 1, 0)
    pass_strips_on()

    def beside(values):
        side = values[halo]
        odd_right = [pltpu.roll(values[2 * h + 1], 1, 1) for h in range(halves)]
        even_left = [pltpu.roll(values[2 * h], LANES - 1, 1) for h in range(halves)]
        side_right, side_left = pltpu.roll(side, 1, 1), pltpu.roll(side, LANES - 1, 1)
        sums = []
        for h in range(halves):
            before = odd_right[h - 1] if h > 0 else side_right
            after = even_left[h + 1] if h < halves - 1 else side_left
            sums.append(jnp.where(first, before, odd_right[h]) + values[2 * h + 1])
            sums.append(values[2 * h] + jnp.where(last, after, even_left[h]))
        sums.append(
            jnp.where(first, odd_right[-1], side_right) + jnp.where(last, even_left[0], side_left)
        )
        return sums

    def squares(parts, scales, acc):
        for part_sum, scale in zip(parts, scales):
            acc = acc + part_sum * scale
        return acc

    def grown(total, new, old):
        step = new - old
        return step * step if total is None else total + step * step

    def fine_tile(m, acc, f_in, q_ref, f_out, count):
        base = FINE_OFF + 16 * m
        upper, lower = pl.ds(base, SUB, stride=2), pl.ds(base + 1, SUB, stride=2)
        above, below = pl.ds(base - 1, SUB, stride=2), pl.ds(base + 2, SUB, stride=2)
        crow = COARSE_OFF + SUB * m
        q_here, q_up, q_down = pl.ds(crow, SUB), pl.ds(crow - 1, SUB), pl.ds(crow + 1, SUB)
        inv_top = [fi[t, upper, :] for t in range(count)]
        inv_low = [fi[t, lower, :] for t in range(count)]
        part_top, part_low = [None] * slabs, [None] * slabs
        for k in range(3):
            tops = [f_in[k, t, upper, :] for t in range(slabs + 1)]
            lows = [f_in[k, t, lower, :] for t in range(slabs + 1)]
            top_sum, low_sum = beside(tops), beside(lows)
            for t in range(count):
                three = 3.0 * q_ref[k, t, q_here, :]
                nb = (lows[t] + f_in[k, t, above, :]) + (top_sum[t] + q_ref[k, t, q_up, :])
                new = (f_a[3 + k, t, upper, :] + (nb + three)) * inv_top[t]
                f_out[k, t, upper, :] = new
                nb2 = (tops[t] + f_in[k, t, below, :]) + (low_sum[t] + q_ref[k, t, q_down, :])
                new2 = (f_a[3 + k, t, lower, :] + (nb2 + three)) * inv_low[t]
                f_out[k, t, lower, :] = new2
                if t < slabs:
                    part_top[t] = grown(part_top[t], new, tops[t])
                    part_low[t] = grown(part_low[t], new2, lows[t])
        acc = squares(part_top, [fd[t, upper, :] for t in range(slabs)], acc)
        return squares(part_low, [fd[t, lower, :] for t in range(slabs)], acc)

    def coarse_sum(m, k, t, f_in, c_ref, w_ref):
        base = FINE_OFF + 16 * m
        upper, lower = pl.ds(base, SUB, stride=2), pl.ds(base + 1, SUB, stride=2)
        if t == coarse_halo:
            four = f_in[k, halo, upper, :] + f_in[k, halo, lower, :]
            four = four + swapped_pairs(four)
        else:
            four = (f_in[k, 2 * t, upper, :] + f_in[k, 2 * t, lower, :]) + (
                f_in[k, 2 * t + 1, upper, :] + f_in[k, 2 * t + 1, lower, :]
            )
        return coarse_near(m, k, t, c_ref, w_ref) + 0.5 * four

    def coarse_step(m, k, t, added, inv):
        rows = pl.ds(coarse_row(m), SUB)
        if t == coarse_halo:
            known = ckh[k, rows, :]
        else:
            known = 4.0 * got_k[m + 1, k, :, pl.ds(LANES * t, LANES)]
        return (known + added) * inv

    def coarse_tile(m, acc, added_of, c_ref, count, use):
        rows = pl.ds(coarse_row(m), SUB)
        inv = [ci[t, rows, :] for t in range(count)]
        parts = [None] * halves
        for k in range(3):
            values = []
            for t in range(count):
                value = coarse_step(m, k, t, added_of(k, t), inv[t])
                values.append(value)
                if t < halves:
                    parts[t] = grown(parts[t], value, c_ref[k, t, rows, :])
            use(k, values)
        return squares(parts, [cd[t, rows, :] for t in range(halves)], acc)

    def near_sum(m, carry):
        base = FINE_OFF + 16 * m
        upper, lower = pl.ds(base, SUB, stride=2), pl.ds(base + 1, SUB, stride=2)
        above, below = pl.ds(base - 1, SUB, stride=2), pl.ds(base + 2, SUB, stride=2)
        for k in range(3):
            tops = [f_b[k, t, upper, :] for t in range(slabs + 1)]
            lows = [f_b[k, t, lower, :] for t in range(slabs + 1)]
            top_sum, low_sum = beside(tops), beside(lows)
            both = [tops[t] + lows[t] for t in range(slabs + 1)]
            for t in range(slabs + 1):
                nb = (lows[t] + f_b[k, t, above, :]) + top_sum[t]
                near[k, t, upper, :] = f_a[3 + k, t, upper, :] + nb
                nb2 = (tops[t] + f_b[k, t, below, :]) + low_sum[t]
                near[k, t, lower, :] = f_a[3 + k, t, lower, :] + nb2
            rows = pl.ds(coarse_row(m), SUB)
            for t in range(halves):
                pre_b[k, t, rows, :] = 0.5 * (both[2 * t] + both[2 * t + 1])
            side = both[halo]
            pre_b[k, coarse_halo, rows, :] = 0.5 * (side + swapped_pairs(side))
        return zero

    def second_fine(m, acc):
        base = FINE_OFF + 16 * m
        upper, lower = pl.ds(base, SUB, stride=2), pl.ds(base + 1, SUB, stride=2)
        crow = COARSE_OFF + SUB * m
        q_here, q_up, q_down = pl.ds(crow, SUB), pl.ds(crow - 1, SUB), pl.ds(crow + 1, SUB)
        for t in range(slabs + 1):
            inv_top, inv_low = fi[t, upper, :], fi[t, lower, :]
            part_top, part_low = None, None
            for k in range(3):
                three = 3.0 * q_b[k, t, q_here, :]
                new = (near[k, t, upper, :] + (three + q_b[k, t, q_up, :])) * inv_top
                f_a[k, t, upper, :] = new
                new2 = (near[k, t, lower, :] + (three + q_b[k, t, q_down, :])) * inv_low
                f_a[k, t, lower, :] = new2
                if t < slabs:
                    part_top = grown(part_top, new, f_b[k, t, upper, :])
                    part_low = grown(part_low, new2, f_b[k, t, lower, :])
            if t < slabs:
                acc = acc + (part_top * fd[t, upper, :] + part_low * fd[t, lower, :])
        return acc

    def coarse_near(m, k, t, c_ref, w_ref):
        crow = COARSE_OFF + SUB * m
        nb = c_ref[k, t, pl.ds(crow - 1, SUB), :] + c_ref[k, t, pl.ds(crow + 1, SUB), :]
        return nb + w_ref[k, t, pl.ds(coarse_row(m), SUB), :]

    def first_sum(m, carry):
        rows = pl.ds(coarse_row(m), SUB)
        for k in range(3):
            for t in range(halves + 1):
                pre[k, t, rows, :] = coarse_sum(m, k, t, f_a, c_a, w_a)
        return zero

    def first_coarse(m, acc):
        rows = pl.ds(coarse_row(m), SUB)

        def use(k, values):
            produce(k, coarse_row(m), values, c_b, q_b, w_b)

        return coarse_tile(m, acc, lambda k, t: pre[k, t, rows, :], c_a, halves + 1, use)

    def second_coarse(m, acc):
        rows = pl.ds(coarse_row(m), SUB)

        def added_of(k, t):
            return pre_b[k, t, rows, :] + coarse_near(m, k, t, c_b, w_b)

        def use(k, values):
            produce(k, coarse_row(m), values, c_a, q_a, w_a, inner=True)

        return coarse_tile(m, acc, added_of, c_b, halves + 1, use)

    def third_coarse(m, acc):
        def added_of(k, t):
            return coarse_sum(m, k, t, f_a, c_a, w_a)

        def use(k, values):
            for t, value in enumerate(values):
                fin[m, k, :, pl.ds(LANES * t, LANES)] = value

        return coarse_tile(m, acc, added_of, c_a, halves, use)

    def every_tile(body, acc, unroll=6):
        def step(n, acc):
            m = n - 1
            part_sum = body(m, zero)
            inner = jnp.where((n > 0) & (n <= tiles), 1.0, 0.0).astype(F32)
            return acc + part_sum * inner

        return lax.fori_loop(0, tiles + 2, step, acc, unroll=unroll)

    def fine_first(m, acc):
        return fine_tile(m, acc, f_a, q_a, f_b, slabs + 1)

    def fine_third(m, acc):
        return fine_tile(m, acc, f_a, q_a, f_b, slabs)

    def both_first(m, acc):
        first_sum(m, 0)
        return fine_first(m, acc)

    fine_sum1 = lax.fori_loop(1, tiles - 1, fine_first, zero, unroll=7)
    lax.fori_loop(1, tiles - 1, first_sum, zero, unroll=7)

    @pl.when(has_up)
    def _():
        row_down.wait_recv()

    @pl.when(has_down)
    def _():
        row_up.wait_recv()

    for row, held in (
        (FINE_OFF - 16, lane < 0),
        (FINE_OFF - 8, (lane >= 0) & has_up),
        (fine_end, (lane >= 0) & has_down),
        (fine_end + 8, lane < 0),
    ):
        diagonal(row, held)

    passed_on()
    lax.fori_loop(0, 2, lambda e, c: spread_first((gy + 1) * e, c), 0, unroll=2)

    def outer_first(e, acc):
        for n in range(2):
            m = jnp.where(e == 0, n - 1, tiles - 1 + n)
            part_sum = both_first(m, zero)
            if n == 0:
                acc = acc + jnp.where(e == 1, 1.0, 0.0).astype(F32) * part_sum
            else:
                acc = acc + jnp.where(e == 0, 1.0, 0.0).astype(F32) * part_sum
        return acc

    fine_sum1 = lax.fori_loop(0, 2, outer_first, fine_sum1, unroll=2)
    every_tile(near_sum, zero)

    all_here(got_k.at[pl.ds(0, peers)], a_recv.at[2, 0])
    lax.fori_loop(1, gy + 1, spread_second, 0, unroll=8)
    strips_passed_on()
    lax.fori_loop(0, 2, lambda e, c: spread_second((gy + 1) * e, c), 0, unroll=2)

    @pl.when(has_down)
    def _():
        row_down.wait_send()

    @pl.when(has_up)
    def _():
        row_up.wait_send()

    def inner_share(m):
        return jnp.where((m >= 0) & (m < tiles), 1.0, 0.0).astype(F32)

    def lead(m, sums):
        share = inner_share(m)
        return (sums[0] + share * first_coarse(m, zero), sums[1], sums[2])

    def follow(m, sums):
        share = inner_share(m)
        fine_part = second_fine(m, zero)
        coarse_part = second_coarse(m, zero)
        return (sums[0], sums[1] + share * fine_part, sums[2] + share * coarse_part)

    def lead_and_follow(m, sums):
        return lead(m + 1, follow(m - 1, sums))

    sums = lax.fori_loop(-1, 1, lead, (zero, zero, zero), unroll=2)
    sums = lax.fori_loop(0, tiles, lead_and_follow, sums, unroll=4)
    sums = lax.fori_loop(tiles - 1, tiles + 1, follow, sums, unroll=2)
    coarse_sum1, fine_sum2, coarse_sum2 = sums
    coarse_sum3 = lax.fori_loop(0, tiles, third_coarse, zero, unroll=4)

    my_cols = pl.ds(pl.multiple_of(j * wide, LANES), wide)
    for step in order:
        to = torus_add(j, step)
        copy = remote(
            fin.at[to], coarse_out.at[:, :, my_cols], fin_sem.at[0], fin_sem.at[1], i, to
        )
        copy.start()
    for k in range(3):
        for t in range(halves):
            cols = pl.ds(pl.multiple_of(j * wide + LANES * t, LANES), LANES)
            coarse_out[k, :, cols] = fin[j, k, :, pl.ds(LANES * t, LANES)]

    fine_sum3 = lax.fori_loop(0, tiles, fine_third, zero, unroll=8)

    row_of = lax.broadcasted_iota(jnp.int32, (SUB, LANES), 0)
    mine = zero
    sums = ((fine_sum1, coarse_sum1), (fine_sum2, coarse_sum2), (fine_sum3, coarse_sum3))
    for s, (fine_part, coarse_part) in enumerate(sums):
        line = jnp.sum(fine_part + coarse_part, axis=0, keepdims=True)
        mine = jnp.where(row_of == s, line, mine)
    part[0] = mine
    for step in range(1, gx):
        copy = remote(
            part.at[0],
            part_gx.at[step],
            norm_sem.at[0],
            norm_sem.at[1],
            lax.rem(i + step, gx),
            j,
        )
        copy.start()

    def join_columns(k, carry):
        for b in range(sh.blocks):
            rows = pl.ds(FINE_OFF + LANES * b, LANES)
            for s in range(slabs):
                begin = 2 * LANES * (s // 2) + s % 2
                swapped[b, pl.ds(begin, LANES, stride=2), :] = f_b[k, s, rows, :].T
            for t in range(slabs):
                natural = swapped[b, pl.ds(LANES * t, LANES), :].T
                fine_out[k, pl.ds(LANES * b, LANES), pl.ds(LANES * t, LANES)] = natural
        return carry

    lax.fori_loop(0, 3, join_columns, 0)

    all_here(part_gx.at[pl.ds(1, gx - 1)], norm_sem.at[1])
    for step in range(1, gx):
        mine = mine + part_gx[step]
    part[1] = mine
    for step in order:
        copy = remote(
            part.at[1],
            part_gy.at[step],
            norm_sem.at[2],
            norm_sem.at[3],
            i,
            torus_add(j, step),
        )
        copy.start()
    all_here(part_gy.at[pl.ds(1, peers)], norm_sem.at[3])
    for step in order:
        mine = mine + part_gy[step]
    total = jnp.sum(mine, axis=1, keepdims=True) * (1.0 / sh.cells)
    norm_out[...] = jnp.broadcast_to(jnp.sqrt(total), (SUB, LANES))

    @pl.when(has_right)
    def _():
        edge_right.wait_send()

    @pl.when(has_left)
    def _():
        edge_left.wait_send()

    @pl.when(has_down)
    def _():
        for kind in range(2):
            fwd_copies[kind][0].wait_send()
        strip_copies[0].wait_send()

    @pl.when(has_up)
    def _():
        for kind in range(2):
            fwd_copies[kind][1].wait_send()
        strip_copies[1].wait_send()

    for kind, ref in enumerate((got_c, got_p, got_k)):
        all_sent(ref.at[pl.ds(0, peers)], a_send.at[kind])

    @pl.when((j == 0) | (j == gy - 1))
    def _():
        all_sent(strip_out.at[pl.ds(0, peers)], strip_send.at[0])

    all_sent(fin.at[pl.ds(0, peers)], fin_sem.at[0])
    all_here(fin.at[pl.ds(0, peers)], fin_sem.at[1])
    all_sent(part_gx.at[pl.ds(1, gx - 1)], norm_sem.at[0])
    all_sent(part_gy.at[pl.ds(1, peers)], norm_sem.at[2])


def store_kernel(fine, coarse, norms, fine_out, coarse_out, norm_out, scalars, sem):
    stores = [
        pltpu.make_async_copy(fine, fine_out, sem.at[0]),
        pltpu.make_async_copy(coarse, coarse_out, sem.at[1]),
        pltpu.make_async_copy(scalars, norm_out, sem.at[2]),
    ]
    stores[0].start()
    stores[1].start()
    for s in range(SWEEPS):
        scalars[s] = norms[s, 0]
    stores[2].start()
    for copy in stores:
        copy.wait()


def solution(mesh):
    gx, gy = mesh.shape["gx"], mesh.shape["gy"]

    def on_device(fine_start, fine_known, fine_mu, coarse_start, coarse_known, coarse_mu):
        sh = Shape(gx, gy, *fine_mu.shape)
        dma = pltpu.SemaphoreType.DMA
        in_hbm = pl.BlockSpec(memory_space=pltpu.HBM)
        on_chip = pl.BlockSpec(memory_space=pltpu.VMEM)

        def fine(*lead):
            return pltpu.VMEM((*lead, sh.slabs + 1, sh.fine_buf, LANES), F32)

        def coarse(*lead):
            return pltpu.VMEM((*lead, sh.coarse_buf, LANES), F32)

        few = sh.halves + 1
        fine_v, coarse_v, norm_v = pl.pallas_call(
            functools.partial(kernel, sh),
            out_shape=(
                pltpu.VMEM(fine_start.shape, F32),
                pltpu.VMEM(coarse_start.shape, F32),
                pltpu.VMEM((SUB, LANES), F32),
            ),
            in_specs=[in_hbm] * 6,
            out_specs=(on_chip, on_chip, on_chip),
            scratch_shapes=[
                pltpu.VMEM((PLANES, sh.slabs, sh.fine_rows, LANES), F32),
                pltpu.VMEM((PLANES, sh.blocks, sh.slabs * LANES, LANES), F32),
                pltpu.VMEM((sh.blocks, sh.slabs * LANES, LANES), F32),
                fine(PLANES),
                fine(3),
                fine(),
                fine(),
                coarse(3, few),
                coarse(3, few),
                coarse(3, sh.slabs + 1),
                coarse(3, sh.slabs + 1),
                coarse(3, few),
                coarse(3, few),
                coarse(3),
                coarse(few),
                coarse(few),
                coarse(3, few),
                coarse(3, few),
                fine(3),
                pltpu.VMEM((PLANES, SUB, gy * sh.wide), F32),
                pltpu.VMEM((PLANES, gy * SUB, LANES), F32),
                pltpu.VMEM((gy, SUB, LANES), F32),
                pltpu.VMEM((gy + 2, 3, SUB, sh.wide), F32),
                pltpu.VMEM((gy + 2, SUB, LANES), F32),
                pltpu.VMEM((gy + 2, 4, SUB, sh.wide), F32),
                pltpu.VMEM((gy, SUB, sh.wide), F32),
                pltpu.VMEM((2, SUB, sh.wide), F32),
                pltpu.VMEM((2, SUB, sh.wide), F32),
                pltpu.VMEM((2, PLANES, SUB, LANES), F32),
                pltpu.VMEM((2, PLANES, SUB, LANES), F32),
                pltpu.VMEM((gy, 3, SUB, sh.wide), F32),
                pltpu.VMEM((2, SUB, LANES), F32),
                pltpu.VMEM((gy, SUB, LANES), F32),
                pltpu.VMEM((gx, SUB, LANES), F32),
                dma((2,)),
                dma((2,)),
                dma((2,)),
                dma((2,)),
                dma((2,)),
                dma((3,)),
                dma((3, 4)),
                dma((2, 3)),
                dma((2, 3)),
                dma((1,)),
                dma((2,)),
                dma((2,)),
                dma((4,)),
            ],
            compiler_params=pltpu.CompilerParams(
                collective_id=0, has_side_effects=True, vmem_limit_bytes=64_500_000
            ),
            name="interface_sweeps",
        )(fine_start, fine_known, fine_mu, coarse_start, coarse_known, coarse_mu)
        anywhere = pl.BlockSpec(memory_space=pl.ANY)
        return pl.pallas_call(
            store_kernel,
            out_shape=(
                jax.ShapeDtypeStruct(fine_start.shape, F32),
                jax.ShapeDtypeStruct(coarse_start.shape, F32),
                jax.ShapeDtypeStruct((SWEEPS,), F32),
            ),
            in_specs=[anywhere, anywhere, on_chip],
            out_specs=(in_hbm, in_hbm, in_hbm),
            scratch_shapes=[pltpu.SMEM((SWEEPS,), F32), dma((3,))],
            compiler_params=pltpu.CompilerParams(vmem_limit_bytes=1_000_000),
            name="store_results",
        )(fine_v, coarse_v, norm_v)

    return jax.shard_map(
        on_device,
        mesh=mesh,
        in_specs=(
            P(None, "gx", "gy"),
            P(None, "gx", "gy"),
            P("gx", "gy"),
            P(None, ("gx", "gy"), None),
            P(None, ("gx", "gy"), None),
            P(("gx", "gy"), None),
        ),
        out_specs=(P(None, "gx", "gy"), P(None, ("gx", "gy"), None), P(None)),
        check_vma=False,
    )
```

```python
import functools

import jax
import jax.numpy as jnp
from jax import lax
from jax.experimental import pallas as pl
from jax.experimental.pallas import tpu as pltpu
from jax.sharding import PartitionSpec as P

MESH = pl.DeviceIdType.MESH
F32 = jnp.float32
BF16 = jnp.bfloat16
SWEEPS = 3
LANES = 128
SUB = 8
FINE_OFF = 24
COARSE_OFF = 16
EDGE = 4
PLANES = 7


class Shape:
    def __init__(self, gx, gy, fine_rows, fine_cols):
        self.gx, self.gy = gx, gy
        self.fine_rows, self.fine_cols = fine_rows, fine_cols
        self.coarse_rows, self.wide = fine_rows // 2, fine_cols // 2
        self.tiles = self.coarse_rows // SUB
        self.halves = self.wide // LANES
        self.slabs = 2 * self.halves
        self.fine_buf = fine_rows + 2 * FINE_OFF
        self.coarse_buf = self.coarse_rows + 2 * COARSE_OFF + SUB
        self.blocks = fine_rows // LANES
        self.cells = 3.0 * gx * gy * fine_rows * fine_cols * 1.25


RING = 4


def hops(step):
    return sum(min(d, RING - d) for d in divmod(step, RING))


def far_first(count):
    return sorted(range(1, count), key=lambda step: -hops(step))


def torus_add(at, step):
    row, column = at // RING + step // RING, lax.rem(at, RING) + step % RING
    return lax.rem(row, RING) * RING + lax.rem(column, RING)


def torus_back(at, step):
    row, column = at // RING + RING - step // RING, lax.rem(at, RING) + RING - step % RING
    return lax.rem(row, RING) * RING + lax.rem(column, RING)


def lane_iota():
    return lax.broadcasted_iota(jnp.int32, (SUB, LANES), 1)


def exact_dot(values, table):
    high = values.astype(BF16)
    rest = values - high.astype(F32)
    middle = rest.astype(BF16)
    low = (rest - middle.astype(F32)).astype(BF16)
    total = jnp.dot(high, table, preferred_element_type=F32)
    total = total + jnp.dot(middle, table, preferred_element_type=F32)
    return total + jnp.dot(low, table, preferred_element_type=F32)


def kernel(
    sh,
    fine_start,
    fine_known,
    fine_mu,
    coarse_start,
    coarse_known,
    coarse_mu,
    fine_out,
    coarse_out,
    norm_out,
    nat,
    turned,
    swapped,
    f_a,
    f_b,
    fd,
    fi,
    c_a,
    c_b,
    q_a,
    q_b,
    w_a,
    w_b,
    ckh,
    cd,
    ci,
    pre,
    pre_b,
    near,
    own,
    comb,
    pack,
    got_c,
    got_p,
    got_k,
    strip_out,
    strip_in,
    strip_far,
    edge_out,
    edge_in,
    fin,
    part,
    part_gy,
    part_gx,
    load_sem,
    edge_send,
    edge_recv,
    row_send,
    row_recv,
    a_send,
    a_recv,
    fwd_send,
    fwd_recv,
    strip_send,
    strip_recv,
    fin_sem,
    norm_sem,
):
    gx, gy = sh.gx, sh.gy
    i = lax.axis_index("gx")
    j = lax.axis_index("gy")
    halves, slabs, tiles, wide = sh.halves, sh.slabs, sh.tiles, sh.wide
    halo, coarse_halo = slabs, halves
    lane = lane_iota()
    even = lane % 2 == 0
    first = lane == 0
    last = lane == LANES - 1
    has_up, has_down = i > 0, i < gx - 1
    has_left, has_right = j > 0, j < gy - 1

    def remote(src, dst, send, recv, to_i, to_j):
        return pltpu.make_async_remote_copy(
            src_ref=src,
            dst_ref=dst,
            send_sem=send,
            recv_sem=recv,
            device_id=(to_i, to_j),
            device_id_type=MESH,
        )

    def load(src, dst, kind):
        pltpu.make_async_copy(src, dst, load_sem.at[kind]).start()

    load(coarse_start, own.at[pl.ds(0, 3)], 0)
    load(coarse_known, own.at[pl.ds(3, 3)], 0)
    load(coarse_mu, own.at[6], 0)
    for t in [0, slabs - 1] + list(range(1, slabs - 1)):
        cols = pl.ds(LANES * t, LANES)
        load(fine_start.at[:, :, cols], nat.at[pl.ds(0, 3), t], 1)
        load(fine_known.at[:, :, cols], nat.at[pl.ds(3, 3), t], 1)
        load(fine_mu.at[:, cols], nat.at[6, t], 1)

    barrier = pltpu.get_barrier_semaphore()
    for step in far_first(gy):
        pl.semaphore_signal(
            barrier, inc=1, device_id=(i, torus_add(j, step)), device_id_type=MESH
        )
    for step in range(1, gx):
        pl.semaphore_signal(
            barrier, inc=1, device_id=(lax.rem(i + step, gx), j), device_id_type=MESH
        )

    zero = jnp.zeros((SUB, LANES), F32)
    fine_end = FINE_OFF + sh.fine_rows
    for t in range(slabs + 1):
        for row in (0, 8, fine_end + 8, fine_end + 16):
            for p in range(PLANES):
                f_a[p, t, pl.ds(row, SUB), :] = zero
        for k in range(3):
            for row in (0, fine_end + 16):
                f_b[k, t, pl.ds(row, SUB), :] = zero
            for row in (0, sh.coarse_buf - 8):
                q_a[k, t, pl.ds(row, SUB), :] = zero
                q_b[k, t, pl.ds(row, SUB), :] = zero
                if t <= halves:
                    c_a[k, t, pl.ds(row, SUB), :] = zero
                    c_b[k, t, pl.ds(row, SUB), :] = zero

    for slot in (0, gy + 1):
        for u in range(halves):
            for p in range(4):
                got_k[slot, p, :, pl.ds(LANES * u, LANES)] = zero

    def clear_rows(row, slot):
        for p in range(PLANES):
            for t in range(slabs + 1):
                f_a[p, t, pl.ds(row, SUB), :] = zero
        got_p[slot] = zero
        for u in range(halves):
            for p in range(3):
                got_c[slot, p, :, pl.ds(LANES * u, LANES)] = zero

    def clear_columns(side):
        for p in range(PLANES):
            edge_in[side, p] = zero

    pl.when(i == 0)(lambda: clear_rows(FINE_OFF - SUB, 0))
    pl.when(i == gx - 1)(lambda: clear_rows(fine_end, gy + 1))
    pl.when(j == 0)(lambda: clear_columns(0))
    pl.when(j == gy - 1)(lambda: clear_columns(1))

    pltpu.make_async_copy(own, own, load_sem.at[0]).wait()

    for dest in range(gy):
        for p in range(PLANES):
            after = own[p, :, pl.ds((dest + 1) * wide, LANES)] if dest < gy - 1 else zero
            before = own[p, :, pl.ds(dest * wide - LANES, LANES)] if dest > 0 else zero
            comb[p, pl.ds(SUB * dest, SUB), :] = jnp.where(lane < 64, after, before)
    source = lax.broadcasted_iota(jnp.int32, (LANES, LANES), 0)
    target = lax.broadcasted_iota(jnp.int32, (LANES, LANES), 1)
    inside = target % 16
    wanted = jnp.where(inside < 8, LANES - EDGE + inside // 2, (inside - 8) // 2)
    packed = None
    for p in range(PLANES):
        table = ((source == wanted) & (target // 16 == p)).astype(F32).astype(BF16)
        piece = exact_dot(comb[p], table)
        packed = piece if packed is None else packed + piece
    for dest in range(gy):
        pack[dest] = packed[SUB * dest : SUB * (dest + 1), :]

    def pack_strip(begin):
        for dest in range(gy):
            for p in range(4):
                piece = own[3 + p, begin : begin + 2, pl.ds(dest * wide, wide)]
                strip_out[dest, pl.ds(2 * p, 2), :] = piece

    pl.when(j == gy - 1)(lambda: pack_strip(SUB - 2))
    pl.when(j == 0)(lambda: pack_strip(0))

    pltpu.make_async_copy(nat, nat, load_sem.at[1]).wait()

    def turn_edges(p, carry):
        for b in range(sh.blocks):
            rows = pl.ds(LANES * b, LANES)
            low = nat[p, 0, rows, :].T
            high = nat[p, slabs - 1, rows, :].T
            turned[p, b, pl.ds(0, LANES), :] = low
            turned[p, b, pl.ds(LANES * (slabs - 1), LANES), :] = high
            edge_out[0, p, pl.ds(EDGE * b, EDGE), :] = high[LANES - EDGE :, :]
            edge_out[1, p, pl.ds(EDGE * b, EDGE), :] = low[:EDGE, :]
        return carry

    lax.fori_loop(0, PLANES, turn_edges, 0, unroll=PLANES)

    pl.semaphore_wait(barrier, gy + gx - 2)

    edge_right = remote(
        edge_out.at[0], edge_in.at[0], edge_send.at[0], edge_recv.at[0], i, lax.rem(j + 1, gy)
    )
    edge_left = remote(
        edge_out.at[1], edge_in.at[1], edge_send.at[1], edge_recv.at[1], i, lax.rem(j + gy - 1, gy)
    )

    @pl.when(has_right)
    def _():
        edge_right.start()

    @pl.when(has_left)
    def _():
        edge_left.start()

    def sends_of(step):
        to = torus_add(j, step)
        cols = pl.ds(pl.multiple_of(to * wide, LANES), wide)
        ends = (
            (own.at[pl.ds(0, 3), :, cols], got_c),
            (pack.at[to], got_p),
            (own.at[pl.ds(3, 4), :, cols], got_k),
        )
        return [
            remote(src, dst.at[j + 1], a_send.at[n], a_recv.at[n, group_of(n, step)], i, to)
            for n, (src, dst) in enumerate(ends)
        ]

    order = far_first(gy)
    peers = gy - 1
    group = 4

    def group_of(kind, step):
        return 0 if kind == 2 else (1 + order.index(step)) // group

    def all_sent(ref, sem):
        remote(ref, ref, sem, sem, i, j).wait_send()

    def all_here(ref, sem):
        remote(ref, ref, sem, sem, i, j).wait_recv()

    sends = {step: sends_of(step) for step in order}
    def strip_of(step, side):
        to = torus_add(j, step)
        return remote(
            strip_out.at[to], strip_in.at[side], strip_send.at[0], strip_recv.at[side], i, to
        )

    for step in order:
        sends[step][0].start()
        sends[step][1].start()

    def send_strips(side):
        for step in order:
            strip_of(step, side).start()
        strip_in[side] = strip_out[j]

    pl.when(j == gy - 1)(lambda: send_strips(0))
    pl.when(j == 0)(lambda: send_strips(1))

    got_p[j + 1] = pack[j]
    for u in range(halves):
        cols = pl.ds(pl.multiple_of(j * wide + LANES * u, LANES), LANES)
        for p in range(PLANES):
            piece = own[p, :, cols]
            if p < 3:
                got_c[j + 1, p, :, pl.ds(LANES * u, LANES)] = piece
            else:
                got_k[j + 1, p - 3, :, pl.ds(LANES * u, LANES)] = piece

    def scale_of(p):
        return jnp.where((p >= 3) & (p < 6), 4.0, 1.0).astype(F32)

    def split_columns(p, carry):
        scale = scale_of(p)
        for b in range(sh.blocks):
            rows = pl.ds(LANES * b, LANES)
            for t in range(1, slabs - 1):
                turned[p, b, pl.ds(LANES * t, LANES), :] = nat[p, t, rows, :].T
        for b in range(sh.blocks):
            rows = pl.ds(FINE_OFF + LANES * b, LANES)
            for s in range(slabs):
                begin = 2 * LANES * (s // 2) + s % 2
                f_a[p, s, rows, :] = turned[p, b, pl.ds(begin, LANES, stride=2), :].T * scale
        return carry

    lax.fori_loop(0, PLANES, split_columns, 0)

    @pl.when(has_left)
    def _():
        edge_right.wait_recv()

    @pl.when(has_right)
    def _():
        edge_left.wait_recv()

    between = jnp.zeros((LANES - 2 * EDGE, LANES), F32)

    def unpack_edges(p, carry):
        for b in range(sh.blocks):
            from_left = edge_in[0, p, pl.ds(EDGE * b, EDGE), :]
            from_right = edge_in[1, p, pl.ds(EDGE * b, EDGE), :]
            slab = jnp.concatenate([from_right, between, from_left], axis=0).T * scale_of(p)
            f_a[p, halo, pl.ds(FINE_OFF + LANES * b, LANES), :] = slab
        return carry

    lax.fori_loop(0, PLANES, unpack_edges, 0, unroll=PLANES)

    down_i, up_i = lax.rem(i + 1, gx), lax.rem(i + gx - 1, gx)
    row_down = remote(
        f_a.at[:, :, pl.ds(fine_end - SUB, SUB), :],
        f_a.at[:, :, pl.ds(FINE_OFF - SUB, SUB), :],
        row_send.at[0],
        row_recv.at[0],
        down_i,
        j,
    )
    row_up = remote(
        f_a.at[:, :, pl.ds(FINE_OFF, SUB), :],
        f_a.at[:, :, pl.ds(fine_end, SUB), :],
        row_send.at[1],
        row_recv.at[1],
        up_i,
        j,
    )

    @pl.when(has_down)
    def _():
        row_down.start()

    @pl.when(has_up)
    def _():
        row_up.start()

    def coarse_row(m):
        return pl.multiple_of(COARSE_OFF + SUB * m, SUB)

    def halo_of(slot, p):
        return pltpu.roll(got_p[slot], (LANES - (16 * p + 8)) % LANES, 1)

    def swapped_pairs(value):
        return jnp.where(even, pltpu.roll(value, LANES - 1, 1), pltpu.roll(value, 1, 1))

    def produce(k, row, values, c_ref, q_ref, w_ref, inner=False):
        right = [pltpu.roll(v, 1, 1) for v in values]
        left = [pltpu.roll(v, LANES - 1, 1) for v in values]
        rows = pl.ds(row, SUB)
        count = len(values)
        for t, value in enumerate(values):
            if t == coarse_halo and inner:
                continue
            before = jnp.where(first, right[t - 1], right[t])
            after = jnp.where(last, left[(t + 1) % count], left[t])
            c_ref[k, t, rows, :] = value
            main = 0.375 * value
            if t == coarse_halo:
                outer = jnp.where(even, before, after)
                q_ref[k, halo, rows, :] = main + 0.125 * outer
                w_ref[k, t, rows, :] = outer + swapped_pairs(outer)
            else:
                q_ref[k, 2 * t, rows, :] = main + 0.125 * before
                q_ref[k, 2 * t + 1, rows, :] = main + 0.125 * after
                w_ref[k, t, rows, :] = before + after

    def spread_first(slot, carry):
        for k in range(3):
            values = [got_c[slot, k, :, pl.ds(LANES * t, LANES)] for t in range(halves)]
            values.append(halo_of(slot, k))
            produce(k, coarse_row(slot - 1), values, c_a, q_a, w_a)
        return carry

    halo_lanes = ((lane < 2 * EDGE) & has_right) | ((lane >= LANES - 2 * EDGE) & has_left)
    halo_lanes_fine = ((lane < EDGE) & has_right) | ((lane >= LANES - EDGE) & has_left)

    def spread_second(slot, carry):
        rows = pl.ds(coarse_row(slot - 1), SUB)
        held = ((slot > 0) | has_up) & ((slot <= gy) | has_down)
        for k in range(3):
            ckh[k, rows, :] = 4.0 * halo_of(slot, 3 + k)
        for t in range(halves + 1):
            if t == coarse_halo:
                value, valid = halo_of(slot, 6), halo_lanes & held
            else:
                value, valid = got_k[slot, 3, :, pl.ds(LANES * t, LANES)], (lane >= 0) & held
            diag = value + 1.0
            cd[t, rows, :] = diag * diag
            ci[t, rows, :] = jnp.where(valid, 0.25 * (1.0 / diag), 0.0)
        return carry

    fwd_copies = {}
    for n, ref in enumerate((got_c, got_p)):
        fwd_copies[n] = (
            remote(ref.at[gy], ref.at[0], fwd_send.at[0, n], fwd_recv.at[0, n], down_i, j),
            remote(ref.at[1], ref.at[gy + 1], fwd_send.at[1, n], fwd_recv.at[1, n], up_i, j),
        )

    strip_copies = (
        remote(strip_in.at[0], strip_far.at[0], fwd_send.at[0, 2], fwd_recv.at[0, 2], down_i, j),
        remote(strip_in.at[1], strip_far.at[1], fwd_send.at[1, 2], fwd_recv.at[1, 2], up_i, j),
    )

    def pass_strips_on():
        pl.when(j < gy - 1)(lambda: strip_of(1, 0).wait_recv())
        pl.when(has_down)(lambda: strip_copies[0].start())
        pl.when(j > 0)(lambda: strip_of(1, 1).wait_recv())
        pl.when(has_up)(lambda: strip_copies[1].start())

    def strips_passed_on():
        @pl.when(has_up)
        def _():
            strip_copies[0].wait_recv()
            for p in range(4):
                got_k[0, p, pl.ds(SUB - 2, 2), :] = strip_far[0, pl.ds(2 * p, 2), :]

        @pl.when(has_down)
        def _():
            strip_copies[1].wait_recv()
            for p in range(4):
                got_k[gy + 1, p, pl.ds(0, 2), :] = strip_far[1, pl.ds(2 * p, 2), :]

    def pass_on(source):
        @pl.when((source == gy - 1) & has_down)
        def _():
            fwd_copies[0][0].start()
            fwd_copies[1][0].start()

        @pl.when((source == 0) & has_up)
        def _():
            fwd_copies[0][1].start()
            fwd_copies[1][1].start()

    def passed_on():
        @pl.when(has_up)
        def _():
            fwd_copies[0][0].wait_recv()
            fwd_copies[1][0].wait_recv()

        @pl.when(has_down)
        def _():
            fwd_copies[0][1].wait_recv()
            fwd_copies[1][1].wait_recv()

    def diagonal(row, held):
        rows = pl.ds(row, SUB)
        for t in range(slabs + 1):
            diag = f_a[6, t, rows, :] + 1.0
            valid = (halo_lanes_fine if t == halo else (lane >= 0)) & held
            fd[t, rows, :] = diag * diag
            fi[t, rows, :] = jnp.where(valid, 0.25 * (1.0 / diag), 0.0)

    def diagonals(step, carry):
        for n in range(4):
            diagonal(pl.multiple_of(FINE_OFF + SUB * (4 * step + n), SUB), lane >= 0)
        return carry

    lax.fori_loop(0, sh.fine_rows // (4 * SUB), diagonals, 0)

    for begin in range(0, gy, group):
        if begin in (0, gy // 2):
            for step in order[::-1] if begin == 0 else order:
                if (order.index(step) > 9) == (begin == 0):
                    sends[step][2].start()
        steps = ([0] + order)[begin : begin + group]
        count = len(steps) - steps.count(0)
        all_here(got_c.at[pl.ds(0, count)], a_recv.at[0, begin // group])
        all_here(got_p.at[pl.ds(0, count)], a_recv.at[1, begin // group])
        sources = [torus_back(j, step) if step else j for step in steps]
        for source in sources:
            pass_on(source)
        for source in sources:
            spread_first(source + 1, 0)
    pass_strips_on()

    def beside(values):
        side = values[halo]
        odd_right = [pltpu.roll(values[2 * h + 1], 1, 1) for h in range(halves)]
        even_left = [pltpu.roll(values[2 * h], LANES - 1, 1) for h in range(halves)]
        side_right, side_left = pltpu.roll(side, 1, 1), pltpu.roll(side, LANES - 1, 1)
        sums = []
        for h in range(halves):
            before = odd_right[h - 1] if h > 0 else side_right
            after = even_left[h + 1] if h < halves - 1 else side_left
            sums.append(jnp.where(first, before, odd_right[h]) + values[2 * h + 1])
            sums.append(values[2 * h] + jnp.where(last, after, even_left[h]))
        sums.append(
            jnp.where(first, odd_right[-1], side_right) + jnp.where(last, even_left[0], side_left)
        )
        return sums

    def squares(parts, scales, acc):
        for part_sum, scale in zip(parts, scales):
            acc = acc + part_sum * scale
        return acc

    def grown(total, new, old):
        step = new - old
        return step * step if total is None else total + step * step

    def fine_tile(m, acc, f_in, q_ref, f_out, count):
        base = FINE_OFF + 16 * m
        upper, lower = pl.ds(base, SUB, stride=2), pl.ds(base + 1, SUB, stride=2)
        above, below = pl.ds(base - 1, SUB, stride=2), pl.ds(base + 2, SUB, stride=2)
        crow = COARSE_OFF + SUB * m
        q_here, q_up, q_down = pl.ds(crow, SUB), pl.ds(crow - 1, SUB), pl.ds(crow + 1, SUB)
        inv_top = [fi[t, upper, :] for t in range(count)]
        inv_low = [fi[t, lower, :] for t in range(count)]
        part_top, part_low = [None] * slabs, [None] * slabs
        for k in range(3):
            tops = [f_in[k, t, upper, :] for t in range(slabs + 1)]
            lows = [f_in[k, t, lower, :] for t in range(slabs + 1)]
            top_sum, low_sum = beside(tops), beside(lows)
            for t in range(count):
                three = 3.0 * q_ref[k, t, q_here, :]
                nb = (lows[t] + f_in[k, t, above, :]) + (top_sum[t] + q_ref[k, t, q_up, :])
                new = (f_a[3 + k, t, upper, :] + (nb + three)) * inv_top[t]
                f_out[k, t, upper, :] = new
                nb2 = (tops[t] + f_in[k, t, below, :]) + (low_sum[t] + q_ref[k, t, q_down, :])
                new2 = (f_a[3 + k, t, lower, :] + (nb2 + three)) * inv_low[t]
                f_out[k, t, lower, :] = new2
                if t < slabs:
                    part_top[t] = grown(part_top[t], new, tops[t])
                    part_low[t] = grown(part_low[t], new2, lows[t])
        acc = squares(part_top, [fd[t, upper, :] for t in range(slabs)], acc)
        return squares(part_low, [fd[t, lower, :] for t in range(slabs)], acc)

    def coarse_sum(m, k, t, f_in, c_ref, w_ref):
        base = FINE_OFF + 16 * m
        upper, lower = pl.ds(base, SUB, stride=2), pl.ds(base + 1, SUB, stride=2)
        if t == coarse_halo:
            four = f_in[k, halo, upper, :] + f_in[k, halo, lower, :]
            four = four + swapped_pairs(four)
        else:
            four = (f_in[k, 2 * t, upper, :] + f_in[k, 2 * t, lower, :]) + (
                f_in[k, 2 * t + 1, upper, :] + f_in[k, 2 * t + 1, lower, :]
            )
        return coarse_near(m, k, t, c_ref, w_ref) + 0.5 * four

    def coarse_step(m, k, t, added, inv):
        rows = pl.ds(coarse_row(m), SUB)
        if t == coarse_halo:
            known = ckh[k, rows, :]
        else:
            known = 4.0 * got_k[m + 1, k, :, pl.ds(LANES * t, LANES)]
        return (known + added) * inv

    def coarse_tile(m, acc, added_of, c_ref, count, use):
        rows = pl.ds(coarse_row(m), SUB)
        inv = [ci[t, rows, :] for t in range(count)]
        parts = [None] * halves
        for k in range(3):
            values = []
            for t in range(count):
                value = coarse_step(m, k, t, added_of(k, t), inv[t])
                values.append(value)
                if t < halves:
                    parts[t] = grown(parts[t], value, c_ref[k, t, rows, :])
            use(k, values)
        return squares(parts, [cd[t, rows, :] for t in range(halves)], acc)

    def near_sum(m, carry):
        base = FINE_OFF + 16 * m
        upper, lower = pl.ds(base, SUB, stride=2), pl.ds(base + 1, SUB, stride=2)
        above, below = pl.ds(base - 1, SUB, stride=2), pl.ds(base + 2, SUB, stride=2)
        for k in range(3):
            tops = [f_b[k, t, upper, :] for t in range(slabs + 1)]
            lows = [f_b[k, t, lower, :] for t in range(slabs + 1)]
            top_sum, low_sum = beside(tops), beside(lows)
            both = [tops[t] + lows[t] for t in range(slabs + 1)]
            for t in range(slabs + 1):
                nb = (lows[t] + f_b[k, t, above, :]) + top_sum[t]
                near[k, t, upper, :] = f_a[3 + k, t, upper, :] + nb
                nb2 = (tops[t] + f_b[k, t, below, :]) + low_sum[t]
                near[k, t, lower, :] = f_a[3 + k, t, lower, :] + nb2
            rows = pl.ds(coarse_row(m), SUB)
            for t in range(halves):
                pre_b[k, t, rows, :] = 0.5 * (both[2 * t] + both[2 * t + 1])
            side = both[halo]
            pre_b[k, coarse_halo, rows, :] = 0.5 * (side + swapped_pairs(side))
        return zero

    def second_fine(m, acc):
        base = FINE_OFF + 16 * m
        upper, lower = pl.ds(base, SUB, stride=2), pl.ds(base + 1, SUB, stride=2)
        crow = COARSE_OFF + SUB * m
        q_here, q_up, q_down = pl.ds(crow, SUB), pl.ds(crow - 1, SUB), pl.ds(crow + 1, SUB)
        for t in range(slabs + 1):
            inv_top, inv_low = fi[t, upper, :], fi[t, lower, :]
            part_top, part_low = None, None
            for k in range(3):
                three = 3.0 * q_b[k, t, q_here, :]
                new = (near[k, t, upper, :] + (three + q_b[k, t, q_up, :])) * inv_top
                f_a[k, t, upper, :] = new
                new2 = (near[k, t, lower, :] + (three + q_b[k, t, q_down, :])) * inv_low
                f_a[k, t, lower, :] = new2
                if t < slabs:
                    part_top = grown(part_top, new, f_b[k, t, upper, :])
                    part_low = grown(part_low, new2, f_b[k, t, lower, :])
            if t < slabs:
                acc = acc + (part_top * fd[t, upper, :] + part_low * fd[t, lower, :])
        return acc

    def coarse_near(m, k, t, c_ref, w_ref):
        crow = COARSE_OFF + SUB * m
        nb = c_ref[k, t, pl.ds(crow - 1, SUB), :] + c_ref[k, t, pl.ds(crow + 1, SUB), :]
        return nb + w_ref[k, t, pl.ds(coarse_row(m), SUB), :]

    def first_sum(m, carry):
        rows = pl.ds(coarse_row(m), SUB)
        for k in range(3):
            for t in range(halves + 1):
                pre[k, t, rows, :] = coarse_sum(m, k, t, f_a, c_a, w_a)
        return zero

    def first_coarse(m, acc):
        rows = pl.ds(coarse_row(m), SUB)

        def use(k, values):
            produce(k, coarse_row(m), values, c_b, q_b, w_b)

        return coarse_tile(m, acc, lambda k, t: pre[k, t, rows, :], c_a, halves + 1, use)

    def second_coarse(m, acc):
        rows = pl.ds(coarse_row(m), SUB)

        def added_of(k, t):
            return pre_b[k, t, rows, :] + coarse_near(m, k, t, c_b, w_b)

        def use(k, values):
            produce(k, coarse_row(m), values, c_a, q_a, w_a, inner=True)

        return coarse_tile(m, acc, added_of, c_b, halves + 1, use)

    def third_coarse(m, acc):
        def added_of(k, t):
            return coarse_sum(m, k, t, f_a, c_a, w_a)

        def use(k, values):
            for t, value in enumerate(values):
                fin[m, k, :, pl.ds(LANES * t, LANES)] = value

        return coarse_tile(m, acc, added_of, c_a, halves, use)

    def every_tile(body, acc, unroll=6):
        def step(n, acc):
            m = n - 1
            part_sum = body(m, zero)
            inner = jnp.where((n > 0) & (n <= tiles), 1.0, 0.0).astype(F32)
            return acc + part_sum * inner

        return lax.fori_loop(0, tiles + 2, step, acc, unroll=unroll)

    def fine_first(m, acc):
        return fine_tile(m, acc, f_a, q_a, f_b, slabs + 1)

    def fine_third(m, acc):
        return fine_tile(m, acc, f_a, q_a, f_b, slabs)

    def both_first(m, acc):
        first_sum(m, 0)
        return fine_first(m, acc)

    fine_sum1 = lax.fori_loop(1, tiles - 1, fine_first, zero, unroll=7)
    lax.fori_loop(1, tiles - 1, first_sum, zero, unroll=7)

    @pl.when(has_up)
    def _():
        row_down.wait_recv()

    @pl.when(has_down)
    def _():
        row_up.wait_recv()

    for row, held in (
        (FINE_OFF - 16, lane < 0),
        (FINE_OFF - 8, (lane >= 0) & has_up),
        (fine_end, (lane >= 0) & has_down),
        (fine_end + 8, lane < 0),
    ):
        diagonal(row, held)

    passed_on()
    lax.fori_loop(0, 2, lambda e, c: spread_first((gy + 1) * e, c), 0, unroll=2)

    def outer_first(e, acc):
        for n in range(2):
            m = jnp.where(e == 0, n - 1, tiles - 1 + n)
            part_sum = both_first(m, zero)
            if n == 0:
                acc = acc + jnp.where(e == 1, 1.0, 0.0).astype(F32) * part_sum
            else:
                acc = acc + jnp.where(e == 0, 1.0, 0.0).astype(F32) * part_sum
        return acc

    fine_sum1 = lax.fori_loop(0, 2, outer_first, fine_sum1, unroll=2)
    every_tile(near_sum, zero)

    all_here(got_k.at[pl.ds(0, peers)], a_recv.at[2, 0])
    lax.fori_loop(1, gy + 1, spread_second, 0, unroll=8)
    strips_passed_on()
    lax.fori_loop(0, 2, lambda e, c: spread_second((gy + 1) * e, c), 0, unroll=2)

    @pl.when(has_down)
    def _():
        row_down.wait_send()

    @pl.when(has_up)
    def _():
        row_up.wait_send()

    def inner_share(m):
        return jnp.where((m >= 0) & (m < tiles), 1.0, 0.0).astype(F32)

    def lead(m, sums):
        share = inner_share(m)
        return (sums[0] + share * first_coarse(m, zero), sums[1], sums[2])

    def follow(m, sums):
        share = inner_share(m)
        fine_part = second_fine(m, zero)
        coarse_part = second_coarse(m, zero)
        return (sums[0], sums[1] + share * fine_part, sums[2] + share * coarse_part)

    def lead_and_follow(m, sums):
        return lead(m + 1, follow(m - 1, sums))

    sums = lax.fori_loop(-1, 1, lead, (zero, zero, zero), unroll=2)
    sums = lax.fori_loop(0, tiles, lead_and_follow, sums, unroll=4)
    sums = lax.fori_loop(tiles - 1, tiles + 1, follow, sums, unroll=2)
    coarse_sum1, fine_sum2, coarse_sum2 = sums
    coarse_sum3 = lax.fori_loop(0, tiles, third_coarse, zero, unroll=4)

    my_cols = pl.ds(pl.multiple_of(j * wide, LANES), wide)
    for step in order:
        to = torus_add(j, step)
        copy = remote(
            fin.at[to], coarse_out.at[:, :, my_cols], fin_sem.at[0], fin_sem.at[1], i, to
        )
        copy.start()
    for k in range(3):
        for t in range(halves):
            cols = pl.ds(pl.multiple_of(j * wide + LANES * t, LANES), LANES)
            coarse_out[k, :, cols] = fin[j, k, :, pl.ds(LANES * t, LANES)]

    fine_sum3 = lax.fori_loop(0, tiles, fine_third, zero, unroll=8)

    row_of = lax.broadcasted_iota(jnp.int32, (SUB, LANES), 0)
    mine = zero
    sums = ((fine_sum1, coarse_sum1), (fine_sum2, coarse_sum2), (fine_sum3, coarse_sum3))
    for s, (fine_part, coarse_part) in enumerate(sums):
        line = jnp.sum(fine_part + coarse_part, axis=0, keepdims=True)
        mine = jnp.where(row_of == s, line, mine)
    part[0] = mine
    for step in range(1, gx):
        copy = remote(
            part.at[0],
            part_gx.at[step],
            norm_sem.at[0],
            norm_sem.at[1],
            lax.rem(i + step, gx),
            j,
        )
        copy.start()

    def join_columns(k, carry):
        for b in range(sh.blocks):
            rows = pl.ds(FINE_OFF + LANES * b, LANES)
            for s in range(slabs):
                begin = 2 * LANES * (s // 2) + s % 2
                swapped[b, pl.ds(begin, LANES, stride=2), :] = f_b[k, s, rows, :].T
            for t in range(slabs):
                natural = swapped[b, pl.ds(LANES * t, LANES), :].T
                fine_out[k, pl.ds(LANES * b, LANES), pl.ds(LANES * t, LANES)] = natural
        return carry

    lax.fori_loop(0, 3, join_columns, 0)

    all_here(part_gx.at[pl.ds(1, gx - 1)], norm_sem.at[1])
    for step in range(1, gx):
        mine = mine + part_gx[step]
    part[1] = mine
    for step in order:
        copy = remote(
            part.at[1],
            part_gy.at[step],
            norm_sem.at[2],
            norm_sem.at[3],
            i,
            torus_add(j, step),
        )
        copy.start()
    all_here(part_gy.at[pl.ds(1, peers)], norm_sem.at[3])
    for step in order:
        mine = mine + part_gy[step]
    total = jnp.sum(mine, axis=1, keepdims=True) * (1.0 / sh.cells)
    norm_out[...] = jnp.broadcast_to(jnp.sqrt(total), (SUB, LANES))

    @pl.when(has_right)
    def _():
        edge_right.wait_send()

    @pl.when(has_left)
    def _():
        edge_left.wait_send()

    @pl.when(has_down)
    def _():
        for kind in range(2):
            fwd_copies[kind][0].wait_send()
        strip_copies[0].wait_send()

    @pl.when(has_up)
    def _():
        for kind in range(2):
            fwd_copies[kind][1].wait_send()
        strip_copies[1].wait_send()

    for kind, ref in enumerate((got_c, got_p, got_k)):
        all_sent(ref.at[pl.ds(0, peers)], a_send.at[kind])

    @pl.when((j == 0) | (j == gy - 1))
    def _():
        all_sent(strip_out.at[pl.ds(0, peers)], strip_send.at[0])

    all_sent(fin.at[pl.ds(0, peers)], fin_sem.at[0])
    all_here(fin.at[pl.ds(0, peers)], fin_sem.at[1])
    all_sent(part_gx.at[pl.ds(1, gx - 1)], norm_sem.at[0])
    all_sent(part_gy.at[pl.ds(1, peers)], norm_sem.at[2])


def store_kernel(fine, coarse, norms, fine_out, coarse_out, norm_out, scalars, sem):
    half = fine.shape[1] // 2
    for k in range(fine.shape[0]):
        for part in range(2):
            rows = pl.ds(half * part, half)
            pltpu.make_async_copy(fine.at[k, rows], fine_out.at[k, rows], sem.at[0]).start()
    stores = [
        pltpu.make_async_copy(coarse, coarse_out, sem.at[1]),
        pltpu.make_async_copy(scalars, norm_out, sem.at[2]),
    ]
    stores[0].start()
    for s in range(SWEEPS):
        scalars[s] = norms[s, 0]
    stores[1].start()
    for copy in stores:
        copy.wait()
    pltpu.make_async_copy(fine, fine_out, sem.at[0]).wait()


def solution(mesh):
    gx, gy = mesh.shape["gx"], mesh.shape["gy"]

    def on_device(fine_start, fine_known, fine_mu, coarse_start, coarse_known, coarse_mu):
        sh = Shape(gx, gy, *fine_mu.shape)
        dma = pltpu.SemaphoreType.DMA
        in_hbm = pl.BlockSpec(memory_space=pltpu.HBM)
        on_chip = pl.BlockSpec(memory_space=pltpu.VMEM)

        def fine(*lead):
            return pltpu.VMEM((*lead, sh.slabs + 1, sh.fine_buf, LANES), F32)

        def coarse(*lead):
            return pltpu.VMEM((*lead, sh.coarse_buf, LANES), F32)

        few = sh.halves + 1
        fine_v, coarse_v, norm_v = pl.pallas_call(
            functools.partial(kernel, sh),
            out_shape=(
                pltpu.VMEM(fine_start.shape, F32),
                pltpu.VMEM(coarse_start.shape, F32),
                pltpu.VMEM((SUB, LANES), F32),
            ),
            in_specs=[in_hbm] * 6,
            out_specs=(on_chip, on_chip, on_chip),
            scratch_shapes=[
                pltpu.VMEM((PLANES, sh.slabs, sh.fine_rows, LANES), F32),
                pltpu.VMEM((PLANES, sh.blocks, sh.slabs * LANES + SUB, LANES), F32),
                pltpu.VMEM((sh.blocks, sh.slabs * LANES + SUB, LANES), F32),
                fine(PLANES),
                fine(3),
                fine(),
                fine(),
                coarse(3, few),
                coarse(3, few),
                coarse(3, sh.slabs + 1),
                coarse(3, sh.slabs + 1),
                coarse(3, few),
                coarse(3, few),
                coarse(3),
                coarse(few),
                coarse(few),
                coarse(3, few),
                coarse(3, few),
                fine(3),
                pltpu.VMEM((PLANES, SUB, gy * sh.wide), F32),
                pltpu.VMEM((PLANES, gy * SUB, LANES), F32),
                pltpu.VMEM((gy, SUB, LANES), F32),
                pltpu.VMEM((gy + 2, 3, SUB, sh.wide), F32),
                pltpu.VMEM((gy + 2, SUB, LANES), F32),
                pltpu.VMEM((gy + 2, 4, SUB, sh.wide), F32),
                pltpu.VMEM((gy, SUB, sh.wide), F32),
                pltpu.VMEM((2, SUB, sh.wide), F32),
                pltpu.VMEM((2, SUB, sh.wide), F32),
                pltpu.VMEM((2, PLANES, SUB, LANES), F32),
                pltpu.VMEM((2, PLANES, SUB, LANES), F32),
                pltpu.VMEM((gy, 3, SUB, sh.wide), F32),
                pltpu.VMEM((2, SUB, LANES), F32),
                pltpu.VMEM((gy, SUB, LANES), F32),
                pltpu.VMEM((gx, SUB, LANES), F32),
                dma((2,)),
                dma((2,)),
                dma((2,)),
                dma((2,)),
                dma((2,)),
                dma((3,)),
                dma((3, 4)),
                dma((2, 3)),
                dma((2, 3)),
                dma((1,)),
                dma((2,)),
                dma((2,)),
                dma((4,)),
            ],
            compiler_params=pltpu.CompilerParams(
                collective_id=0, has_side_effects=True, vmem_limit_bytes=64_500_000
            ),
            name="interface_sweeps",
        )(fine_start, fine_known, fine_mu, coarse_start, coarse_known, coarse_mu)
        anywhere = pl.BlockSpec(memory_space=pl.ANY)
        return pl.pallas_call(
            store_kernel,
            out_shape=(
                jax.ShapeDtypeStruct(fine_start.shape, F32),
                jax.ShapeDtypeStruct(coarse_start.shape, F32),
                jax.ShapeDtypeStruct((SWEEPS,), F32),
            ),
            in_specs=[anywhere, anywhere, on_chip],
            out_specs=(in_hbm, in_hbm, in_hbm),
            scratch_shapes=[pltpu.SMEM((SWEEPS,), F32), dma((3,))],
            compiler_params=pltpu.CompilerParams(vmem_limit_bytes=1_000_000),
            name="store_results",
        )(fine_v, coarse_v, norm_v)

    return jax.shard_map(
        on_device,
        mesh=mesh,
        in_specs=(
            P(None, "gx", "gy"),
            P(None, "gx", "gy"),
            P("gx", "gy"),
            P(None, ("gx", "gy"), None),
            P(None, ("gx", "gy"), None),
            P(("gx", "gy"), None),
        ),
        out_specs=(P(None, "gx", "gy"), P(None, ("gx", "gy"), None), P(None)),
        check_vma=False,
    )
```

```python
import functools

import jax
import jax.numpy as jnp
from jax import lax
from jax.experimental import pallas as pl
from jax.experimental.pallas import tpu as pltpu
from jax.sharding import PartitionSpec as P

MESH = pl.DeviceIdType.MESH
F32 = jnp.float32
BF16 = jnp.bfloat16
SWEEPS = 3
LANES = 128
SUB = 8
FINE_OFF = 24
COARSE_OFF = 16
EDGE = 4
PLANES = 7


class Shape:
    def __init__(self, gx, gy, fine_rows, fine_cols):
        self.gx, self.gy = gx, gy
        self.fine_rows, self.fine_cols = fine_rows, fine_cols
        self.coarse_rows, self.wide = fine_rows // 2, fine_cols // 2
        self.tiles = self.coarse_rows // SUB
        self.halves = self.wide // LANES
        self.slabs = 2 * self.halves
        self.fine_buf = fine_rows + 2 * FINE_OFF + SUB
        self.coarse_buf = self.coarse_rows + 2 * COARSE_OFF + SUB
        self.blocks = fine_rows // LANES
        self.cells = 3.0 * gx * gy * fine_rows * fine_cols * 1.25


RING = 4


def hops(step):
    return sum(min(d, RING - d) for d in divmod(step, RING))


def far_first(count):
    return sorted(range(1, count), key=lambda step: -hops(step))


def torus_add(at, step):
    row, column = at // RING + step // RING, lax.rem(at, RING) + step % RING
    return lax.rem(row, RING) * RING + lax.rem(column, RING)


def torus_back(at, step):
    row, column = at // RING + RING - step // RING, lax.rem(at, RING) + RING - step % RING
    return lax.rem(row, RING) * RING + lax.rem(column, RING)


def lane_iota():
    return lax.broadcasted_iota(jnp.int32, (SUB, LANES), 1)


def exact_dot(values, table):
    high = values.astype(BF16)
    rest = values - high.astype(F32)
    middle = rest.astype(BF16)
    low = (rest - middle.astype(F32)).astype(BF16)
    total = jnp.dot(high, table, preferred_element_type=F32)
    total = total + jnp.dot(middle, table, preferred_element_type=F32)
    return total + jnp.dot(low, table, preferred_element_type=F32)


def kernel(
    sh,
    fine_start,
    fine_known,
    fine_mu,
    coarse_start,
    coarse_known,
    coarse_mu,
    fine_out,
    coarse_out,
    norm_out,
    nat,
    turned,
    swapped,
    f_a,
    f_b,
    fd,
    fi,
    c_a,
    c_b,
    q_a,
    q_b,
    w_a,
    w_b,
    ckh,
    cd,
    ci,
    pre,
    pre_b,
    near,
    own,
    comb,
    pack,
    got_c,
    got_p,
    got_k,
    strip_out,
    strip_in,
    strip_far,
    edge_out,
    edge_in,
    fin,
    part,
    part_gy,
    part_gx,
    load_sem,
    edge_send,
    edge_recv,
    row_send,
    row_recv,
    a_send,
    a_recv,
    fwd_send,
    fwd_recv,
    strip_send,
    strip_recv,
    fin_sem,
    norm_sem,
):
    gx, gy = sh.gx, sh.gy
    i = lax.axis_index("gx")
    j = lax.axis_index("gy")
    halves, slabs, tiles, wide = sh.halves, sh.slabs, sh.tiles, sh.wide
    halo, coarse_halo = slabs, halves
    lane = lane_iota()
    even = lane % 2 == 0
    first = lane == 0
    last = lane == LANES - 1
    has_up, has_down = i > 0, i < gx - 1
    has_left, has_right = j > 0, j < gy - 1

    def remote(src, dst, send, recv, to_i, to_j):
        return pltpu.make_async_remote_copy(
            src_ref=src,
            dst_ref=dst,
            send_sem=send,
            recv_sem=recv,
            device_id=(to_i, to_j),
            device_id_type=MESH,
        )

    def load(src, dst, kind):
        pltpu.make_async_copy(src, dst, load_sem.at[kind]).start()

    load(coarse_start, own.at[pl.ds(0, 3)], 0)
    load(coarse_known, own.at[pl.ds(3, 3)], 0)
    load(coarse_mu, own.at[6], 0)
    for t in [0, slabs - 1] + list(range(1, slabs - 1)):
        cols = pl.ds(LANES * t, LANES)
        load(fine_start.at[:, :, cols], nat.at[pl.ds(0, 3), t], 1)
        load(fine_known.at[:, :, cols], nat.at[pl.ds(3, 3), t], 1)
        load(fine_mu.at[:, cols], nat.at[6, t], 1)

    barrier = pltpu.get_barrier_semaphore()
    for step in far_first(gy):
        pl.semaphore_signal(
            barrier, inc=1, device_id=(i, torus_add(j, step)), device_id_type=MESH
        )
    for step in range(1, gx):
        pl.semaphore_signal(
            barrier, inc=1, device_id=(lax.rem(i + step, gx), j), device_id_type=MESH
        )

    zero = jnp.zeros((SUB, LANES), F32)
    fine_end = FINE_OFF + sh.fine_rows
    for t in range(slabs + 1):
        for row in (0, 8, fine_end + 8, fine_end + 16):
            for p in range(PLANES):
                f_a[p, t, pl.ds(row, SUB), :] = zero
        for k in range(3):
            for row in (0, fine_end + 16):
                f_b[k, t, pl.ds(row, SUB), :] = zero
            for row in (0, sh.coarse_buf - 8):
                q_a[k, t, pl.ds(row, SUB), :] = zero
                q_b[k, t, pl.ds(row, SUB), :] = zero
                if t <= halves:
                    c_a[k, t, pl.ds(row, SUB), :] = zero
                    c_b[k, t, pl.ds(row, SUB), :] = zero

    for slot in (0, gy + 1):
        for u in range(halves):
            for p in range(4):
                got_k[slot, p, :, pl.ds(LANES * u, LANES)] = zero

    def clear_rows(row, slot):
        for p in range(PLANES):
            for t in range(slabs + 1):
                f_a[p, t, pl.ds(row, SUB), :] = zero
        got_p[slot] = zero
        for u in range(halves):
            for p in range(3):
                got_c[slot, p, :, pl.ds(LANES * u, LANES)] = zero

    def clear_columns(side):
        for p in range(PLANES):
            edge_in[side, p] = zero

    pl.when(i == 0)(lambda: clear_rows(FINE_OFF - SUB, 0))
    pl.when(i == gx - 1)(lambda: clear_rows(fine_end, gy + 1))
    pl.when(j == 0)(lambda: clear_columns(0))
    pl.when(j == gy - 1)(lambda: clear_columns(1))

    pltpu.make_async_copy(own, own, load_sem.at[0]).wait()

    for dest in range(gy):
        for p in range(PLANES):
            after = own[p, :, pl.ds((dest + 1) * wide, LANES)] if dest < gy - 1 else zero
            before = own[p, :, pl.ds(dest * wide - LANES, LANES)] if dest > 0 else zero
            comb[p, pl.ds(SUB * dest, SUB), :] = jnp.where(lane < 64, after, before)
    source = lax.broadcasted_iota(jnp.int32, (LANES, LANES), 0)
    target = lax.broadcasted_iota(jnp.int32, (LANES, LANES), 1)
    inside = target % 16
    wanted = jnp.where(inside < 8, LANES - EDGE + inside // 2, (inside - 8) // 2)
    packed = None
    for p in range(PLANES):
        table = ((source == wanted) & (target // 16 == p)).astype(F32).astype(BF16)
        piece = exact_dot(comb[p], table)
        packed = piece if packed is None else packed + piece
    for dest in range(gy):
        pack[dest] = packed[SUB * dest : SUB * (dest + 1), :]

    def pack_strip(begin):
        for dest in range(gy):
            for p in range(4):
                piece = own[3 + p, begin : begin + 2, pl.ds(dest * wide, wide)]
                strip_out[dest, pl.ds(2 * p, 2), :] = piece

    pl.when(j == gy - 1)(lambda: pack_strip(SUB - 2))
    pl.when(j == 0)(lambda: pack_strip(0))

    pltpu.make_async_copy(nat, nat, load_sem.at[1]).wait()

    def turn_edges(p, carry):
        for b in range(sh.blocks):
            rows = pl.ds(LANES * b, LANES)
            low = nat[p, 0, rows, :].T
            high = nat[p, slabs - 1, rows, :].T
            turned[p, b, pl.ds(0, LANES), :] = low
            turned[p, b, pl.ds(LANES * (slabs - 1), LANES), :] = high
            edge_out[0, p, pl.ds(EDGE * b, EDGE), :] = high[LANES - EDGE :, :]
            edge_out[1, p, pl.ds(EDGE * b, EDGE), :] = low[:EDGE, :]
        return carry

    lax.fori_loop(0, PLANES, turn_edges, 0, unroll=PLANES)

    pl.semaphore_wait(barrier, gy + gx - 2)

    edge_right = remote(
        edge_out.at[0], edge_in.at[0], edge_send.at[0], edge_recv.at[0], i, lax.rem(j + 1, gy)
    )
    edge_left = remote(
        edge_out.at[1], edge_in.at[1], edge_send.at[1], edge_recv.at[1], i, lax.rem(j + gy - 1, gy)
    )

    @pl.when(has_right)
    def _():
        edge_right.start()

    @pl.when(has_left)
    def _():
        edge_left.start()

    def sends_of(step):
        to = torus_add(j, step)
        cols = pl.ds(pl.multiple_of(to * wide, LANES), wide)
        ends = (
            (own.at[pl.ds(0, 3), :, cols], got_c),
            (pack.at[to], got_p),
            (own.at[pl.ds(3, 4), :, cols], got_k),
        )
        return [
            remote(src, dst.at[j + 1], a_send.at[n], a_recv.at[n, group_of(n, step)], i, to)
            for n, (src, dst) in enumerate(ends)
        ]

    order = far_first(gy)
    peers = gy - 1
    group = 4

    def group_of(kind, step):
        return 0 if kind == 2 else (1 + order.index(step)) // group

    def all_sent(ref, sem):
        remote(ref, ref, sem, sem, i, j).wait_send()

    def all_here(ref, sem):
        remote(ref, ref, sem, sem, i, j).wait_recv()

    sends = {step: sends_of(step) for step in order}
    def strip_of(step, side):
        to = torus_add(j, step)
        return remote(
            strip_out.at[to], strip_in.at[side], strip_send.at[0], strip_recv.at[side], i, to
        )

    for step in order:
        sends[step][0].start()
        sends[step][1].start()

    def send_strips(side):
        for step in order:
            strip_of(step, side).start()
        strip_in[side] = strip_out[j]

    pl.when(j == gy - 1)(lambda: send_strips(0))
    pl.when(j == 0)(lambda: send_strips(1))

    got_p[j + 1] = pack[j]
    for u in range(halves):
        cols = pl.ds(pl.multiple_of(j * wide + LANES * u, LANES), LANES)
        for p in range(PLANES):
            piece = own[p, :, cols]
            if p < 3:
                got_c[j + 1, p, :, pl.ds(LANES * u, LANES)] = piece
            else:
                got_k[j + 1, p - 3, :, pl.ds(LANES * u, LANES)] = piece

    def scale_of(p):
        return jnp.where((p >= 3) & (p < 6), 4.0, 1.0).astype(F32)

    def split_columns(p, carry):
        scale = scale_of(p)
        for b in range(sh.blocks):
            rows = pl.ds(LANES * b, LANES)
            for t in range(1, slabs - 1):
                turned[p, b, pl.ds(LANES * t, LANES), :] = nat[p, t, rows, :].T
        for b in range(sh.blocks):
            rows = pl.ds(FINE_OFF + LANES * b, LANES)
            for s in range(slabs):
                begin = 2 * LANES * (s // 2) + s % 2
                f_a[p, s, rows, :] = turned[p, b, pl.ds(begin, LANES, stride=2), :].T * scale
        return carry

    lax.fori_loop(0, PLANES, split_columns, 0)

    @pl.when(has_left)
    def _():
        edge_right.wait_recv()

    @pl.when(has_right)
    def _():
        edge_left.wait_recv()

    between = jnp.zeros((LANES - 2 * EDGE, LANES), F32)

    def unpack_edges(p, carry):
        for b in range(sh.blocks):
            from_left = edge_in[0, p, pl.ds(EDGE * b, EDGE), :]
            from_right = edge_in[1, p, pl.ds(EDGE * b, EDGE), :]
            slab = jnp.concatenate([from_right, between, from_left], axis=0).T * scale_of(p)
            f_a[p, halo, pl.ds(FINE_OFF + LANES * b, LANES), :] = slab
        return carry

    lax.fori_loop(0, PLANES, unpack_edges, 0, unroll=PLANES)

    down_i, up_i = lax.rem(i + 1, gx), lax.rem(i + gx - 1, gx)
    row_down = remote(
        f_a.at[:, :, pl.ds(fine_end - SUB, SUB), :],
        f_a.at[:, :, pl.ds(FINE_OFF - SUB, SUB), :],
        row_send.at[0],
        row_recv.at[0],
        down_i,
        j,
    )
    row_up = remote(
        f_a.at[:, :, pl.ds(FINE_OFF, SUB), :],
        f_a.at[:, :, pl.ds(fine_end, SUB), :],
        row_send.at[1],
        row_recv.at[1],
        up_i,
        j,
    )

    @pl.when(has_down)
    def _():
        row_down.start()

    @pl.when(has_up)
    def _():
        row_up.start()

    def coarse_row(m):
        return pl.multiple_of(COARSE_OFF + SUB * m, SUB)

    def halo_of(slot, p):
        return pltpu.roll(got_p[slot], (LANES - (16 * p + 8)) % LANES, 1)

    def swapped_pairs(value):
        return jnp.where(even, pltpu.roll(value, LANES - 1, 1), pltpu.roll(value, 1, 1))

    def produce(k, row, values, c_ref, q_ref, w_ref, inner=False):
        right = [pltpu.roll(v, 1, 1) for v in values]
        left = [pltpu.roll(v, LANES - 1, 1) for v in values]
        rows = pl.ds(row, SUB)
        count = len(values)
        for t, value in enumerate(values):
            if t == coarse_halo and inner:
                continue
            before = jnp.where(first, right[t - 1], right[t])
            after = jnp.where(last, left[(t + 1) % count], left[t])
            c_ref[k, t, rows, :] = value
            main = 0.375 * value
            if t == coarse_halo:
                outer = jnp.where(even, before, after)
                q_ref[k, halo, rows, :] = main + 0.125 * outer
                w_ref[k, t, rows, :] = outer + swapped_pairs(outer)
            else:
                q_ref[k, 2 * t, rows, :] = main + 0.125 * before
                q_ref[k, 2 * t + 1, rows, :] = main + 0.125 * after
                w_ref[k, t, rows, :] = before + after

    def spread_first(slot, carry):
        for k in range(3):
            values = [got_c[slot, k, :, pl.ds(LANES * t, LANES)] for t in range(halves)]
            values.append(halo_of(slot, k))
            produce(k, coarse_row(slot - 1), values, c_a, q_a, w_a)
        return carry

    halo_lanes = ((lane < 2 * EDGE) & has_right) | ((lane >= LANES - 2 * EDGE) & has_left)
    halo_lanes_fine = ((lane < EDGE) & has_right) | ((lane >= LANES - EDGE) & has_left)

    def spread_second(slot, carry):
        rows = pl.ds(coarse_row(slot - 1), SUB)
        held = ((slot > 0) | has_up) & ((slot <= gy) | has_down)
        for k in range(3):
            ckh[k, rows, :] = 4.0 * halo_of(slot, 3 + k)
        for t in range(halves + 1):
            if t == coarse_halo:
                value, valid = halo_of(slot, 6), halo_lanes & held
            else:
                value, valid = got_k[slot, 3, :, pl.ds(LANES * t, LANES)], (lane >= 0) & held
            diag = value + 1.0
            cd[t, rows, :] = diag * diag
            ci[t, rows, :] = jnp.where(valid, 0.25 * (1.0 / diag), 0.0)
        return carry

    fwd_copies = {}
    for n, ref in enumerate((got_c, got_p)):
        fwd_copies[n] = (
            remote(ref.at[gy], ref.at[0], fwd_send.at[0, n], fwd_recv.at[0, n], down_i, j),
            remote(ref.at[1], ref.at[gy + 1], fwd_send.at[1, n], fwd_recv.at[1, n], up_i, j),
        )

    strip_copies = (
        remote(strip_in.at[0], strip_far.at[0], fwd_send.at[0, 2], fwd_recv.at[0, 2], down_i, j),
        remote(strip_in.at[1], strip_far.at[1], fwd_send.at[1, 2], fwd_recv.at[1, 2], up_i, j),
    )

    def pass_strips_on():
        pl.when(j < gy - 1)(lambda: strip_of(1, 0).wait_recv())
        pl.when(has_down)(lambda: strip_copies[0].start())
        pl.when(j > 0)(lambda: strip_of(1, 1).wait_recv())
        pl.when(has_up)(lambda: strip_copies[1].start())

    def strips_passed_on():
        @pl.when(has_up)
        def _():
            strip_copies[0].wait_recv()
            for p in range(4):
                got_k[0, p, pl.ds(SUB - 2, 2), :] = strip_far[0, pl.ds(2 * p, 2), :]

        @pl.when(has_down)
        def _():
            strip_copies[1].wait_recv()
            for p in range(4):
                got_k[gy + 1, p, pl.ds(0, 2), :] = strip_far[1, pl.ds(2 * p, 2), :]

    def pass_on(source):
        @pl.when((source == gy - 1) & has_down)
        def _():
            fwd_copies[0][0].start()
            fwd_copies[1][0].start()

        @pl.when((source == 0) & has_up)
        def _():
            fwd_copies[0][1].start()
            fwd_copies[1][1].start()

    def passed_on():
        @pl.when(has_up)
        def _():
            fwd_copies[0][0].wait_recv()
            fwd_copies[1][0].wait_recv()

        @pl.when(has_down)
        def _():
            fwd_copies[0][1].wait_recv()
            fwd_copies[1][1].wait_recv()

    def diagonal(row, held):
        rows = pl.ds(row, SUB)
        for t in range(slabs + 1):
            diag = f_a[6, t, rows, :] + 1.0
            valid = (halo_lanes_fine if t == halo else (lane >= 0)) & held
            fd[t, rows, :] = diag * diag
            fi[t, rows, :] = jnp.where(valid, 0.25 * (1.0 / diag), 0.0)

    def diagonals(step, carry):
        for n in range(4):
            diagonal(pl.multiple_of(FINE_OFF + SUB * (4 * step + n), SUB), lane >= 0)
        return carry

    lax.fori_loop(0, sh.fine_rows // (4 * SUB), diagonals, 0)

    for begin in range(0, gy, group):
        if begin in (0, gy // 2):
            for step in order[::-1] if begin == 0 else order:
                if (order.index(step) > 9) == (begin == 0):
                    sends[step][2].start()
        steps = ([0] + order)[begin : begin + group]
        count = len(steps) - steps.count(0)
        all_here(got_c.at[pl.ds(0, count)], a_recv.at[0, begin // group])
        all_here(got_p.at[pl.ds(0, count)], a_recv.at[1, begin // group])
        sources = [torus_back(j, step) if step else j for step in steps]
        for source in sources:
            pass_on(source)
        for source in sources:
            spread_first(source + 1, 0)
    pass_strips_on()

    def beside(values):
        side = values[halo]
        odd_right = [pltpu.roll(values[2 * h + 1], 1, 1) for h in range(halves)]
        even_left = [pltpu.roll(values[2 * h], LANES - 1, 1) for h in range(halves)]
        side_right, side_left = pltpu.roll(side, 1, 1), pltpu.roll(side, LANES - 1, 1)
        sums = []
        for h in range(halves):
            before = odd_right[h - 1] if h > 0 else side_right
            after = even_left[h + 1] if h < halves - 1 else side_left
            sums.append(jnp.where(first, before, odd_right[h]) + values[2 * h + 1])
            sums.append(values[2 * h] + jnp.where(last, after, even_left[h]))
        sums.append(
            jnp.where(first, odd_right[-1], side_right) + jnp.where(last, even_left[0], side_left)
        )
        return sums

    def squares(parts, scales, acc):
        for part_sum, scale in zip(parts, scales):
            acc = acc + part_sum * scale
        return acc

    def grown(total, new, old):
        step = new - old
        return step * step if total is None else total + step * step

    def fine_tile(m, acc, f_in, q_ref, f_out, count):
        base = FINE_OFF + 16 * m
        upper, lower = pl.ds(base, SUB, stride=2), pl.ds(base + 1, SUB, stride=2)
        above, below = pl.ds(base - 1, SUB, stride=2), pl.ds(base + 2, SUB, stride=2)
        crow = COARSE_OFF + SUB * m
        q_here, q_up, q_down = pl.ds(crow, SUB), pl.ds(crow - 1, SUB), pl.ds(crow + 1, SUB)
        inv_top = [fi[t, upper, :] for t in range(count)]
        inv_low = [fi[t, lower, :] for t in range(count)]
        part_top, part_low = [None] * slabs, [None] * slabs
        for k in range(3):
            tops = [f_in[k, t, upper, :] for t in range(slabs + 1)]
            lows = [f_in[k, t, lower, :] for t in range(slabs + 1)]
            top_sum, low_sum = beside(tops), beside(lows)
            for t in range(count):
                three = 3.0 * q_ref[k, t, q_here, :]
                nb = (lows[t] + f_in[k, t, above, :]) + (top_sum[t] + q_ref[k, t, q_up, :])
                new = (f_a[3 + k, t, upper, :] + (nb + three)) * inv_top[t]
                f_out[k, t, upper, :] = new
                nb2 = (tops[t] + f_in[k, t, below, :]) + (low_sum[t] + q_ref[k, t, q_down, :])
                new2 = (f_a[3 + k, t, lower, :] + (nb2 + three)) * inv_low[t]
                f_out[k, t, lower, :] = new2
                if t < slabs:
                    part_top[t] = grown(part_top[t], new, tops[t])
                    part_low[t] = grown(part_low[t], new2, lows[t])
        acc = squares(part_top, [fd[t, upper, :] for t in range(slabs)], acc)
        return squares(part_low, [fd[t, lower, :] for t in range(slabs)], acc)

    def coarse_sum(m, k, t, f_in, c_ref, w_ref):
        base = FINE_OFF + 16 * m
        upper, lower = pl.ds(base, SUB, stride=2), pl.ds(base + 1, SUB, stride=2)
        if t == coarse_halo:
            four = f_in[k, halo, upper, :] + f_in[k, halo, lower, :]
            four = four + swapped_pairs(four)
        else:
            four = (f_in[k, 2 * t, upper, :] + f_in[k, 2 * t, lower, :]) + (
                f_in[k, 2 * t + 1, upper, :] + f_in[k, 2 * t + 1, lower, :]
            )
        return coarse_near(m, k, t, c_ref, w_ref) + 0.5 * four

    def coarse_step(m, k, t, added, inv):
        rows = pl.ds(coarse_row(m), SUB)
        if t == coarse_halo:
            known = ckh[k, rows, :]
        else:
            known = 4.0 * got_k[m + 1, k, :, pl.ds(LANES * t, LANES)]
        return (known + added) * inv

    def coarse_tile(m, acc, added_of, c_ref, count, use):
        rows = pl.ds(coarse_row(m), SUB)
        inv = [ci[t, rows, :] for t in range(count)]
        parts = [None] * halves
        for k in range(3):
            values = []
            for t in range(count):
                value = coarse_step(m, k, t, added_of(k, t), inv[t])
                values.append(value)
                if t < halves:
                    parts[t] = grown(parts[t], value, c_ref[k, t, rows, :])
            use(k, values)
        return squares(parts, [cd[t, rows, :] for t in range(halves)], acc)

    def near_sum(m, carry):
        base = FINE_OFF + 16 * m
        upper, lower = pl.ds(base, SUB, stride=2), pl.ds(base + 1, SUB, stride=2)
        above, below = pl.ds(base - 1, SUB, stride=2), pl.ds(base + 2, SUB, stride=2)
        for k in range(3):
            tops = [f_b[k, t, upper, :] for t in range(slabs + 1)]
            lows = [f_b[k, t, lower, :] for t in range(slabs + 1)]
            top_sum, low_sum = beside(tops), beside(lows)
            both = [tops[t] + lows[t] for t in range(slabs + 1)]
            for t in range(slabs + 1):
                nb = (lows[t] + f_b[k, t, above, :]) + top_sum[t]
                near[k, t, upper, :] = f_a[3 + k, t, upper, :] + nb
                nb2 = (tops[t] + f_b[k, t, below, :]) + low_sum[t]
                near[k, t, lower, :] = f_a[3 + k, t, lower, :] + nb2
            rows = pl.ds(coarse_row(m), SUB)
            for t in range(halves):
                pre_b[k, t, rows, :] = 0.5 * (both[2 * t] + both[2 * t + 1])
            side = both[halo]
            pre_b[k, coarse_halo, rows, :] = 0.5 * (side + swapped_pairs(side))
        return zero

    def second_fine(m, acc):
        base = FINE_OFF + 16 * m
        upper, lower = pl.ds(base, SUB, stride=2), pl.ds(base + 1, SUB, stride=2)
        crow = COARSE_OFF + SUB * m
        q_here, q_up, q_down = pl.ds(crow, SUB), pl.ds(crow - 1, SUB), pl.ds(crow + 1, SUB)
        for t in range(slabs + 1):
            inv_top, inv_low = fi[t, upper, :], fi[t, lower, :]
            part_top, part_low = None, None
            for k in range(3):
                three = 3.0 * q_b[k, t, q_here, :]
                new = (near[k, t, upper, :] + (three + q_b[k, t, q_up, :])) * inv_top
                f_a[k, t, upper, :] = new
                new2 = (near[k, t, lower, :] + (three + q_b[k, t, q_down, :])) * inv_low
                f_a[k, t, lower, :] = new2
                if t < slabs:
                    part_top = grown(part_top, new, f_b[k, t, upper, :])
                    part_low = grown(part_low, new2, f_b[k, t, lower, :])
            if t < slabs:
                acc = acc + (part_top * fd[t, upper, :] + part_low * fd[t, lower, :])
        return acc

    def coarse_near(m, k, t, c_ref, w_ref):
        crow = COARSE_OFF + SUB * m
        nb = c_ref[k, t, pl.ds(crow - 1, SUB), :] + c_ref[k, t, pl.ds(crow + 1, SUB), :]
        return nb + w_ref[k, t, pl.ds(coarse_row(m), SUB), :]

    def first_sum(m, carry):
        rows = pl.ds(coarse_row(m), SUB)
        for k in range(3):
            for t in range(halves + 1):
                pre[k, t, rows, :] = coarse_sum(m, k, t, f_a, c_a, w_a)
        return zero

    def first_coarse(m, acc):
        rows = pl.ds(coarse_row(m), SUB)

        def use(k, values):
            produce(k, coarse_row(m), values, c_b, q_b, w_b)

        return coarse_tile(m, acc, lambda k, t: pre[k, t, rows, :], c_a, halves + 1, use)

    def second_coarse(m, acc):
        rows = pl.ds(coarse_row(m), SUB)

        def added_of(k, t):
            return pre_b[k, t, rows, :] + coarse_near(m, k, t, c_b, w_b)

        def use(k, values):
            produce(k, coarse_row(m), values, c_a, q_a, w_a, inner=True)

        return coarse_tile(m, acc, added_of, c_b, halves + 1, use)

    def third_coarse(m, acc):
        def added_of(k, t):
            return coarse_sum(m, k, t, f_a, c_a, w_a)

        def use(k, values):
            for t, value in enumerate(values):
                fin[m, k, :, pl.ds(LANES * t, LANES)] = value

        return coarse_tile(m, acc, added_of, c_a, halves, use)

    def every_tile(body, acc, unroll=6):
        def step(n, acc):
            m = n - 1
            part_sum = body(m, zero)
            inner = jnp.where((n > 0) & (n <= tiles), 1.0, 0.0).astype(F32)
            return acc + part_sum * inner

        return lax.fori_loop(0, tiles + 2, step, acc, unroll=unroll)

    def fine_first(m, acc):
        return fine_tile(m, acc, f_a, q_a, f_b, slabs + 1)

    def fine_third(m, acc):
        return fine_tile(m, acc, f_a, q_a, f_b, slabs)

    def both_first(m, acc):
        first_sum(m, 0)
        return fine_first(m, acc)

    fine_sum1 = lax.fori_loop(1, tiles - 1, fine_first, zero, unroll=7)
    lax.fori_loop(1, tiles - 1, first_sum, zero, unroll=7)

    @pl.when(has_up)
    def _():
        row_down.wait_recv()

    @pl.when(has_down)
    def _():
        row_up.wait_recv()

    for row, held in (
        (FINE_OFF - 16, lane < 0),
        (FINE_OFF - 8, (lane >= 0) & has_up),
        (fine_end, (lane >= 0) & has_down),
        (fine_end + 8, lane < 0),
    ):
        diagonal(row, held)

    passed_on()
    lax.fori_loop(0, 2, lambda e, c: spread_first((gy + 1) * e, c), 0, unroll=2)

    def outer_first(e, acc):
        for n in range(2):
            m = jnp.where(e == 0, n - 1, tiles - 1 + n)
            part_sum = both_first(m, zero)
            if n == 0:
                acc = acc + jnp.where(e == 1, 1.0, 0.0).astype(F32) * part_sum
            else:
                acc = acc + jnp.where(e == 0, 1.0, 0.0).astype(F32) * part_sum
        return acc

    fine_sum1 = lax.fori_loop(0, 2, outer_first, fine_sum1, unroll=2)
    every_tile(near_sum, zero)

    all_here(got_k.at[pl.ds(0, peers)], a_recv.at[2, 0])
    lax.fori_loop(1, gy + 1, spread_second, 0, unroll=8)
    strips_passed_on()
    lax.fori_loop(0, 2, lambda e, c: spread_second((gy + 1) * e, c), 0, unroll=2)

    @pl.when(has_down)
    def _():
        row_down.wait_send()

    @pl.when(has_up)
    def _():
        row_up.wait_send()

    def inner_share(m):
        return jnp.where((m >= 0) & (m < tiles), 1.0, 0.0).astype(F32)

    def lead(m, sums):
        share = inner_share(m)
        return (sums[0] + share * first_coarse(m, zero), sums[1], sums[2])

    def follow(m, sums):
        share = inner_share(m)
        fine_part = second_fine(m, zero)
        coarse_part = second_coarse(m, zero)
        return (sums[0], sums[1] + share * fine_part, sums[2] + share * coarse_part)

    def lead_and_follow(m, sums):
        return lead(m + 1, follow(m - 1, sums))

    sums = lax.fori_loop(-1, 1, lead, (zero, zero, zero), unroll=2)
    sums = lax.fori_loop(0, tiles, lead_and_follow, sums, unroll=4)
    sums = lax.fori_loop(tiles - 1, tiles + 1, follow, sums, unroll=2)
    coarse_sum1, fine_sum2, coarse_sum2 = sums
    coarse_sum3 = lax.fori_loop(0, tiles, third_coarse, zero, unroll=8)

    my_cols = pl.ds(pl.multiple_of(j * wide, LANES), wide)
    for step in order:
        to = torus_add(j, step)
        copy = remote(
            fin.at[to], coarse_out.at[:, :, my_cols], fin_sem.at[0], fin_sem.at[1], i, to
        )
        copy.start()
    for k in range(3):
        for t in range(halves):
            cols = pl.ds(pl.multiple_of(j * wide + LANES * t, LANES), LANES)
            coarse_out[k, :, cols] = fin[j, k, :, pl.ds(LANES * t, LANES)]

    fine_sum3 = lax.fori_loop(0, tiles, fine_third, zero, unroll=16)

    row_of = lax.broadcasted_iota(jnp.int32, (SUB, LANES), 0)
    mine = zero
    sums = ((fine_sum1, coarse_sum1), (fine_sum2, coarse_sum2), (fine_sum3, coarse_sum3))
    for s, (fine_part, coarse_part) in enumerate(sums):
        line = jnp.sum(fine_part + coarse_part, axis=0, keepdims=True)
        mine = jnp.where(row_of == s, line, mine)
    part[0] = mine
    for step in range(1, gx):
        copy = remote(
            part.at[0],
            part_gx.at[step],
            norm_sem.at[0],
            norm_sem.at[1],
            lax.rem(i + step, gx),
            j,
        )
        copy.start()

    def join_columns(k, carry):
        for b in range(sh.blocks):
            rows = pl.ds(FINE_OFF + LANES * b, LANES)
            for s in range(slabs):
                begin = 2 * LANES * (s // 2) + s % 2
                swapped[b, pl.ds(begin, LANES, stride=2), :] = f_b[k, s, rows, :].T
            for t in range(slabs):
                natural = swapped[b, pl.ds(LANES * t, LANES), :].T
                fine_out[k, pl.ds(LANES * b, LANES), pl.ds(LANES * t, LANES)] = natural
        return carry

    lax.fori_loop(0, 3, join_columns, 0)

    all_here(part_gx.at[pl.ds(1, gx - 1)], norm_sem.at[1])
    for step in range(1, gx):
        mine = mine + part_gx[step]
    part[1] = mine
    for step in order:
        copy = remote(
            part.at[1],
            part_gy.at[step],
            norm_sem.at[2],
            norm_sem.at[3],
            i,
            torus_add(j, step),
        )
        copy.start()
    all_here(part_gy.at[pl.ds(1, peers)], norm_sem.at[3])
    for step in order:
        mine = mine + part_gy[step]
    total = jnp.sum(mine, axis=1, keepdims=True) * (1.0 / sh.cells)
    norm_out[...] = jnp.broadcast_to(jnp.sqrt(total), (SUB, LANES))

    @pl.when(has_right)
    def _():
        edge_right.wait_send()

    @pl.when(has_left)
    def _():
        edge_left.wait_send()

    @pl.when(has_down)
    def _():
        for kind in range(2):
            fwd_copies[kind][0].wait_send()
        strip_copies[0].wait_send()

    @pl.when(has_up)
    def _():
        for kind in range(2):
            fwd_copies[kind][1].wait_send()
        strip_copies[1].wait_send()

    for kind, ref in enumerate((got_c, got_p, got_k)):
        all_sent(ref.at[pl.ds(0, peers)], a_send.at[kind])

    @pl.when((j == 0) | (j == gy - 1))
    def _():
        all_sent(strip_out.at[pl.ds(0, peers)], strip_send.at[0])

    all_sent(fin.at[pl.ds(0, peers)], fin_sem.at[0])
    all_here(fin.at[pl.ds(0, peers)], fin_sem.at[1])
    all_sent(part_gx.at[pl.ds(1, gx - 1)], norm_sem.at[0])
    all_sent(part_gy.at[pl.ds(1, peers)], norm_sem.at[2])


def store_kernel(fine, coarse, norms, fine_out, coarse_out, norm_out, scalars, sem):
    half = fine.shape[1] // 2
    for k in range(fine.shape[0]):
        for part in range(2):
            rows = pl.ds(half * part, half)
            pltpu.make_async_copy(fine.at[k, rows], fine_out.at[k, rows], sem.at[0]).start()
    stores = [
        pltpu.make_async_copy(coarse, coarse_out, sem.at[1]),
        pltpu.make_async_copy(scalars, norm_out, sem.at[2]),
    ]
    stores[0].start()
    for s in range(SWEEPS):
        scalars[s] = norms[s, 0]
    stores[1].start()
    for copy in stores:
        copy.wait()
    pltpu.make_async_copy(fine, fine_out, sem.at[0]).wait()


def solution(mesh):
    gx, gy = mesh.shape["gx"], mesh.shape["gy"]

    def on_device(fine_start, fine_known, fine_mu, coarse_start, coarse_known, coarse_mu):
        sh = Shape(gx, gy, *fine_mu.shape)
        dma = pltpu.SemaphoreType.DMA
        in_hbm = pl.BlockSpec(memory_space=pltpu.HBM)
        on_chip = pl.BlockSpec(memory_space=pltpu.VMEM)

        def fine(*lead):
            return pltpu.VMEM((*lead, sh.slabs + 1, sh.fine_buf, LANES), F32)

        def coarse(*lead):
            return pltpu.VMEM((*lead, sh.coarse_buf, LANES), F32)

        few = sh.halves + 1
        fine_v, coarse_v, norm_v = pl.pallas_call(
            functools.partial(kernel, sh),
            out_shape=(
                pltpu.VMEM(fine_start.shape, F32),
                pltpu.VMEM(coarse_start.shape, F32),
                pltpu.VMEM((SUB, LANES), F32),
            ),
            in_specs=[in_hbm] * 6,
            out_specs=(on_chip, on_chip, on_chip),
            scratch_shapes=[
                pltpu.VMEM((PLANES, sh.slabs, sh.fine_rows, LANES), F32),
                pltpu.VMEM((PLANES, sh.blocks, sh.slabs * LANES + SUB, LANES), F32),
                pltpu.VMEM((sh.blocks, sh.slabs * LANES + SUB, LANES), F32),
                fine(PLANES),
                fine(3),
                fine(),
                fine(),
                coarse(3, few),
                coarse(3, few),
                coarse(3, sh.slabs + 1),
                coarse(3, sh.slabs + 1),
                coarse(3, few),
                coarse(3, few),
                coarse(3),
                coarse(few),
                coarse(few),
                coarse(3, few),
                coarse(3, few),
                fine(3),
                pltpu.VMEM((PLANES, SUB, gy * sh.wide), F32),
                pltpu.VMEM((PLANES, gy * SUB, LANES), F32),
                pltpu.VMEM((gy, SUB, LANES), F32),
                pltpu.VMEM((gy + 2, 3, SUB, sh.wide), F32),
                pltpu.VMEM((gy + 2, SUB, LANES), F32),
                pltpu.VMEM((gy + 2, 4, SUB, sh.wide), F32),
                pltpu.VMEM((gy, SUB, sh.wide), F32),
                pltpu.VMEM((2, SUB, sh.wide), F32),
                pltpu.VMEM((2, SUB, sh.wide), F32),
                pltpu.VMEM((2, PLANES, SUB, LANES), F32),
                pltpu.VMEM((2, PLANES, SUB, LANES), F32),
                pltpu.VMEM((gy, 3, SUB, sh.wide), F32),
                pltpu.VMEM((2, SUB, LANES), F32),
                pltpu.VMEM((gy, SUB, LANES), F32),
                pltpu.VMEM((gx, SUB, LANES), F32),
                dma((2,)),
                dma((2,)),
                dma((2,)),
                dma((2,)),
                dma((2,)),
                dma((3,)),
                dma((3, 4)),
                dma((2, 3)),
                dma((2, 3)),
                dma((1,)),
                dma((2,)),
                dma((2,)),
                dma((4,)),
            ],
            compiler_params=pltpu.CompilerParams(
                collective_id=0, has_side_effects=True, vmem_limit_bytes=64_500_000
            ),
            name="interface_sweeps",
        )(fine_start, fine_known, fine_mu, coarse_start, coarse_known, coarse_mu)
        anywhere = pl.BlockSpec(memory_space=pl.ANY)
        return pl.pallas_call(
            store_kernel,
            out_shape=(
                jax.ShapeDtypeStruct(fine_start.shape, F32),
                jax.ShapeDtypeStruct(coarse_start.shape, F32),
                jax.ShapeDtypeStruct((SWEEPS,), F32),
            ),
            in_specs=[anywhere, anywhere, on_chip],
            out_specs=(in_hbm, in_hbm, in_hbm),
            scratch_shapes=[pltpu.SMEM((SWEEPS,), F32), dma((3,))],
            compiler_params=pltpu.CompilerParams(vmem_limit_bytes=1_000_000),
            name="store_results",
        )(fine_v, coarse_v, norm_v)

    return jax.shard_map(
        on_device,
        mesh=mesh,
        in_specs=(
            P(None, "gx", "gy"),
            P(None, "gx", "gy"),
            P("gx", "gy"),
            P(None, ("gx", "gy"), None),
            P(None, ("gx", "gy"), None),
            P(("gx", "gy"), None),
        ),
        out_specs=(P(None, "gx", "gy"), P(None, ("gx", "gy"), None), P(None)),
        check_vma=False,
    )
```

```python
import functools

import jax
import jax.numpy as jnp
from jax import lax
from jax.experimental import pallas as pl
from jax.experimental.pallas import tpu as pltpu
from jax.sharding import PartitionSpec as P

MESH = pl.DeviceIdType.MESH
F32 = jnp.float32
BF16 = jnp.bfloat16
SWEEPS = 3
LANES = 128
SUB = 8
FINE_OFF = 24
COARSE_OFF = 16
EDGE = 4
PLANES = 7


class Shape:
    def __init__(self, gx, gy, fine_rows, fine_cols):
        self.gx, self.gy = gx, gy
        self.fine_rows, self.fine_cols = fine_rows, fine_cols
        self.coarse_rows, self.wide = fine_rows // 2, fine_cols // 2
        self.tiles = self.coarse_rows // SUB
        self.halves = self.wide // LANES
        self.slabs = 2 * self.halves
        self.fine_buf = fine_rows + 2 * FINE_OFF + SUB
        self.coarse_buf = self.coarse_rows + 2 * COARSE_OFF + SUB
        self.blocks = fine_rows // LANES
        self.cells = 3.0 * gx * gy * fine_rows * fine_cols * 1.25


RING = 4


def hops(step):
    return sum(min(d, RING - d) for d in divmod(step, RING))


def far_first(count):
    return sorted(range(1, count), key=lambda step: -hops(step))


def torus_add(at, step):
    row, column = at // RING + step // RING, lax.rem(at, RING) + step % RING
    return lax.rem(row, RING) * RING + lax.rem(column, RING)


def torus_back(at, step):
    row, column = at // RING + RING - step // RING, lax.rem(at, RING) + RING - step % RING
    return lax.rem(row, RING) * RING + lax.rem(column, RING)


def lane_iota():
    return lax.broadcasted_iota(jnp.int32, (SUB, LANES), 1)


def exact_dot(values, table):
    high = values.astype(BF16)
    rest = values - high.astype(F32)
    middle = rest.astype(BF16)
    low = (rest - middle.astype(F32)).astype(BF16)
    total = jnp.dot(high, table, preferred_element_type=F32)
    total = total + jnp.dot(middle, table, preferred_element_type=F32)
    return total + jnp.dot(low, table, preferred_element_type=F32)


def kernel(
    sh,
    fine_start,
    fine_known,
    fine_mu,
    coarse_start,
    coarse_known,
    coarse_mu,
    fine_out,
    coarse_out,
    norm_out,
    nat,
    turned,
    swapped,
    f_a,
    f_b,
    fd,
    fi,
    c_a,
    c_b,
    q_a,
    q_b,
    w_a,
    w_b,
    ckh,
    cd,
    ci,
    pre,
    pre_b,
    near,
    own,
    comb,
    pack,
    got_c,
    got_p,
    got_k,
    strip_out,
    strip_in,
    strip_far,
    edge_out,
    edge_in,
    fin,
    part,
    part_gy,
    part_gx,
    load_sem,
    edge_send,
    edge_recv,
    row_send,
    row_recv,
    a_send,
    a_recv,
    fwd_send,
    fwd_recv,
    strip_send,
    strip_recv,
    fin_sem,
    norm_sem,
):
    gx, gy = sh.gx, sh.gy
    i = lax.axis_index("gx")
    j = lax.axis_index("gy")
    halves, slabs, tiles, wide = sh.halves, sh.slabs, sh.tiles, sh.wide
    halo, coarse_halo = slabs, halves
    lane = lane_iota()
    even = lane % 2 == 0
    first = lane == 0
    last = lane == LANES - 1
    has_up, has_down = i > 0, i < gx - 1
    has_left, has_right = j > 0, j < gy - 1

    def remote(src, dst, send, recv, to_i, to_j):
        return pltpu.make_async_remote_copy(
            src_ref=src,
            dst_ref=dst,
            send_sem=send,
            recv_sem=recv,
            device_id=(to_i, to_j),
            device_id_type=MESH,
        )

    def load(src, dst, kind):
        pltpu.make_async_copy(src, dst, load_sem.at[kind]).start()

    load(coarse_start, own.at[pl.ds(0, 3)], 0)
    load(coarse_known, own.at[pl.ds(3, 3)], 0)
    load(coarse_mu, own.at[6], 0)
    for t in [0, slabs - 1] + list(range(1, slabs - 1)):
        cols = pl.ds(LANES * t, LANES)
        load(fine_start.at[:, :, cols], nat.at[pl.ds(0, 3), t], 1)
        load(fine_known.at[:, :, cols], nat.at[pl.ds(3, 3), t], 1)
        load(fine_mu.at[:, cols], nat.at[6, t], 1)

    barrier = pltpu.get_barrier_semaphore()
    for step in far_first(gy):
        pl.semaphore_signal(
            barrier, inc=1, device_id=(i, torus_add(j, step)), device_id_type=MESH
        )
    for step in range(1, gx):
        pl.semaphore_signal(
            barrier, inc=1, device_id=(lax.rem(i + step, gx), j), device_id_type=MESH
        )

    zero = jnp.zeros((SUB, LANES), F32)
    fine_end = FINE_OFF + sh.fine_rows
    for t in range(slabs + 1):
        for row in (0, 8, fine_end + 8, fine_end + 16):
            for p in range(PLANES):
                f_a[p, t, pl.ds(row, SUB), :] = zero
        for k in range(3):
            for row in (0, fine_end + 16):
                f_b[k, t, pl.ds(row, SUB), :] = zero
            for row in (0, sh.coarse_buf - 8):
                q_a[k, t, pl.ds(row, SUB), :] = zero
                q_b[k, t, pl.ds(row, SUB), :] = zero
                if t <= halves:
                    c_a[k, t, pl.ds(row, SUB), :] = zero
                    c_b[k, t, pl.ds(row, SUB), :] = zero

    for slot in (0, gy + 1):
        for u in range(halves):
            for p in range(4):
                got_k[slot, p, :, pl.ds(LANES * u, LANES)] = zero

    def clear_rows(row, slot):
        for p in range(PLANES):
            for t in range(slabs + 1):
                f_a[p, t, pl.ds(row, SUB), :] = zero
        got_p[slot] = zero
        for u in range(halves):
            for p in range(3):
                got_c[slot, p, :, pl.ds(LANES * u, LANES)] = zero

    def clear_columns(side):
        for p in range(PLANES):
            edge_in[side, p] = zero

    pl.when(i == 0)(lambda: clear_rows(FINE_OFF - SUB, 0))
    pl.when(i == gx - 1)(lambda: clear_rows(fine_end, gy + 1))
    pl.when(j == 0)(lambda: clear_columns(0))
    pl.when(j == gy - 1)(lambda: clear_columns(1))

    pltpu.make_async_copy(own, own, load_sem.at[0]).wait()

    for dest in range(gy):
        for p in range(PLANES):
            after = own[p, :, pl.ds((dest + 1) * wide, LANES)] if dest < gy - 1 else zero
            before = own[p, :, pl.ds(dest * wide - LANES, LANES)] if dest > 0 else zero
            comb[p, pl.ds(SUB * dest, SUB), :] = jnp.where(lane < 64, after, before)
    source = lax.broadcasted_iota(jnp.int32, (LANES, LANES), 0)
    target = lax.broadcasted_iota(jnp.int32, (LANES, LANES), 1)
    inside = target % 16
    wanted = jnp.where(inside < 8, LANES - EDGE + inside // 2, (inside - 8) // 2)
    packed = None
    for p in range(PLANES):
        table = ((source == wanted) & (target // 16 == p)).astype(F32).astype(BF16)
        piece = exact_dot(comb[p], table)
        packed = piece if packed is None else packed + piece
    for dest in range(gy):
        pack[dest] = packed[SUB * dest : SUB * (dest + 1), :]

    def pack_strip(begin):
        for dest in range(gy):
            for p in range(4):
                piece = own[3 + p, begin : begin + 2, pl.ds(dest * wide, wide)]
                strip_out[dest, pl.ds(2 * p, 2), :] = piece

    pl.when(j == gy - 1)(lambda: pack_strip(SUB - 2))
    pl.when(j == 0)(lambda: pack_strip(0))

    pltpu.make_async_copy(nat, nat, load_sem.at[1]).wait()

    def turn_edges(p, carry):
        for b in range(sh.blocks):
            rows = pl.ds(LANES * b, LANES)
            low = nat[p, 0, rows, :].T
            high = nat[p, slabs - 1, rows, :].T
            turned[p, b, pl.ds(0, LANES), :] = low
            turned[p, b, pl.ds(LANES * (slabs - 1), LANES), :] = high
            edge_out[0, p, pl.ds(EDGE * b, EDGE), :] = high[LANES - EDGE :, :]
            edge_out[1, p, pl.ds(EDGE * b, EDGE), :] = low[:EDGE, :]
        return carry

    lax.fori_loop(0, PLANES, turn_edges, 0, unroll=PLANES)

    pl.semaphore_wait(barrier, gy + gx - 2)

    edge_right = remote(
        edge_out.at[0], edge_in.at[0], edge_send.at[0], edge_recv.at[0], i, lax.rem(j + 1, gy)
    )
    edge_left = remote(
        edge_out.at[1], edge_in.at[1], edge_send.at[1], edge_recv.at[1], i, lax.rem(j + gy - 1, gy)
    )

    @pl.when(has_right)
    def _():
        edge_right.start()

    @pl.when(has_left)
    def _():
        edge_left.start()

    def sends_of(step):
        to = torus_add(j, step)
        cols = pl.ds(pl.multiple_of(to * wide, LANES), wide)
        ends = (
            (own.at[pl.ds(0, 3), :, cols], got_c),
            (pack.at[to], got_p),
            (own.at[pl.ds(3, 4), :, cols], got_k),
        )
        return [
            remote(src, dst.at[j + 1], a_send.at[n], a_recv.at[n, group_of(n, step)], i, to)
            for n, (src, dst) in enumerate(ends)
        ]

    order = far_first(gy)
    peers = gy - 1
    group = 4

    def group_of(kind, step):
        return 0 if kind == 2 else (1 + order.index(step)) // group

    def all_sent(ref, sem):
        remote(ref, ref, sem, sem, i, j).wait_send()

    def all_here(ref, sem):
        remote(ref, ref, sem, sem, i, j).wait_recv()

    sends = {step: sends_of(step) for step in order}
    def strip_of(step, side):
        to = torus_add(j, step)
        return remote(
            strip_out.at[to], strip_in.at[side], strip_send.at[0], strip_recv.at[side], i, to
        )

    for step in order:
        sends[step][0].start()
        sends[step][1].start()

    def send_strips(side):
        for step in order:
            strip_of(step, side).start()
        strip_in[side] = strip_out[j]

    pl.when(j == gy - 1)(lambda: send_strips(0))
    pl.when(j == 0)(lambda: send_strips(1))

    got_p[j + 1] = pack[j]
    for u in range(halves):
        cols = pl.ds(pl.multiple_of(j * wide + LANES * u, LANES), LANES)
        for p in range(PLANES):
            piece = own[p, :, cols]
            if p < 3:
                got_c[j + 1, p, :, pl.ds(LANES * u, LANES)] = piece
            else:
                got_k[j + 1, p - 3, :, pl.ds(LANES * u, LANES)] = piece

    def scale_of(p):
        return jnp.where((p >= 3) & (p < 6), 4.0, 1.0).astype(F32)

    def split_columns(p, carry):
        scale = scale_of(p)
        for b in range(sh.blocks):
            rows = pl.ds(LANES * b, LANES)
            for t in range(1, slabs - 1):
                turned[p, b, pl.ds(LANES * t, LANES), :] = nat[p, t, rows, :].T
        for b in range(sh.blocks):
            rows = pl.ds(FINE_OFF + LANES * b, LANES)
            for s in range(slabs):
                begin = 2 * LANES * (s // 2) + s % 2
                f_a[p, s, rows, :] = turned[p, b, pl.ds(begin, LANES, stride=2), :].T * scale
        return carry

    lax.fori_loop(0, PLANES, split_columns, 0)

    @pl.when(has_left)
    def _():
        edge_right.wait_recv()

    @pl.when(has_right)
    def _():
        edge_left.wait_recv()

    between = jnp.zeros((LANES - 2 * EDGE, LANES), F32)

    def unpack_edges(p, carry):
        for b in range(sh.blocks):
            from_left = edge_in[0, p, pl.ds(EDGE * b, EDGE), :]
            from_right = edge_in[1, p, pl.ds(EDGE * b, EDGE), :]
            slab = jnp.concatenate([from_right, between, from_left], axis=0).T * scale_of(p)
            f_a[p, halo, pl.ds(FINE_OFF + LANES * b, LANES), :] = slab
        return carry

    lax.fori_loop(0, PLANES, unpack_edges, 0, unroll=PLANES)

    down_i, up_i = lax.rem(i + 1, gx), lax.rem(i + gx - 1, gx)
    row_down = remote(
        f_a.at[:, :, pl.ds(fine_end - SUB, SUB), :],
        f_a.at[:, :, pl.ds(FINE_OFF - SUB, SUB), :],
        row_send.at[0],
        row_recv.at[0],
        down_i,
        j,
    )
    row_up = remote(
        f_a.at[:, :, pl.ds(FINE_OFF, SUB), :],
        f_a.at[:, :, pl.ds(fine_end, SUB), :],
        row_send.at[1],
        row_recv.at[1],
        up_i,
        j,
    )

    @pl.when(has_down)
    def _():
        row_down.start()

    @pl.when(has_up)
    def _():
        row_up.start()

    def coarse_row(m):
        return pl.multiple_of(COARSE_OFF + SUB * m, SUB)

    def halo_of(slot, p):
        return pltpu.roll(got_p[slot], (LANES - (16 * p + 8)) % LANES, 1)

    def swapped_pairs(value):
        return jnp.where(even, pltpu.roll(value, LANES - 1, 1), pltpu.roll(value, 1, 1))

    def produce(k, row, values, c_ref, q_ref, w_ref, inner=False):
        right = [pltpu.roll(v, 1, 1) for v in values]
        left = [pltpu.roll(v, LANES - 1, 1) for v in values]
        rows = pl.ds(row, SUB)
        count = len(values)
        for t, value in enumerate(values):
            if t == coarse_halo and inner:
                continue
            before = jnp.where(first, right[t - 1], right[t])
            after = jnp.where(last, left[(t + 1) % count], left[t])
            c_ref[k, t, rows, :] = value
            main = 0.375 * value
            if t == coarse_halo:
                outer = jnp.where(even, before, after)
                q_ref[k, halo, rows, :] = main + 0.125 * outer
                w_ref[k, t, rows, :] = outer + swapped_pairs(outer)
            else:
                q_ref[k, 2 * t, rows, :] = main + 0.125 * before
                q_ref[k, 2 * t + 1, rows, :] = main + 0.125 * after
                w_ref[k, t, rows, :] = before + after

    def spread_first(slot, carry):
        for k in range(3):
            values = [got_c[slot, k, :, pl.ds(LANES * t, LANES)] for t in range(halves)]
            values.append(halo_of(slot, k))
            produce(k, coarse_row(slot - 1), values, c_a, q_a, w_a)
        return carry

    halo_lanes = ((lane < 2 * EDGE) & has_right) | ((lane >= LANES - 2 * EDGE) & has_left)
    halo_lanes_fine = ((lane < EDGE) & has_right) | ((lane >= LANES - EDGE) & has_left)

    def spread_second(slot, carry):
        rows = pl.ds(coarse_row(slot - 1), SUB)
        held = ((slot > 0) | has_up) & ((slot <= gy) | has_down)
        for k in range(3):
            ckh[k, rows, :] = 4.0 * halo_of(slot, 3 + k)
        for t in range(halves + 1):
            if t == coarse_halo:
                value, valid = halo_of(slot, 6), halo_lanes & held
            else:
                value, valid = got_k[slot, 3, :, pl.ds(LANES * t, LANES)], (lane >= 0) & held
            diag = value + 1.0
            cd[t, rows, :] = diag * diag
            ci[t, rows, :] = jnp.where(valid, 0.25 * (1.0 / diag), 0.0)
        return carry

    fwd_copies = {}
    for n, ref in enumerate((got_c, got_p)):
        fwd_copies[n] = (
            remote(ref.at[gy], ref.at[0], fwd_send.at[0, n], fwd_recv.at[0, n], down_i, j),
            remote(ref.at[1], ref.at[gy + 1], fwd_send.at[1, n], fwd_recv.at[1, n], up_i, j),
        )

    strip_copies = (
        remote(strip_in.at[0], strip_far.at[0], fwd_send.at[0, 2], fwd_recv.at[0, 2], down_i, j),
        remote(strip_in.at[1], strip_far.at[1], fwd_send.at[1, 2], fwd_recv.at[1, 2], up_i, j),
    )

    def pass_strips_on():
        pl.when(j < gy - 1)(lambda: strip_of(1, 0).wait_recv())
        pl.when(has_down)(lambda: strip_copies[0].start())
        pl.when(j > 0)(lambda: strip_of(1, 1).wait_recv())
        pl.when(has_up)(lambda: strip_copies[1].start())

    def strips_passed_on():
        @pl.when(has_up)
        def _():
            strip_copies[0].wait_recv()
            for p in range(4):
                got_k[0, p, pl.ds(SUB - 2, 2), :] = strip_far[0, pl.ds(2 * p, 2), :]

        @pl.when(has_down)
        def _():
            strip_copies[1].wait_recv()
            for p in range(4):
                got_k[gy + 1, p, pl.ds(0, 2), :] = strip_far[1, pl.ds(2 * p, 2), :]

    def pass_on(source):
        @pl.when((source == gy - 1) & has_down)
        def _():
            fwd_copies[0][0].start()
            fwd_copies[1][0].start()

        @pl.when((source == 0) & has_up)
        def _():
            fwd_copies[0][1].start()
            fwd_copies[1][1].start()

    def passed_on():
        @pl.when(has_up)
        def _():
            fwd_copies[0][0].wait_recv()
            fwd_copies[1][0].wait_recv()

        @pl.when(has_down)
        def _():
            fwd_copies[0][1].wait_recv()
            fwd_copies[1][1].wait_recv()

    def diagonal(row, held):
        rows = pl.ds(row, SUB)
        for t in range(slabs + 1):
            diag = f_a[6, t, rows, :] + 1.0
            valid = (halo_lanes_fine if t == halo else (lane >= 0)) & held
            fd[t, rows, :] = diag * diag
            fi[t, rows, :] = jnp.where(valid, 0.25 * (1.0 / diag), 0.0)

    def diagonals(step, carry):
        for n in range(4):
            diagonal(pl.multiple_of(FINE_OFF + SUB * (4 * step + n), SUB), lane >= 0)
        return carry

    lax.fori_loop(0, sh.fine_rows // (4 * SUB), diagonals, 0)

    for begin in range(0, gy, group):
        if begin in (0, gy // 2):
            for step in order[::-1] if begin == 0 else order:
                if (order.index(step) > 9) == (begin == 0):
                    sends[step][2].start()
        steps = ([0] + order)[begin : begin + group]
        count = len(steps) - steps.count(0)
        all_here(got_c.at[pl.ds(0, count)], a_recv.at[0, begin // group])
        all_here(got_p.at[pl.ds(0, count)], a_recv.at[1, begin // group])
        sources = [torus_back(j, step) if step else j for step in steps]
        for source in sources:
            pass_on(source)
        for source in sources:
            spread_first(source + 1, 0)
    pass_strips_on()

    def beside(values):
        side = values[halo]
        odd_right = [pltpu.roll(values[2 * h + 1], 1, 1) for h in range(halves)]
        even_left = [pltpu.roll(values[2 * h], LANES - 1, 1) for h in range(halves)]
        side_right, side_left = pltpu.roll(side, 1, 1), pltpu.roll(side, LANES - 1, 1)
        sums = []
        for h in range(halves):
            before = odd_right[h - 1] if h > 0 else side_right
            after = even_left[h + 1] if h < halves - 1 else side_left
            sums.append(jnp.where(first, before, odd_right[h]) + values[2 * h + 1])
            sums.append(values[2 * h] + jnp.where(last, after, even_left[h]))
        sums.append(
            jnp.where(first, odd_right[-1], side_right) + jnp.where(last, even_left[0], side_left)
        )
        return sums

    def squares(parts, scales, acc):
        for part_sum, scale in zip(parts, scales):
            acc = acc + part_sum * scale
        return acc

    def grown(total, new, old):
        step = new - old
        return step * step if total is None else total + step * step

    def fine_tile(m, acc, f_in, q_ref, f_out, count):
        base = FINE_OFF + 16 * m
        upper, lower = pl.ds(base, SUB, stride=2), pl.ds(base + 1, SUB, stride=2)
        above, below = pl.ds(base - 1, SUB, stride=2), pl.ds(base + 2, SUB, stride=2)
        crow = COARSE_OFF + SUB * m
        q_here, q_up, q_down = pl.ds(crow, SUB), pl.ds(crow - 1, SUB), pl.ds(crow + 1, SUB)
        inv_top = [fi[t, upper, :] for t in range(count)]
        inv_low = [fi[t, lower, :] for t in range(count)]
        part_top, part_low = [None] * slabs, [None] * slabs
        for k in range(3):
            tops = [f_in[k, t, upper, :] for t in range(slabs + 1)]
            lows = [f_in[k, t, lower, :] for t in range(slabs + 1)]
            top_sum, low_sum = beside(tops), beside(lows)
            for t in range(count):
                three = 3.0 * q_ref[k, t, q_here, :]
                nb = (lows[t] + f_in[k, t, above, :]) + (top_sum[t] + q_ref[k, t, q_up, :])
                new = (f_a[3 + k, t, upper, :] + (nb + three)) * inv_top[t]
                f_out[k, t, upper, :] = new
                nb2 = (tops[t] + f_in[k, t, below, :]) + (low_sum[t] + q_ref[k, t, q_down, :])
                new2 = (f_a[3 + k, t, lower, :] + (nb2 + three)) * inv_low[t]
                f_out[k, t, lower, :] = new2
                if t < slabs:
                    part_top[t] = grown(part_top[t], new, tops[t])
                    part_low[t] = grown(part_low[t], new2, lows[t])
        acc = squares(part_top, [fd[t, upper, :] for t in range(slabs)], acc)
        return squares(part_low, [fd[t, lower, :] for t in range(slabs)], acc)

    def coarse_sum(m, k, t, f_in, c_ref, w_ref):
        base = FINE_OFF + 16 * m
        upper, lower = pl.ds(base, SUB, stride=2), pl.ds(base + 1, SUB, stride=2)
        if t == coarse_halo:
            four = f_in[k, halo, upper, :] + f_in[k, halo, lower, :]
            four = four + swapped_pairs(four)
        else:
            four = (f_in[k, 2 * t, upper, :] + f_in[k, 2 * t, lower, :]) + (
                f_in[k, 2 * t + 1, upper, :] + f_in[k, 2 * t + 1, lower, :]
            )
        return coarse_near(m, k, t, c_ref, w_ref) + 0.5 * four

    def coarse_step(m, k, t, added, inv):
        rows = pl.ds(coarse_row(m), SUB)
        if t == coarse_halo:
            known = ckh[k, rows, :]
        else:
            known = 4.0 * got_k[m + 1, k, :, pl.ds(LANES * t, LANES)]
        return (known + added) * inv

    def coarse_tile(m, acc, added_of, c_ref, count, use):
        rows = pl.ds(coarse_row(m), SUB)
        inv = [ci[t, rows, :] for t in range(count)]
        parts = [None] * halves
        for k in range(3):
            values = []
            for t in range(count):
                value = coarse_step(m, k, t, added_of(k, t), inv[t])
                values.append(value)
                if t < halves:
                    parts[t] = grown(parts[t], value, c_ref[k, t, rows, :])
            use(k, values)
        return squares(parts, [cd[t, rows, :] for t in range(halves)], acc)

    def near_sum(m, carry):
        base = FINE_OFF + 16 * m
        upper, lower = pl.ds(base, SUB, stride=2), pl.ds(base + 1, SUB, stride=2)
        above, below = pl.ds(base - 1, SUB, stride=2), pl.ds(base + 2, SUB, stride=2)
        for k in range(3):
            tops = [f_b[k, t, upper, :] for t in range(slabs + 1)]
            lows = [f_b[k, t, lower, :] for t in range(slabs + 1)]
            top_sum, low_sum = beside(tops), beside(lows)
            both = [tops[t] + lows[t] for t in range(slabs + 1)]
            for t in range(slabs + 1):
                nb = (lows[t] + f_b[k, t, above, :]) + top_sum[t]
                near[k, t, upper, :] = f_a[3 + k, t, upper, :] + nb
                nb2 = (tops[t] + f_b[k, t, below, :]) + low_sum[t]
                near[k, t, lower, :] = f_a[3 + k, t, lower, :] + nb2
            rows = pl.ds(coarse_row(m), SUB)
            for t in range(halves):
                pre_b[k, t, rows, :] = 0.5 * (both[2 * t] + both[2 * t + 1])
            side = both[halo]
            pre_b[k, coarse_halo, rows, :] = 0.5 * (side + swapped_pairs(side))
        return zero

    def second_fine(m, acc):
        base = FINE_OFF + 16 * m
        upper, lower = pl.ds(base, SUB, stride=2), pl.ds(base + 1, SUB, stride=2)
        crow = COARSE_OFF + SUB * m
        q_here, q_up, q_down = pl.ds(crow, SUB), pl.ds(crow - 1, SUB), pl.ds(crow + 1, SUB)
        for t in range(slabs + 1):
            inv_top, inv_low = fi[t, upper, :], fi[t, lower, :]
            part_top, part_low = None, None
            for k in range(3):
                three = 3.0 * q_b[k, t, q_here, :]
                new = (near[k, t, upper, :] + (three + q_b[k, t, q_up, :])) * inv_top
                f_a[k, t, upper, :] = new
                new2 = (near[k, t, lower, :] + (three + q_b[k, t, q_down, :])) * inv_low
                f_a[k, t, lower, :] = new2
                if t < slabs:
                    part_top = grown(part_top, new, f_b[k, t, upper, :])
                    part_low = grown(part_low, new2, f_b[k, t, lower, :])
            if t < slabs:
                acc = acc + (part_top * fd[t, upper, :] + part_low * fd[t, lower, :])
        return acc

    def coarse_near(m, k, t, c_ref, w_ref):
        crow = COARSE_OFF + SUB * m
        nb = c_ref[k, t, pl.ds(crow - 1, SUB), :] + c_ref[k, t, pl.ds(crow + 1, SUB), :]
        return nb + w_ref[k, t, pl.ds(coarse_row(m), SUB), :]

    def first_sum(m, carry):
        rows = pl.ds(coarse_row(m), SUB)
        for k in range(3):
            for t in range(halves + 1):
                pre[k, t, rows, :] = coarse_sum(m, k, t, f_a, c_a, w_a)
        return zero

    def first_coarse(m, acc):
        rows = pl.ds(coarse_row(m), SUB)

        def use(k, values):
            produce(k, coarse_row(m), values, c_b, q_b, w_b)

        return coarse_tile(m, acc, lambda k, t: pre[k, t, rows, :], c_a, halves + 1, use)

    def second_coarse(m, acc):
        rows = pl.ds(coarse_row(m), SUB)

        def added_of(k, t):
            return pre_b[k, t, rows, :] + coarse_near(m, k, t, c_b, w_b)

        def use(k, values):
            produce(k, coarse_row(m), values, c_a, q_a, w_a, inner=True)

        return coarse_tile(m, acc, added_of, c_b, halves + 1, use)

    def third_coarse(m, acc):
        def added_of(k, t):
            return coarse_sum(m, k, t, f_a, c_a, w_a)

        def use(k, values):
            for t, value in enumerate(values):
                fin[m, k, :, pl.ds(LANES * t, LANES)] = value

        return coarse_tile(m, acc, added_of, c_a, halves, use)

    def every_tile(body, acc, unroll=6):
        def step(n, acc):
            m = n - 1
            part_sum = body(m, zero)
            inner = jnp.where((n > 0) & (n <= tiles), 1.0, 0.0).astype(F32)
            return acc + part_sum * inner

        return lax.fori_loop(0, tiles + 2, step, acc, unroll=unroll)

    def fine_first(m, acc):
        return fine_tile(m, acc, f_a, q_a, f_b, slabs + 1)

    def fine_third(m, acc):
        return fine_tile(m, acc, f_a, q_a, f_b, slabs)

    def both_first(m, acc):
        first_sum(m, 0)
        return fine_first(m, acc)

    fine_sum1 = lax.fori_loop(1, tiles - 1, fine_first, zero, unroll=14)
    lax.fori_loop(1, tiles - 1, first_sum, zero, unroll=7)

    @pl.when(has_up)
    def _():
        row_down.wait_recv()

    @pl.when(has_down)
    def _():
        row_up.wait_recv()

    for row, held in (
        (FINE_OFF - 16, lane < 0),
        (FINE_OFF - 8, (lane >= 0) & has_up),
        (fine_end, (lane >= 0) & has_down),
        (fine_end + 8, lane < 0),
    ):
        diagonal(row, held)

    passed_on()
    lax.fori_loop(0, 2, lambda e, c: spread_first((gy + 1) * e, c), 0, unroll=2)

    def outer_first(e, acc):
        for n in range(2):
            m = jnp.where(e == 0, n - 1, tiles - 1 + n)
            part_sum = both_first(m, zero)
            if n == 0:
                acc = acc + jnp.where(e == 1, 1.0, 0.0).astype(F32) * part_sum
            else:
                acc = acc + jnp.where(e == 0, 1.0, 0.0).astype(F32) * part_sum
        return acc

    fine_sum1 = lax.fori_loop(0, 2, outer_first, fine_sum1, unroll=2)
    every_tile(near_sum, zero)

    strips_passed_on()
    lax.fori_loop(0, 2, lambda e, c: spread_second((gy + 1) * e, c), 0, unroll=2)
    all_here(got_k.at[pl.ds(0, peers)], a_recv.at[2, 0])
    lax.fori_loop(1, gy + 1, spread_second, 0, unroll=8)

    @pl.when(has_down)
    def _():
        row_down.wait_send()

    @pl.when(has_up)
    def _():
        row_up.wait_send()

    def inner_share(m):
        return jnp.where((m >= 0) & (m < tiles), 1.0, 0.0).astype(F32)

    def lead(m, sums):
        share = inner_share(m)
        return (sums[0] + share * first_coarse(m, zero), sums[1], sums[2])

    def follow(m, sums):
        share = inner_share(m)
        fine_part = second_fine(m, zero)
        coarse_part = second_coarse(m, zero)
        return (sums[0], sums[1] + share * fine_part, sums[2] + share * coarse_part)

    def lead_and_follow(m, sums):
        return lead(m + 1, follow(m - 1, sums))

    sums = lax.fori_loop(-1, 1, lead, (zero, zero, zero), unroll=2)
    sums = lax.fori_loop(0, tiles, lead_and_follow, sums, unroll=4)
    sums = lax.fori_loop(tiles - 1, tiles + 1, follow, sums, unroll=2)
    coarse_sum1, fine_sum2, coarse_sum2 = sums
    coarse_sum3 = lax.fori_loop(0, tiles, third_coarse, zero, unroll=8)

    my_cols = pl.ds(pl.multiple_of(j * wide, LANES), wide)
    for step in order:
        to = torus_add(j, step)
        copy = remote(
            fin.at[to], coarse_out.at[:, :, my_cols], fin_sem.at[0], fin_sem.at[1], i, to
        )
        copy.start()
    for k in range(3):
        for t in range(halves):
            cols = pl.ds(pl.multiple_of(j * wide + LANES * t, LANES), LANES)
            coarse_out[k, :, cols] = fin[j, k, :, pl.ds(LANES * t, LANES)]

    fine_sum3 = lax.fori_loop(0, tiles, fine_third, zero, unroll=16)

    row_of = lax.broadcasted_iota(jnp.int32, (SUB, LANES), 0)
    mine = zero
    sums = ((fine_sum1, coarse_sum1), (fine_sum2, coarse_sum2), (fine_sum3, coarse_sum3))
    for s, (fine_part, coarse_part) in enumerate(sums):
        line = jnp.sum(fine_part + coarse_part, axis=0, keepdims=True)
        mine = jnp.where(row_of == s, line, mine)
    part[0] = mine
    for step in range(1, gx):
        copy = remote(
            part.at[0],
            part_gx.at[step],
            norm_sem.at[0],
            norm_sem.at[1],
            lax.rem(i + step, gx),
            j,
        )
        copy.start()

    def join_columns(k, carry):
        for b in range(sh.blocks):
            rows = pl.ds(FINE_OFF + LANES * b, LANES)
            for s in range(slabs):
                begin = 2 * LANES * (s // 2) + s % 2
                swapped[b, pl.ds(begin, LANES, stride=2), :] = f_b[k, s, rows, :].T
            for t in range(slabs):
                natural = swapped[b, pl.ds(LANES * t, LANES), :].T
                fine_out[k, pl.ds(LANES * b, LANES), pl.ds(LANES * t, LANES)] = natural
        return carry

    lax.fori_loop(0, 3, join_columns, 0)

    all_here(part_gx.at[pl.ds(1, gx - 1)], norm_sem.at[1])
    for step in range(1, gx):
        mine = mine + part_gx[step]
    part[1] = mine
    for step in order:
        copy = remote(
            part.at[1],
            part_gy.at[step],
            norm_sem.at[2],
            norm_sem.at[3],
            i,
            torus_add(j, step),
        )
        copy.start()
    all_here(part_gy.at[pl.ds(1, peers)], norm_sem.at[3])
    for step in order:
        mine = mine + part_gy[step]
    total = jnp.sum(mine, axis=1, keepdims=True) * (1.0 / sh.cells)
    norm_out[...] = jnp.broadcast_to(jnp.sqrt(total), (SUB, LANES))

    @pl.when(has_right)
    def _():
        edge_right.wait_send()

    @pl.when(has_left)
    def _():
        edge_left.wait_send()

    @pl.when(has_down)
    def _():
        for kind in range(2):
            fwd_copies[kind][0].wait_send()
        strip_copies[0].wait_send()

    @pl.when(has_up)
    def _():
        for kind in range(2):
            fwd_copies[kind][1].wait_send()
        strip_copies[1].wait_send()

    for kind, ref in enumerate((got_c, got_p, got_k)):
        all_sent(ref.at[pl.ds(0, peers)], a_send.at[kind])

    @pl.when((j == 0) | (j == gy - 1))
    def _():
        all_sent(strip_out.at[pl.ds(0, peers)], strip_send.at[0])

    all_sent(fin.at[pl.ds(0, peers)], fin_sem.at[0])
    all_here(fin.at[pl.ds(0, peers)], fin_sem.at[1])
    all_sent(part_gx.at[pl.ds(1, gx - 1)], norm_sem.at[0])
    all_sent(part_gy.at[pl.ds(1, peers)], norm_sem.at[2])


def store_kernel(fine, coarse, norms, fine_out, coarse_out, norm_out, scalars, sem):
    half = fine.shape[1] // 2
    for k in range(fine.shape[0]):
        for part in range(2):
            rows = pl.ds(half * part, half)
            pltpu.make_async_copy(fine.at[k, rows], fine_out.at[k, rows], sem.at[0]).start()
    stores = [
        pltpu.make_async_copy(coarse, coarse_out, sem.at[1]),
        pltpu.make_async_copy(scalars, norm_out, sem.at[2]),
    ]
    stores[0].start()
    for s in range(SWEEPS):
        scalars[s] = norms[s, 0]
    stores[1].start()
    for copy in stores:
        copy.wait()
    pltpu.make_async_copy(fine, fine_out, sem.at[0]).wait()


def solution(mesh):
    gx, gy = mesh.shape["gx"], mesh.shape["gy"]

    def on_device(fine_start, fine_known, fine_mu, coarse_start, coarse_known, coarse_mu):
        sh = Shape(gx, gy, *fine_mu.shape)
        dma = pltpu.SemaphoreType.DMA
        in_hbm = pl.BlockSpec(memory_space=pltpu.HBM)
        on_chip = pl.BlockSpec(memory_space=pltpu.VMEM)

        def fine(*lead):
            return pltpu.VMEM((*lead, sh.slabs + 1, sh.fine_buf, LANES), F32)

        def coarse(*lead):
            return pltpu.VMEM((*lead, sh.coarse_buf, LANES), F32)

        few = sh.halves + 1
        fine_v, coarse_v, norm_v = pl.pallas_call(
            functools.partial(kernel, sh),
            out_shape=(
                pltpu.VMEM(fine_start.shape, F32),
                pltpu.VMEM(coarse_start.shape, F32),
                pltpu.VMEM((SUB, LANES), F32),
            ),
            in_specs=[in_hbm] * 6,
            out_specs=(on_chip, on_chip, on_chip),
            scratch_shapes=[
                pltpu.VMEM((PLANES, sh.slabs, sh.fine_rows, LANES), F32),
                pltpu.VMEM((PLANES, sh.blocks, sh.slabs * LANES + SUB, LANES), F32),
                pltpu.VMEM((sh.blocks, sh.slabs * LANES + SUB, LANES), F32),
                fine(PLANES),
                fine(3),
                fine(),
                fine(),
                coarse(3, few),
                coarse(3, few),
                coarse(3, sh.slabs + 1),
                coarse(3, sh.slabs + 1),
                coarse(3, few),
                coarse(3, few),
                coarse(3),
                coarse(few),
                coarse(few),
                coarse(3, few),
                coarse(3, few),
                fine(3),
                pltpu.VMEM((PLANES, SUB, gy * sh.wide), F32),
                pltpu.VMEM((PLANES, gy * SUB, LANES), F32),
                pltpu.VMEM((gy, SUB, LANES), F32),
                pltpu.VMEM((gy + 2, 3, SUB, sh.wide), F32),
                pltpu.VMEM((gy + 2, SUB, LANES), F32),
                pltpu.VMEM((gy + 2, 4, SUB, sh.wide), F32),
                pltpu.VMEM((gy, SUB, sh.wide), F32),
                pltpu.VMEM((2, SUB, sh.wide), F32),
                pltpu.VMEM((2, SUB, sh.wide), F32),
                pltpu.VMEM((2, PLANES, SUB, LANES), F32),
                pltpu.VMEM((2, PLANES, SUB, LANES), F32),
                pltpu.VMEM((gy, 3, SUB, sh.wide), F32),
                pltpu.VMEM((2, SUB, LANES), F32),
                pltpu.VMEM((gy, SUB, LANES), F32),
                pltpu.VMEM((gx, SUB, LANES), F32),
                dma((2,)),
                dma((2,)),
                dma((2,)),
                dma((2,)),
                dma((2,)),
                dma((3,)),
                dma((3, 4)),
                dma((2, 3)),
                dma((2, 3)),
                dma((1,)),
                dma((2,)),
                dma((2,)),
                dma((4,)),
            ],
            compiler_params=pltpu.CompilerParams(
                collective_id=0, has_side_effects=True, vmem_limit_bytes=64_500_000
            ),
            name="interface_sweeps",
        )(fine_start, fine_known, fine_mu, coarse_start, coarse_known, coarse_mu)
        anywhere = pl.BlockSpec(memory_space=pl.ANY)
        return pl.pallas_call(
            store_kernel,
            out_shape=(
                jax.ShapeDtypeStruct(fine_start.shape, F32),
                jax.ShapeDtypeStruct(coarse_start.shape, F32),
                jax.ShapeDtypeStruct((SWEEPS,), F32),
            ),
            in_specs=[anywhere, anywhere, on_chip],
            out_specs=(in_hbm, in_hbm, in_hbm),
            scratch_shapes=[pltpu.SMEM((SWEEPS,), F32), dma((3,))],
            compiler_params=pltpu.CompilerParams(vmem_limit_bytes=1_000_000),
            name="store_results",
        )(fine_v, coarse_v, norm_v)

    return jax.shard_map(
        on_device,
        mesh=mesh,
        in_specs=(
            P(None, "gx", "gy"),
            P(None, "gx", "gy"),
            P("gx", "gy"),
            P(None, ("gx", "gy"), None),
            P(None, ("gx", "gy"), None),
            P(("gx", "gy"), None),
        ),
        out_specs=(P(None, "gx", "gy"), P(None, ("gx", "gy"), None), P(None)),
        check_vma=False,
    )
```
